256 devices in a mesh: robot: 16 (over y, x_lo, core), seed: 16 (over x_hi, z).
Axes of the slice: x: 4 (x_hi: 2, x_lo: 2; x = x_hi * 2 + x_lo), y: 4, z: 8, core: 2. Of those that a mesh axis runs over, the one named last changes fastest.
Arguments:
- centres: float32 [32, 3, 52, 4096], P('robot', None, None, 'seed'), may hold values from -52 to 52
- sphere_radius: float32 [32, 52], P('robot'), may hold values from 0.2 to 0.8
- counts: int32 [32], P('robot'), may hold values from 26 to 52
- adjacency: int32 [32, 32], P('robot'), may hold values from 0 to 1, as said below
Outputs:
- collision_cost: float32 [32, 4096], P('robot', 'seed')
- blended_path: float32 [32, 3, 52, 32], P('robot')
The draws below stay inside these ranges and needn't reach their ends.
Inputs may be any that keep to these rules, and one draw needn't show every extreme that they name: `adjacency`: symmetric, with zeros on the diagonal.
All inputs are finite; a program needn't handle non-finite values.
Results may differ from the reference program's by a relative error of at most 0.0003.
Values sent between devices are 32-bit elements; how exact they have to be, the bound alone decides.
A program may use at most 64 MiB of HBM per device.

```python
import math
import jax
import jax.numpy as jnp
import numpy as np
from jax import lax

P_SIZE = 52
W = 32
ROBOTS = 32
SEEDS = 128


grid_columns = 4


spacing = 1.8


def cell_slots(key):
    return jax.random.permutation(jax.random.fold_in(key, 7), ROBOTS).astype(jnp.int32)


def draw_adjacency(key, part):
    slot = cell_slots(key)
    grid_row = slot // grid_columns
    grid_col = slot % grid_columns
    row_gap = jnp.abs(grid_row[:, None] - grid_row[None, :])
    col_gap = jnp.abs(grid_col[:, None] - grid_col[None, :])
    linked = (row_gap <= 1) & (col_gap <= 1) & (slot[:, None] != slot[None, :])
    return linked.astype(jnp.int32)


def draw_centres(key, part):
    slot = cell_slots(key)
    grid_row = (slot // grid_columns).astype(jnp.float32)
    grid_col = (slot % grid_columns).astype(jnp.float32)
    row_total = ROBOTS // grid_columns
    base_x = spacing * (grid_col - 0.5 * (grid_columns - 1))
    base_y = spacing * (grid_row - 0.5 * (row_total - 1))
    base = jnp.stack([base_x, base_y, jnp.zeros_like(base_x)], axis=1)
    sphere_order = jnp.arange(P_SIZE, dtype=jnp.int32)
    side = jnp.where(sphere_order < P_SIZE // 2, -0.6, 0.6).astype(jnp.float32)
    lobes = jnp.stack([jnp.zeros_like(side), side, jnp.full_like(side, 0.8)], axis=0)
    arm_key = jax.random.fold_in(key, 31)
    shift_key = jax.random.fold_in(key, 37)
    scale_key = jax.random.fold_in(key, 41)
    step_key = jax.random.fold_in(key, 43)
    step_scale = jnp.exp(jax.random.uniform(scale_key, (ROBOTS, 1, P_SIZE, 1, 1), jnp.float32, jnp.log(0.04), jnp.log(0.15)))
    arm = 0.5 * jnp.clip(jax.random.normal(arm_key, (ROBOTS, 3, P_SIZE), jnp.float32), -4.0, 4.0)
    shift = 0.5 * jnp.clip(jax.random.normal(shift_key, (ROBOTS, 3, SEEDS), jnp.float32), -3.0, 3.0)
    steps = step_scale * jnp.clip(jax.random.normal(step_key, (ROBOTS, 3, P_SIZE, SEEDS, W - 1), jnp.float32), -3.0, 3.0)
    walk = jnp.concatenate([jnp.zeros((ROBOTS, 3, P_SIZE, SEEDS, 1), jnp.float32), jnp.cumsum(steps, axis=4)], axis=4)
    centre = base[:, :, None, None, None] + lobes[None, :, :, None, None] + arm[:, :, :, None, None]
    centre = centre + shift[:, :, None, :, None] + walk
    return centre.reshape(ROBOTS, 3, P_SIZE, SEEDS * W)


def with_ends(result, own_key, smallest, high):
    longest = result.shape.index(max(result.shape))
    spots = []
    for shift in (0, 1):
        where = [jax.random.randint(jax.random.fold_in(own_key, axis), (), 0, length) for axis, length in enumerate(result.shape)]
        where[longest] = (where[longest] + shift) % result.shape[longest]
        spots.append(tuple(where))
    return result.at[spots[0]].set(smallest).at[spots[1]].set(high)


def shard_levels(stream_key, extent, shards, low, top_value):
    level, own = 1.0, jax.random.fold_in(stream_key, 6)
    for position, shards_of in shards:
        steps = jnp.exp(jax.random.uniform(jax.random.fold_in(own, position), (shards_of,), jnp.float32, low / len(shards), top_value / len(shards)))
        level = level * jnp.repeat(steps, extent[position] // shards_of).reshape([-1 if axis == position else 1 for axis in range(len(extent))])
    return level


def setup_inputs(seed: int = 0) -> dict:
    seeds = jax.random.split(jax.random.key(seed), 5)
    centres = draw_centres(jax.random.fold_in(seeds[4], 71), 0)
    sphere_radius = jnp.clip(jnp.exp(math.log(0.8) - 1.3862944 * jax.random.uniform(seeds[1], (ROBOTS, P_SIZE), jnp.float32) ** shard_levels(seeds[1], (ROBOTS, P_SIZE), ((0, 16),), -0.2, 0.2)), 0.2, 0.8)
    counts = with_ends(jax.random.randint(seeds[2], (ROBOTS,), P_SIZE // 2, P_SIZE + 1), jax.random.fold_in(seeds[2], 1), P_SIZE // 2, P_SIZE).astype(jnp.int32)
    adjacency = draw_adjacency(jax.random.fold_in(seeds[4], 71), 0)
    return {"centres": centres, "sphere_radius": sphere_radius, "counts": counts, "adjacency": adjacency}


lane_width = 128

def swept_blocks(centres, sphere_radius):
    robots_here, _, spheres, columns = centres.shape
    shaped = centres.reshape(robots_here, 3, spheres, columns // W, W)
    ahead_point = jnp.concatenate([shaped[..., 1:], shaped[..., -1:]], axis=4)
    middle = 0.5 * (shaped + ahead_point)
    step_length = jnp.sqrt(lax.optimization_barrier(jnp.sum((ahead_point - shaped) ** 2, axis=1)) + 1e-06)
    swept_radius = sphere_radius[:, :, None, None] + 0.5 * step_length
    swept_block = jnp.concatenate([middle, swept_radius[:, None]], axis=1)
    return swept_block.reshape(robots_here, 4, spheres, columns)

def active_spheres(counts, spheres):
    return (jnp.arange(spheres, dtype=jnp.int32)[None, :] < counts[:, None]).astype(jnp.float32)

def pair_cost(first_block, first_active, second_block, second_active, sphere_mask):
    spheres = first_block.shape[1]
    columns = first_block.shape[2]
    weights = first_active[:, None] * second_active[None, :] * sphere_mask

    def tile_cost(tile_index):
        offset = tile_index * lane_width
        first_tile = lax.dynamic_slice_in_dim(first_block, offset, lane_width, 2)
        second_tile = lax.dynamic_slice_in_dim(second_block, offset, lane_width, 2)
        distance = jnp.zeros((spheres, spheres, lane_width), jnp.float32)
        for axis_index in range(3):
            gap = first_tile[axis_index][:, None, :] - second_tile[axis_index][None, :, :]
            distance = distance + gap * gap
        spread = first_tile[3][:, None, :] + second_tile[3][None, :, :]
        return lax.optimization_barrier(jnp.sum(weights[:, :, None] * jnp.exp(-distance / (spread * spread)), axis=(0, 1)))
    tiles = lax.map(tile_cost, jnp.arange(columns // lane_width, dtype=jnp.int32))
    return tiles.reshape(columns) / (spheres * spheres)

def self_costs(own_blocks, own_active):
    spheres = own_blocks.shape[2]
    order = jnp.arange(spheres, dtype=jnp.int32)
    apart = (order[None, :] >= order[:, None] + 2).astype(jnp.float32)

    def single(robot_row):
        return pair_cost(own_blocks[robot_row], own_active[robot_row], own_blocks[robot_row], own_active[robot_row], apart)
    return lax.map(single, jnp.arange(own_blocks.shape[0], dtype=jnp.int32))

def seed_weights(centres, robot_cost):
    robots_here, _, spheres, columns = centres.shape
    seed_count = columns // W
    seed_cost = lax.optimization_barrier(jnp.sum(robot_cost.reshape(robots_here, seed_count, W), axis=2))
    weight = 1.0 / (1.0 + seed_cost)
    shaped = centres.reshape(robots_here, 3, spheres, seed_count, W)
    weighted = lax.optimization_barrier(jnp.sum(shaped * weight[:, None, None, :, None], axis=3))
    return (weighted, lax.optimization_barrier(jnp.sum(weight, axis=1)))

def reference(centres, sphere_radius, counts, adjacency):
    blocks = swept_blocks(centres, sphere_radius)
    spheres = blocks.shape[2]
    columns = blocks.shape[3]
    active = active_spheres(counts, spheres)
    full_mask = jnp.ones((spheres, spheres), jnp.float32)
    start_cost = self_costs(blocks, active)
    firsts, seconds = np.triu_indices(ROBOTS, 1)
    pair_list = jnp.asarray(np.stack([firsts, seconds], axis=1), dtype=jnp.int32)

    def add_pair(totals_now, pair_row):
        first_row = pair_row[0]
        second_row = pair_row[1]
        pair_term = lax.cond(adjacency[first_row, second_row] != 0, lambda: pair_cost(blocks[first_row], active[first_row], blocks[second_row], active[second_row], full_mask), lambda: jnp.zeros((columns,), jnp.float32))
        return (totals_now.at[first_row].add(pair_term).at[second_row].add(pair_term), None)
    robot_cost, _ = lax.scan(add_pair, start_cost, pair_list)
    weighted, totals = seed_weights(centres, robot_cost)
    return (robot_cost, weighted / totals[:, None, None, None])
```

```python
import functools
import math

import jax
import jax.numpy as jnp
from jax import lax
from jax.experimental import pallas as pl
from jax.experimental.pallas import tpu as pltpu
from jax.sharding import PartitionSpec as P

W = 32
SPHERES = 52
GROUPS = 7
FIRST_GROUPS = 4
ROBOTS_HERE = 2
ROBOT_DEVICES = 16
ROBOTS = ROBOTS_HERE * ROBOT_DEVICES
LANES = 128
COLUMNS = 256
PART = 16
ROWS = ROBOTS_HERE * GROUPS * 4
Z = 8
CHUNK = 11
COUNT_LANE = 32
LENGTH_LANE = 32
GROUPS_LANE = 33
ROOT = math.sqrt(math.log2(math.e))
FAR = 1.0e6
MESH = pl.DeviceIdType.MESH


def iota(axis, shape=(8, LANES)):
    return lax.broadcasted_iota(jnp.int32, shape, axis)


def pair_term(a, b):
    dx, dy, dz = a[0] - b[0], a[1] - b[1], a[2] - b[2]
    spread = a[3] + b[3]
    return jnp.exp2((dx * dx + dy * dy + dz * dz) / (-spread * spread))


def spread_kernel(
    counts_ref,
    centres_ref,
    radius_ref,
    adjacency_ref,
    recv_ref,
    self_ref,
    table_ref,
    send,
    swept,
    note_send,
    note_recv,
    note,
    send_sem,
    recv_sem,
    note_send_sem,
    note_recv_sem,
):
    me = lax.axis_index("robot")
    seed = lax.axis_index("seed")
    peers = [lax.rem(me + step, ROBOT_DEVICES) for step in range(1, ROBOT_DEVICES)]

    barrier = pltpu.get_barrier_semaphore()
    for peer in peers:
        pl.semaphore_signal(barrier, inc=1, device_id=(peer, seed), device_id_type=MESH)

    sub, lane = iota(0), iota(1)
    part = lane // PART
    last_waypoint = lane % W == W - 1
    radius_lane = iota(1, (8, SPHERES))
    radius_sub = iota(0, (8, SPHERES))
    for robot in range(ROBOTS_HERE):
        count = counts_ref[robot]
        radius_row = jnp.broadcast_to(radius_ref[robot : robot + 1, :], (8, SPHERES))
        number = (me * ROBOTS_HERE + robot) * 64 + 1
        for group in range(GROUPS):
            radius = jnp.sum(
                jnp.where(radius_lane == radius_sub + 8 * group, radius_row, 0.0),
                axis=1,
                keepdims=True,
            )
            sphere = sub + 8 * group
            active = sphere < count
            far = FAR * (sphere + number).astype(jnp.float32)
            for half in range(2):
                at = slice(half * LANES, (half + 1) * LANES)
                out, square = [], None
                for axis in range(3):
                    if group < GROUPS - 1:
                        here = centres_ref[robot, axis, 8 * group : 8 * group + 8, at]
                    else:
                        here = pltpu.roll(
                            centres_ref[robot, axis, SPHERES - 8 : SPHERES, at], 4, 0
                        )
                    ahead = jnp.where(last_waypoint, here, pltpu.roll(here, LANES - 1, 1))
                    step = ahead - here
                    square = step * step if square is None else square + step * step
                    middle = (here + ahead) * (0.5 * ROOT)
                    out.append(jnp.where(active, middle, far if axis == 0 else 0.0))
                out.append(jnp.where(active, radius + 0.5 * jnp.sqrt(square + 1e-6), 1.0))
                for quantity in range(4):
                    value = out[quantity]
                    swept[half * ROBOTS_HERE + robot, quantity, 8 * group : 8 * group + 8, :] = value
                    value = pltpu.roll(value, 0, 1, stride=PART, stride_axis=0)
                    for bit in (1, 2, 4):
                        value = jnp.where(part & bit != 0, pltpu.roll(value, 8 - bit, 0), value)
                    row = (robot * GROUPS + group) * 4 + quantity
                    send[pl.ds(half * 8 * ROWS + row, 8, stride=ROWS), :] = value
        for half in range(2):
            for quantity in range(4):
                fill = FAR * (sub + 56 + number).astype(jnp.float32) if quantity == 0 else jnp.full((8, LANES), float(quantity == 3))
                swept[half * ROBOTS_HERE + robot, quantity, 56:64, :] = fill

    note_send[...] = jnp.zeros((ROBOTS_HERE, LANES), jnp.int32)
    note_send[:, 0:ROBOTS] = adjacency_ref[...]
    for robot in range(ROBOTS_HERE):
        note_send[robot : robot + 1, COUNT_LANE : COUNT_LANE + 1] = jnp.full((1, 1), counts_ref[robot], jnp.int32)

    pl.semaphore_wait(barrier, ROBOT_DEVICES - 1)

    def slot_of(device):
        return (device // 8) * 8 + lax.rem(8 - lax.rem(device, 8), 8)

    def rows_of(slot):
        return pl.ds(pl.multiple_of(slot * ROWS, 8), ROWS)

    notes, copies = [], []
    for number, peer in enumerate(peers):
        copy = pltpu.make_async_remote_copy(
            src_ref=note_send,
            dst_ref=note_recv.at[me],
            send_sem=note_send_sem.at[number],
            recv_sem=note_recv_sem.at[number],
            device_id=(peer, seed),
            device_id_type=MESH,
        )
        copy.start()
        notes.append(copy)
    for number, peer in enumerate(peers):
        copy = pltpu.make_async_remote_copy(
            src_ref=send.at[rows_of(slot_of(peer))],
            dst_ref=recv_ref.at[rows_of(me)],
            send_sem=send_sem.at[number],
            recv_sem=recv_sem.at[number],
            device_id=(peer, seed),
            device_id_type=MESH,
        )
        copy.start()
        copies.append(copy)
    note_recv[me] = note_send[...]
    recv_ref[rows_of(me), :] = send[rows_of(slot_of(me)), :]

    def self_pairs(index, carry):
        half, robot = index // ROBOTS_HERE, lax.rem(index, ROBOTS_HERE)
        sums = [jnp.zeros((8, LANES), jnp.float32) for _ in range(4)]
        turn = 0
        for group in range(GROUPS):
            first = [swept[index, q, 8 * group : 8 * group + 8, :] for q in range(4)]
            for apart in range(2, SPHERES - 8 * group):
                start = 8 * group + apart
                second = [swept[index, q, start : start + 8, :] for q in range(4)]
                sums[turn] = sums[turn] + pair_term(first, second)
                turn = (turn + 1) % 4
        total = jnp.sum((sums[0] + sums[1]) + (sums[2] + sums[3]), axis=0, keepdims=True)
        self_ref[pl.ds(index, 1), :] = total * (1.0 / (SPHERES * SPHERES))
        return carry

    lax.fori_loop(0, 2 * ROBOTS_HERE, self_pairs, 0)

    for copy in notes:
        copy.wait_recv()
    for device in range(ROBOT_DEVICES):
        note[ROBOTS_HERE * device : ROBOTS_HERE * (device + 1), :] = note_recv[device]
    shape = (ROBOTS, LANES)
    row, column = iota(0, shape), iota(1, shape)
    noted = note[...].astype(jnp.float32)
    link = jnp.where((column > row) & (column < ROBOTS) & (noted != 0.0), 1.0, 0.0)
    counts = jnp.sum(jnp.where(column == COUNT_LANE, noted, 0.0), axis=1, keepdims=True)
    before = (iota(0, (LANES, LANES)) < iota(1, (LANES, LANES))).astype(jnp.float32)
    rank = jnp.dot(link, before, preferred_element_type=jnp.float32)
    linked_column = link * column.astype(jnp.float32)
    table = jnp.zeros(shape, jnp.float32)
    for place in range(ROBOTS - 1):
        found = jnp.sum(jnp.where(rank == float(place), linked_column, 0.0), axis=1, keepdims=True)
        table = jnp.where(column == place, found, table)
    table = jnp.where(column == LENGTH_LANE, jnp.sum(link, axis=1, keepdims=True), table)
    table = table.astype(jnp.int32)
    groups = (counts.astype(jnp.int32) + 7) >> 3
    table_ref[...] = jnp.where(column == GROUPS_LANE, groups, table)

    for copy in copies:
        copy.wait_recv()
    for copy in notes + copies:
        copy.wait_send()


def cross_kernel(table, rows, cost_ref, turned, total):
    def prepare(robot, carry):
        for row in range(4 * GROUPS):
            line = rows[pl.ds(robot * (4 * GROUPS) + row, 1), :]
            turned[robot, row] = pltpu.roll(
                jnp.broadcast_to(line, (8, LANES)), 0, 1, stride=PART, stride_axis=0
            )
        total[robot] = jnp.zeros((8, LANES), jnp.float32)
        return carry

    lax.fori_loop(0, ROBOTS, prepare, 0)

    def pair_sum(first_groups, second_groups, first, second):
        sums = [None] * 4
        turn = 0
        for second_group in range(second_groups):
            b = [
                jnp.broadcast_to(
                    rows[pl.ds(second * (4 * GROUPS) + second_group * 4 + q, 1), :], (8, LANES)
                )
                for q in range(4)
            ]
            for first_group in range(first_groups):
                a = [turned[first, first_group * 4 + q] for q in range(4)]
                term = pair_term(a, b)
                sums[turn] = term if sums[turn] is None else sums[turn] + term
                turn = (turn + 1) % 4
        return (sums[0] + sums[1]) + (sums[2] + sums[3])

    def of_robot(first, carry):
        first_groups = table[first, GROUPS_LANE]

        def of_pair(place, carry):
            second = table[first, place]
            second_groups = table[second, GROUPS_LANE]
            case = (first_groups - FIRST_GROUPS) * 4 + (second_groups - FIRST_GROUPS)
            found = lax.switch(
                case,
                [
                    functools.partial(pair_sum, m, n)
                    for m in range(FIRST_GROUPS, GROUPS + 1)
                    for n in range(FIRST_GROUPS, GROUPS + 1)
                ],
                first,
                second,
            )
            total[first] = total[first] + found
            total[second] = total[second] + found
            return carry

        return lax.fori_loop(0, table[first, LENGTH_LANE], of_pair, carry)

    lax.fori_loop(0, ROBOTS, of_robot, 0)

    cost = jnp.sum(total[...], axis=1)
    for shift in (64, 32, 16):
        cost = cost + pltpu.roll(cost, shift, 1)
    cost = cost * (1.0 / (SPHERES * SPHERES))
    for device in range(ROBOT_DEVICES):
        cost_ref[device] = cost[ROBOTS_HERE * device : ROBOTS_HERE * (device + 1), :]


def blend_kernel(
    cost_ref,
    self_ref,
    centres_ref,
    robot_cost_ref,
    blended_ref,
    cost_recv,
    weight,
    packed,
    parts,
    mine,
    other,
    gathered,
    cost_sems,
    part_sems,
    pair_sems,
    gather_sems,
):
    me = lax.axis_index("robot")
    seed = lax.axis_index("seed")
    x, z = seed // Z, lax.rem(seed, Z)
    peers = [lax.rem(me + step, ROBOT_DEVICES) for step in range(1, ROBOT_DEVICES)]
    z_peers = [lax.rem(z + step, Z) for step in range(1, Z)]
    opposite = (1 - x) * Z + z

    barrier = pltpu.get_barrier_semaphore()
    for peer in peers:
        pl.semaphore_signal(barrier, inc=1, device_id=(peer, seed), device_id_type=MESH)
    for peer in z_peers:
        pl.semaphore_signal(barrier, inc=1, device_id=(me, x * Z + peer), device_id_type=MESH)
    pl.semaphore_signal(barrier, inc=1, device_id=(me, opposite), device_id_type=MESH)
    pl.semaphore_wait(barrier, ROBOT_DEVICES - 1 + Z)

    def start(src, dst, sems, number, device):
        copy = pltpu.make_async_remote_copy(
            src_ref=src,
            dst_ref=dst,
            send_sem=sems.at[0, number],
            recv_sem=sems.at[1, number],
            device_id=device,
            device_id_type=MESH,
        )
        copy.start()
        return copy

    copies = [
        start(cost_ref.at[peer], cost_recv.at[me], cost_sems, number, (peer, seed))
        for number, peer in enumerate(peers)
    ]
    cost_recv[me] = cost_ref[me]
    for copy in copies:
        copy.wait_recv()
    sent = copies

    lane = iota(1, (ROBOTS_HERE, LANES))
    part = lane // PART
    for half in range(2):
        cost = self_ref[half * ROBOTS_HERE : (half + 1) * ROBOTS_HERE, :]
        for k in range(8):
            cost = cost + jnp.where(part == k, cost_recv[half * 8 + k], 0.0)
        robot_cost_ref[:, half * LANES : (half + 1) * LANES] = cost
        for bit in (1, 2, 4, 8, 16):
            cost = cost + jnp.where(
                lane & bit != 0, pltpu.roll(cost, bit, 1), pltpu.roll(cost, LANES - bit, 1)
            )
        weight[half] = 1.0 / (1.0 + cost)
    sums = weight[0] + weight[1]
    sums = sums + pltpu.roll(sums, 64, 1)
    sums = sums + pltpu.roll(sums, 32, 1)
    line = iota(1, (1, LANES))
    total_row = jnp.where(line < 64, sums[0:1, :], sums[1:2, :])

    quarter = iota(1) // W
    units = [[], []]
    for robot in range(ROBOTS_HERE):
        weights = [
            jnp.broadcast_to(weight[half, robot : robot + 1, :], (8, LANES)) for half in range(2)
        ]
        for axis in range(3):
            for group in range(GROUPS):
                start_row = min(8 * group, SPHERES - 8)
                value = (
                    centres_ref[robot, axis, start_row : start_row + 8, 0:LANES] * weights[0]
                    + centres_ref[robot, axis, start_row : start_row + 8, LANES:COLUMNS] * weights[1]
                )
                if group == GROUPS - 1:
                    value = pltpu.roll(value, 4, 0)
                value = value + pltpu.roll(value, 64, 1)
                units[robot].append(value + pltpu.roll(value, 32, 1))
        units[robot].append(jnp.zeros((8, LANES), jnp.float32))
    for v in range(CHUNK):
        value = jnp.where(
            quarter < 2,
            jnp.where(quarter == 0, units[0][2 * v], units[0][2 * v + 1]),
            jnp.where(quarter == 2, units[1][2 * v], units[1][2 * v + 1]),
        )
        done = 0
        while done < 8:
            chunk, row = divmod(8 * v + done, CHUNK)
            length = min(8 - done, CHUNK - row)
            packed[chunk, row : row + length, :] = value[done : done + length, :]
            done += length
    for chunk in range(Z):
        packed[chunk, CHUNK : CHUNK + 1, :] = total_row

    copies = [
        start(packed.at[peer], parts.at[number], part_sems, number, (me, x * Z + peer))
        for number, peer in enumerate(z_peers)
    ]
    found = packed[z]
    for number, copy in enumerate(copies):
        copy.wait_recv()
        found = found + parts[number]
    sent = sent + copies

    mine[...] = found
    copy = start(mine, other, pair_sems, 0, (me, opposite))
    copy.wait_recv()
    sent = sent + [copy]
    found = mine[...] + other[...]
    gathered[z] = found / found[CHUNK : CHUNK + 1, :]

    copies = [
        start(gathered.at[z], gathered.at[z], gather_sems, number, (me, x * Z + peer))
        for number, peer in enumerate(z_peers)
    ]
    for copy in copies:
        copy.wait_recv()
    sent = sent + copies

    for chunk in range(Z):
        value = gathered[chunk]
        turned = [value] + [pltpu.roll(value, LANES - W * q, 1) for q in range(1, 4)]
        row = 0
        while row < CHUNK:
            v, at = divmod(CHUNK * chunk + row, 8)
            length = min(8 - at, CHUNK - row)
            for q in range(4):
                robot, unit = q // 2, 2 * v + q % 2
                if unit < 3 * GROUPS:
                    axis, group = divmod(unit, GROUPS)
                    first = 8 * group + at
                    rows = min(length, SPHERES - first)
                    if rows > 0:
                        blended_ref[robot, axis, first : first + rows, :] = turned[q][
                            row : row + rows, 0:W
                        ]
            row += length

    for copy in sent:
        copy.wait_send()


def in_vmem(count):
    return [pl.BlockSpec(memory_space=pltpu.VMEM)] * count


IN_SMEM = pl.BlockSpec(memory_space=pltpu.SMEM)


def local(centres, sphere_radius, counts, adjacency):
    dma = pltpu.SemaphoreType.DMA
    f32 = jnp.float32
    peers = ROBOT_DEVICES - 1
    received, self_cost, table = pl.pallas_call(
        spread_kernel,
        out_shape=(
            jax.ShapeDtypeStruct((ROBOT_DEVICES * ROWS, LANES), f32),
            jax.ShapeDtypeStruct((2 * ROBOTS_HERE, LANES), f32),
            jax.ShapeDtypeStruct((ROBOTS, LANES), jnp.int32),
        ),
        in_specs=[IN_SMEM] + in_vmem(3),
        out_specs=tuple(in_vmem(3)),
        scratch_shapes=[
            pltpu.VMEM((ROBOT_DEVICES * ROWS, LANES), f32),
            pltpu.VMEM((2 * ROBOTS_HERE, 4, 64, LANES), f32),
            pltpu.VMEM((ROBOTS_HERE, LANES), jnp.int32),
            pltpu.VMEM((ROBOT_DEVICES, ROBOTS_HERE, LANES), jnp.int32),
            pltpu.VMEM((ROBOTS, LANES), jnp.int32),
            dma((peers,)),
            dma((peers,)),
            dma((peers,)),
            dma((peers,)),
        ],
        compiler_params=pltpu.CompilerParams(collective_id=0, has_side_effects=True),
        name="spread",
    )(counts, centres, sphere_radius, adjacency)
    cost = pl.pallas_call(
        cross_kernel,
        out_shape=jax.ShapeDtypeStruct((ROBOT_DEVICES, ROBOTS_HERE, LANES), f32),
        in_specs=[IN_SMEM] + in_vmem(1),
        out_specs=in_vmem(1)[0],
        scratch_shapes=[
            pltpu.VMEM((ROBOTS, 4 * GROUPS, 8, LANES), f32),
            pltpu.VMEM((ROBOTS, 8, LANES), f32),
        ],
        name="cross",
    )(table, received)
    return pl.pallas_call(
        blend_kernel,
        out_shape=(
            jax.ShapeDtypeStruct((ROBOTS_HERE, COLUMNS), f32),
            jax.ShapeDtypeStruct((ROBOTS_HERE, 3, SPHERES, W), f32),
        ),
        in_specs=in_vmem(3),
        out_specs=tuple(in_vmem(2)),
        scratch_shapes=[
            pltpu.VMEM((ROBOT_DEVICES, ROBOTS_HERE, LANES), f32),
            pltpu.VMEM((2, ROBOTS_HERE, LANES), f32),
            pltpu.VMEM((Z, CHUNK + 1, LANES), f32),
            pltpu.VMEM((Z - 1, CHUNK + 1, LANES), f32),
            pltpu.VMEM((CHUNK + 1, LANES), f32),
            pltpu.VMEM((CHUNK + 1, LANES), f32),
            pltpu.VMEM((Z, CHUNK + 1, LANES), f32),
            dma((2, peers)),
            dma((2, Z - 1)),
            dma((2, 1)),
            dma((2, Z - 1)),
        ],
        compiler_params=pltpu.CompilerParams(collective_id=1, has_side_effects=True),
        name="blend",
    )(cost, self_cost, centres)


def solution(mesh):
    return jax.shard_map(
        local,
        mesh=mesh,
        in_specs=(P("robot", None, None, "seed"), P("robot", None), P("robot"), P("robot", None)),
        out_specs=(P("robot", "seed"), P("robot", None, None, None)),
        check_vma=False,
    )
```

```python
import functools
import math

import jax
import jax.numpy as jnp
from jax import lax
from jax.experimental import pallas as pl
from jax.experimental.pallas import tpu as pltpu
from jax.sharding import PartitionSpec as P

W = 32
SPHERES = 52
GROUPS = 7
FIRST_GROUPS = 4
ROBOTS_HERE = 2
ROBOT_DEVICES = 16
ROBOTS = ROBOTS_HERE * ROBOT_DEVICES
LANES = 128
COLUMNS = 256
PART = 16
ROWS = ROBOTS_HERE * GROUPS * 4
Z = 8
CHUNK = 11
COUNT_LANE = 32
ROOT = math.sqrt(math.log2(math.e))
FAR = 1.0e6
LIST = 256
STEP_ROWS = 8
ROW_IDS = ROBOTS * GROUPS
STEPS_PLACE = LIST
GROUPS_PLACE = LIST + 1
GRANT = 16 * 1024 * 1024
MESH = pl.DeviceIdType.MESH


def iota(axis, shape=(8, LANES)):
    return lax.broadcasted_iota(jnp.int32, shape, axis)


def pair_term(a, b):
    dx, dy, dz = a[0] - b[0], a[1] - b[1], a[2] - b[2]
    spread = a[3] + b[3]
    return jnp.exp2((dx * dx + dy * dy + dz * dz) / (-spread * spread))


def centre_rows(ref, robot, axis, group, half):
    first = min(8 * group, SPHERES - 8)
    row = ((axis * SPHERES + first) * 2 + half) * ROBOTS_HERE + robot
    value = ref[pl.ds(row, 8, stride=2 * ROBOTS_HERE), :]
    return value if first == 8 * group else pltpu.roll(value, 4, 0)


def spread_kernel(
    counts_ref,
    centres_ref,
    radius_ref,
    adjacency_ref,
    recv_ref,
    self_ref,
    table_ref,
    send,
    swept,
    note_send,
    note_recv,
    note,
    send_sem,
    recv_sem,
    note_send_sem,
    note_recv_sem,
):
    me = lax.axis_index("robot")
    seed = lax.axis_index("seed")
    peers = [lax.rem(me + step, ROBOT_DEVICES) for step in range(1, ROBOT_DEVICES)]

    barrier = pltpu.get_barrier_semaphore()
    for peer in peers:
        pl.semaphore_signal(barrier, inc=1, device_id=(peer, seed), device_id_type=MESH)

    sub, lane = iota(0), iota(1)
    part = lane // PART
    last_waypoint = lane % W == W - 1
    radius_lane = iota(1, (8, SPHERES))
    radius_sub = iota(0, (8, SPHERES))
    for robot in range(ROBOTS_HERE):
        count = counts_ref[robot]
        radius_row = jnp.broadcast_to(radius_ref[robot : robot + 1, :], (8, SPHERES))
        number = (me * ROBOTS_HERE + robot) * 64 + 1
        for group in range(GROUPS):
            radius = jnp.sum(
                jnp.where(radius_lane == radius_sub + 8 * group, radius_row, 0.0),
                axis=1,
                keepdims=True,
            )
            sphere = sub + 8 * group
            active = sphere < count
            far = FAR * (sphere + number).astype(jnp.float32)
            for half in range(2):
                out, square = [], None
                for axis in range(3):
                    here = centre_rows(centres_ref, robot, axis, group, half)
                    ahead = jnp.where(last_waypoint, here, pltpu.roll(here, LANES - 1, 1))
                    step = ahead - here
                    square = step * step if square is None else square + step * step
                    middle = (here + ahead) * (0.5 * ROOT)
                    out.append(jnp.where(active, middle, far if axis == 0 else 0.0))
                out.append(jnp.where(active, radius + 0.5 * jnp.sqrt(square + 1e-6), 1.0))
                for quantity in range(4):
                    value = out[quantity]
                    swept[half * ROBOTS_HERE + robot, quantity, 8 * group : 8 * group + 8, :] = value
                    value = pltpu.roll(value, 0, 1, stride=PART, stride_axis=0)
                    for bit in (1, 2, 4):
                        value = jnp.where(part & bit != 0, pltpu.roll(value, 8 - bit, 0), value)
                    row = (robot * GROUPS + group) * 4 + quantity
                    send[pl.ds(half * 8 * ROWS + row, 8, stride=ROWS), :] = value
        for half in range(2):
            for quantity in range(4):
                fill = FAR * (sub + 56 + number).astype(jnp.float32) if quantity == 0 else jnp.full((8, LANES), float(quantity == 3))
                swept[half * ROBOTS_HERE + robot, quantity, 56:64, :] = fill

    note_send[...] = jnp.zeros((ROBOTS_HERE, LANES), jnp.int32)
    note_send[:, 0:ROBOTS] = adjacency_ref[...]
    for robot in range(ROBOTS_HERE):
        note_send[robot : robot + 1, COUNT_LANE : COUNT_LANE + 1] = jnp.full((1, 1), counts_ref[robot], jnp.int32)

    pl.semaphore_wait(barrier, ROBOT_DEVICES - 1)

    def slot_of(device):
        return (device // 8) * 8 + lax.rem(8 - lax.rem(device, 8), 8)

    def rows_of(slot):
        return pl.ds(pl.multiple_of(slot * ROWS, 8), ROWS)

    notes, copies = [], []
    for number, peer in enumerate(peers):
        copy = pltpu.make_async_remote_copy(
            src_ref=note_send,
            dst_ref=note_recv.at[me],
            send_sem=note_send_sem.at[number],
            recv_sem=note_recv_sem.at[number],
            device_id=(peer, seed),
            device_id_type=MESH,
        )
        copy.start()
        notes.append(copy)
    for number, peer in enumerate(peers):
        copy = pltpu.make_async_remote_copy(
            src_ref=send.at[rows_of(slot_of(peer))],
            dst_ref=recv_ref.at[rows_of(me)],
            send_sem=send_sem.at[number],
            recv_sem=recv_sem.at[number],
            device_id=(peer, seed),
            device_id_type=MESH,
        )
        copy.start()
        copies.append(copy)
    note_recv[me] = note_send[...]
    recv_ref[rows_of(me), :] = send[rows_of(slot_of(me)), :]

    def self_pairs(index, carry):
        half, robot = index // ROBOTS_HERE, lax.rem(index, ROBOTS_HERE)
        sums = [jnp.zeros((8, LANES), jnp.float32) for _ in range(4)]
        turn = 0
        for group in range(GROUPS):
            first = [swept[index, q, 8 * group : 8 * group + 8, :] for q in range(4)]
            for apart in range(2, SPHERES - 8 * group):
                start = 8 * group + apart
                second = [swept[index, q, start : start + 8, :] for q in range(4)]
                sums[turn] = sums[turn] + pair_term(first, second)
                turn = (turn + 1) % 4
        total = jnp.sum((sums[0] + sums[1]) + (sums[2] + sums[3]), axis=0, keepdims=True)
        self_ref[pl.ds(index, 1), :] = total * (1.0 / (SPHERES * SPHERES))
        return carry

    lax.fori_loop(0, 2 * ROBOTS_HERE, self_pairs, 0)

    for copy in notes:
        copy.wait_recv()
    for device in range(ROBOT_DEVICES):
        note[ROBOTS_HERE * device : ROBOTS_HERE * (device + 1), :] = note_recv[device]
    shape = (ROBOTS, LANES)
    row, column = iota(0, shape), iota(1, shape)
    noted = note[...].astype(jnp.float32)
    link = jnp.where((column > row) & (column < ROBOTS) & (noted != 0.0), 1.0, 0.0)
    counts = jnp.sum(jnp.where(column == COUNT_LANE, noted, 0.0), axis=1, keepdims=True)
    groups = jnp.floor((counts + 7.0) * 0.125)
    groups_row = jnp.sum(jnp.where(row == column, groups, 0.0), axis=0, keepdims=True)
    length = link * groups_row
    before = (iota(0, (LANES, LANES)) < iota(1, (LANES, LANES))).astype(jnp.float32)
    start = jnp.dot(length, before, preferred_element_type=jnp.float32)
    end = start + length
    place = iota(1, (ROBOTS, LIST)).astype(jnp.float32)
    rows_listed = jnp.full((ROBOTS, LIST), float(ROW_IDS))
    for robot in range(1, ROBOTS):
        first, past = start[:, robot : robot + 1], end[:, robot : robot + 1]
        rows_listed = jnp.where(
            (place >= first) & (place < past), place + (float(GROUPS * robot) - first), rows_listed
        )
    steps = jnp.floor((jnp.sum(length, axis=1, keepdims=True) + (STEP_ROWS - 1.0)) * (1.0 / STEP_ROWS))
    table_ref[:, 0:LIST] = rows_listed.astype(jnp.int32)
    tail = jnp.where(column == 0, steps, groups)
    table_ref[:, LIST : LIST + LANES] = tail.astype(jnp.int32)
    filling = iota(0)
    recv_ref[ROBOT_DEVICES * ROWS : ROBOT_DEVICES * ROWS + 8, :] = jnp.where(
        filling == 0, -1000.0 * FAR, jnp.where(filling == 3, 1.0, 0.0)
    )

    for copy in copies:
        copy.wait_recv()
    for copy in notes + copies:
        copy.wait_send()


def cross_kernel(table, rows, cost_ref, turned, total):
    def prepare(index, carry):
        for part in range(4):
            robot = index * 4 + part
            for row in range(4 * GROUPS):
                line = rows[pl.ds(robot * (4 * GROUPS) + row, 1), :]
                turned[robot, row] = pltpu.roll(
                    jnp.broadcast_to(line, (8, LANES)), 0, 1, stride=PART, stride_axis=0
                )
            for group in range(GROUPS):
                total[robot * GROUPS + group] = jnp.zeros((8, LANES), jnp.float32)
        return carry

    lax.fori_loop(0, ROBOTS // 4, prepare, 0)

    def of_robot(first, carry):
        first_groups = table[first, GROUPS_PLACE]

        for known_groups in range(FIRST_GROUPS, GROUPS + 1):

            @pl.when(first_groups == known_groups)
            def _():
                def of_rows(step, own):
                    ids = [table[first, step * STEP_ROWS + n] for n in range(STEP_ROWS)]
                    olds = [total[row_id] for row_id in ids]
                    news = []
                    for row_id in ids:
                        b = [
                            jnp.broadcast_to(rows[pl.ds(row_id * 4 + q, 1), :], (8, LANES))
                            for q in range(4)
                        ]
                        found = None
                        for group in range(known_groups):
                            a = [turned[first, group * 4 + q] for q in range(4)]
                            term = pair_term(a, b)
                            found = term if found is None else found + term
                        news.append(found)
                    for row_id, old, new in zip(ids, olds, news):
                        total[row_id] = old + new
                    while len(news) > 1:
                        news = [m + n for m, n in zip(news[0::2], news[1::2])]
                    return own + news[0]

                own = lax.fori_loop(
                    0, table[first, STEPS_PLACE], of_rows, jnp.zeros((8, LANES), jnp.float32)
                )
                total[first * GROUPS] = total[first * GROUPS] + own

        return carry

    lax.fori_loop(0, ROBOTS, of_robot, 0)

    for robot in range(ROBOTS):
        found = total[robot * GROUPS]
        for group in range(1, GROUPS):
            found = found + total[robot * GROUPS + group]
        turned[robot, 0] = found
    cost = jnp.sum(turned[:, 0], axis=1)
    for shift in (64, 32, 16):
        cost = cost + pltpu.roll(cost, shift, 1)
    cost = cost * (1.0 / (SPHERES * SPHERES))
    for device in range(ROBOT_DEVICES):
        cost_ref[device] = cost[ROBOTS_HERE * device : ROBOTS_HERE * (device + 1), :]


def blend_kernel(
    cost_ref,
    self_ref,
    centres_ref,
    robot_cost_ref,
    gathered,
    cost_recv,
    weight,
    packed,
    parts,
    mine,
    other,
    cost_sems,
    part_sems,
    pair_sems,
    gather_sems,
):
    me = lax.axis_index("robot")
    seed = lax.axis_index("seed")
    x, z = seed // Z, lax.rem(seed, Z)
    peers = [lax.rem(me + step, ROBOT_DEVICES) for step in range(1, ROBOT_DEVICES)]
    z_peers = [lax.rem(z + step, Z) for step in range(1, Z)]
    opposite = (1 - x) * Z + z

    barrier = pltpu.get_barrier_semaphore()
    for peer in peers:
        pl.semaphore_signal(barrier, inc=1, device_id=(peer, seed), device_id_type=MESH)
    for peer in z_peers:
        pl.semaphore_signal(barrier, inc=1, device_id=(me, x * Z + peer), device_id_type=MESH)
    pl.semaphore_signal(barrier, inc=1, device_id=(me, opposite), device_id_type=MESH)
    pl.semaphore_wait(barrier, ROBOT_DEVICES - 1 + Z)

    def start(src, dst, sems, number, device):
        copy = pltpu.make_async_remote_copy(
            src_ref=src,
            dst_ref=dst,
            send_sem=sems.at[0, number],
            recv_sem=sems.at[1, number],
            device_id=device,
            device_id_type=MESH,
        )
        copy.start()
        return copy

    copies = [
        start(cost_ref.at[peer], cost_recv.at[me], cost_sems, number, (peer, seed))
        for number, peer in enumerate(peers)
    ]
    cost_recv[me] = cost_ref[me]
    for copy in copies:
        copy.wait_recv()
    sent = copies

    lane = iota(1, (ROBOTS_HERE, LANES))
    part = lane // PART
    for half in range(2):
        cost = self_ref[half * ROBOTS_HERE : (half + 1) * ROBOTS_HERE, :]
        for k in range(8):
            cost = cost + jnp.where(part == k, cost_recv[half * 8 + k], 0.0)
        robot_cost_ref[:, half * LANES : (half + 1) * LANES] = cost
        for bit in (1, 2, 4, 8, 16):
            cost = cost + jnp.where(
                lane & bit != 0, pltpu.roll(cost, bit, 1), pltpu.roll(cost, LANES - bit, 1)
            )
        weight[half] = 1.0 / (1.0 + cost)
    sums = weight[0] + weight[1]
    sums = sums + pltpu.roll(sums, 64, 1)
    sums = sums + pltpu.roll(sums, 32, 1)
    line = iota(1, (1, LANES))
    total_row = jnp.where(line < 64, sums[0:1, :], sums[1:2, :])

    quarter = iota(1) // W
    units = [[], []]
    for robot in range(ROBOTS_HERE):
        weights = [
            jnp.broadcast_to(weight[half, robot : robot + 1, :], (8, LANES)) for half in range(2)
        ]
        for axis in range(3):
            for group in range(GROUPS):
                value = (
                    centre_rows(centres_ref, robot, axis, group, 0) * weights[0]
                    + centre_rows(centres_ref, robot, axis, group, 1) * weights[1]
                )
                value = value + pltpu.roll(value, 64, 1)
                units[robot].append(value + pltpu.roll(value, 32, 1))
        units[robot].append(jnp.zeros((8, LANES), jnp.float32))
    for v in range(CHUNK):
        value = jnp.where(
            quarter < 2,
            jnp.where(quarter == 0, units[0][v], units[0][CHUNK + v]),
            jnp.where(quarter == 2, units[1][v], units[1][CHUNK + v]),
        )
        done = 0
        while done < 8:
            chunk, row = divmod(8 * v + done, CHUNK)
            length = min(8 - done, CHUNK - row)
            packed[chunk, row : row + length, :] = value[done : done + length, :]
            done += length
    for chunk in range(Z):
        packed[chunk, CHUNK : CHUNK + 1, :] = total_row

    copies = [
        start(packed.at[peer], parts.at[number], part_sems, number, (me, x * Z + peer))
        for number, peer in enumerate(z_peers)
    ]
    found = packed[z]
    for number, copy in enumerate(copies):
        copy.wait_recv()
        found = found + parts[number]
    sent = sent + copies

    mine[...] = found
    copy = start(mine, other, pair_sems, 0, (me, opposite))
    copy.wait_recv()
    sent = sent + [copy]
    found = mine[...] + other[...]
    gathered[z] = found / found[CHUNK : CHUNK + 1, :]

    copies = [
        start(gathered.at[z], gathered.at[z], gather_sems, number, (me, x * Z + peer))
        for number, peer in enumerate(z_peers)
    ]
    for copy in copies:
        copy.wait_recv()
    sent = sent + copies

    for copy in sent:
        copy.wait_send()


def finish_kernel(cost_in, gathered, cost_out, blended, lines):
    cost_out[...] = cost_in[...]
    for chunk in range(Z):
        lines[CHUNK * chunk : CHUNK * (chunk + 1), :] = gathered[chunk, 0:CHUNK, :]
    turned = lines[...].T
    for robot in range(ROBOTS_HERE):
        for axis in range(3):
            for quarter in range(2):
                low = max(axis * GROUPS, quarter * CHUNK)
                high = min((axis + 1) * GROUPS, (quarter + 1) * CHUNK)
                if low < high:
                    source = (robot * 2 + quarter) * W
                    lane = 8 * (low - quarter * CHUNK)
                    first = 8 * (low - axis * GROUPS)
                    width = min(8 * (high - low), SPHERES - first)
                    blended[robot, axis, :, first : first + width] = turned[
                        source : source + W, lane : lane + width
                    ]


def in_vmem(count):
    return [pl.BlockSpec(memory_space=pltpu.VMEM)] * count


IN_SMEM = pl.BlockSpec(memory_space=pltpu.SMEM)


def local(centres, sphere_radius, counts, adjacency):
    dma = pltpu.SemaphoreType.DMA
    f32 = jnp.float32
    peers = ROBOT_DEVICES - 1
    rows = centres.transpose(1, 2, 0, 3).reshape(3 * SPHERES, ROBOTS_HERE, 2, LANES)
    rows = rows.transpose(0, 2, 1, 3).reshape(3 * SPHERES * 2 * ROBOTS_HERE, LANES)
    received, self_cost, table = pl.pallas_call(
        spread_kernel,
        out_shape=(
            jax.ShapeDtypeStruct((ROBOT_DEVICES * ROWS + 8, LANES), f32),
            jax.ShapeDtypeStruct((2 * ROBOTS_HERE, LANES), f32),
            jax.ShapeDtypeStruct((ROBOTS, LIST + LANES), jnp.int32),
        ),
        in_specs=[IN_SMEM] + in_vmem(3),
        out_specs=tuple(in_vmem(3)),
        scratch_shapes=[
            pltpu.VMEM((ROBOT_DEVICES * ROWS, LANES), f32),
            pltpu.VMEM((2 * ROBOTS_HERE, 4, 64, LANES), f32),
            pltpu.VMEM((ROBOTS_HERE, LANES), jnp.int32),
            pltpu.VMEM((ROBOT_DEVICES, ROBOTS_HERE, LANES), jnp.int32),
            pltpu.VMEM((ROBOTS, LANES), jnp.int32),
            dma((peers,)),
            dma((peers,)),
            dma((peers,)),
            dma((peers,)),
        ],
        compiler_params=pltpu.CompilerParams(
            collective_id=0, has_side_effects=True, vmem_limit_bytes=GRANT
        ),
        name="spread",
    )(counts, rows, sphere_radius, adjacency)
    cost = pl.pallas_call(
        cross_kernel,
        out_shape=jax.ShapeDtypeStruct((ROBOT_DEVICES, ROBOTS_HERE, LANES), f32),
        in_specs=[IN_SMEM] + in_vmem(1),
        out_specs=in_vmem(1)[0],
        scratch_shapes=[
            pltpu.VMEM((ROBOTS, 4 * GROUPS, 8, LANES), f32),
            pltpu.VMEM((ROW_IDS + 1, 8, LANES), f32),
        ],
        compiler_params=pltpu.CompilerParams(vmem_limit_bytes=GRANT),
        name="cross",
    )(table, received)
    robot_cost, gathered = pl.pallas_call(
        blend_kernel,
        out_shape=(
            jax.ShapeDtypeStruct((ROBOTS_HERE, COLUMNS), f32),
            jax.ShapeDtypeStruct((Z, CHUNK + 1, LANES), f32),
        ),
        in_specs=in_vmem(3),
        out_specs=tuple(in_vmem(2)),
        scratch_shapes=[
            pltpu.VMEM((ROBOT_DEVICES, ROBOTS_HERE, LANES), f32),
            pltpu.VMEM((2, ROBOTS_HERE, LANES), f32),
            pltpu.VMEM((Z, CHUNK + 1, LANES), f32),
            pltpu.VMEM((Z - 1, CHUNK + 1, LANES), f32),
            pltpu.VMEM((CHUNK + 1, LANES), f32),
            pltpu.VMEM((CHUNK + 1, LANES), f32),
            dma((2, peers)),
            dma((2, Z - 1)),
            dma((2, 1)),
            dma((2, Z - 1)),
        ],
        compiler_params=pltpu.CompilerParams(
            collective_id=1, has_side_effects=True, vmem_limit_bytes=GRANT
        ),
        name="blend",
    )(cost, self_cost, rows)
    robot_cost, blended = pl.pallas_call(
        finish_kernel,
        out_shape=(
            jax.ShapeDtypeStruct((ROBOTS_HERE, COLUMNS), f32),
            jax.ShapeDtypeStruct((ROBOTS_HERE, 3, W, SPHERES), f32),
        ),
        in_specs=in_vmem(2),
        out_specs=tuple(in_vmem(2)),
        scratch_shapes=[pltpu.VMEM((LANES, LANES), f32)],
        compiler_params=pltpu.CompilerParams(vmem_limit_bytes=GRANT),
        name="finish",
    )(robot_cost, gathered)
    return robot_cost, blended.transpose(0, 1, 3, 2)


def solution(mesh):
    return jax.shard_map(
        local,
        mesh=mesh,
        in_specs=(P("robot", None, None, "seed"), P("robot", None), P("robot"), P("robot", None)),
        out_specs=(P("robot", "seed"), P("robot", None, None, None)),
        check_vma=False,
    )
```

```python
import functools
import math

import jax
import jax.numpy as jnp
from jax import lax
from jax.experimental import pallas as pl
from jax.experimental.pallas import tpu as pltpu
from jax.sharding import PartitionSpec as P

W = 32
SPHERES = 52
GROUPS = 7
FIRST_GROUPS = 4
ROBOTS_HERE = 2
ROBOT_DEVICES = 16
ROBOTS = ROBOTS_HERE * ROBOT_DEVICES
LANES = 128
COLUMNS = 256
PART = 16
ROWS = ROBOTS_HERE * GROUPS * 4
Z = 8
CHUNK = 11
COUNT_LANE = 32
ROOT = math.sqrt(math.log2(math.e))
FAR = 1.0e6
STEP_ROWS = 8
ROW_IDS = ROBOTS * GROUPS
WORDS = 56
STEPS_WORD = 56
ENTRY = 64
ORDER = ROBOTS * ENTRY
CASE_STEPS = ORDER + 32
CASE_START = ORDER + 40
TABLE_ROWS = 24
EARLY_GROUPS = 3
GRANT = 16 * 1024 * 1024
MESH = pl.DeviceIdType.MESH


def iota(axis, shape=(8, LANES)):
    return lax.broadcasted_iota(jnp.int32, shape, axis)


def pair_argument(a, b):
    dx, dy, dz = a[0] - b[0], a[1] - b[1], a[2] - b[2]
    spread = a[3] + b[3]
    return (dx * dx + dy * dy + dz * dz) / (-spread * spread)


def pair_term(a, b):
    return jnp.exp2(pair_argument(a, b))


def centre_rows(ref, robot, axis, group, half):
    first = min(8 * group, SPHERES - 8)
    row = ((axis * SPHERES + first) * 2 + half) * ROBOTS_HERE + robot
    value = ref[pl.ds(row, 8, stride=2 * ROBOTS_HERE), :]
    return value if first == 8 * group else pltpu.roll(value, 4, 0)


def spread_kernel(
    counts_hbm,
    centres_hbm,
    radius_hbm,
    adjacency_hbm,
    recv_ref,
    turned_ref,
    self_ref,
    table_ref,
    counts_ref,
    centres_ref,
    radius_ref,
    adjacency_ref,
    send,
    swept,
    note_send,
    note_recv,
    note,
    load_sem,
    send_sem,
    recv_sem,
    note_send_sem,
    note_recv_sem,
):
    me = lax.axis_index("robot")
    seed = lax.axis_index("seed")
    peers = [lax.rem(me + step, ROBOT_DEVICES) for step in range(1, ROBOT_DEVICES)]

    barrier = pltpu.get_barrier_semaphore()
    for peer in peers:
        pl.semaphore_signal(barrier, inc=1, device_id=(peer, seed), device_id_type=MESH)

    loads = [
        pltpu.make_async_copy(counts_hbm, counts_ref, load_sem.at[0]),
        pltpu.make_async_copy(radius_hbm, radius_ref, load_sem.at[1]),
        pltpu.make_async_copy(adjacency_hbm, adjacency_ref, load_sem.at[2]),
    ]
    per_axis, early = 4 * SPHERES, 4 * 8 * EARLY_GROUPS
    for axis in range(3):
        at = pl.ds(axis * per_axis, early)
        loads.append(pltpu.make_async_copy(centres_hbm.at[at], centres_ref.at[at], load_sem.at[3 + axis]))
    for axis in range(3):
        at = pl.ds(axis * per_axis + early, per_axis - early)
        loads.append(pltpu.make_async_copy(centres_hbm.at[at], centres_ref.at[at], load_sem.at[6 + axis]))
    for load in loads:
        load.start()
    for load in loads[:6]:
        load.wait()

    sub, lane = iota(0), iota(1)
    part = lane // PART
    last_waypoint = lane % W == W - 1
    radius_lane = iota(1, (8, SPHERES))
    radius_sub = iota(0, (8, SPHERES))
    note_send[...] = jnp.zeros((ROBOTS_HERE, LANES), jnp.int32)
    note_send[:, 0:ROBOTS] = adjacency_ref[...]
    for robot in range(ROBOTS_HERE):
        note_send[robot : robot + 1, COUNT_LANE : COUNT_LANE + 1] = jnp.full((1, 1), counts_ref[robot], jnp.int32)
    for group in range(GROUPS):
        if group == EARLY_GROUPS:
            for load in loads[6:]:
                load.wait()
        for robot in range(ROBOTS_HERE):
            count = counts_ref[robot]
            radius_row = jnp.broadcast_to(radius_ref[robot : robot + 1, :], (8, SPHERES))
            number = (me * ROBOTS_HERE + robot) * 64 + 1
            radius = jnp.sum(
                jnp.where(radius_lane == radius_sub + 8 * group, radius_row, 0.0),
                axis=1,
                keepdims=True,
            )
            sphere = sub + 8 * group
            active = sphere < count
            far = FAR * (sphere + number).astype(jnp.float32)
            for half in range(2):
                out, square = [], None
                for axis in range(3):
                    here = centre_rows(centres_ref, robot, axis, group, half)
                    ahead = jnp.where(last_waypoint, here, pltpu.roll(here, LANES - 1, 1))
                    step = ahead - here
                    square = step * step if square is None else square + step * step
                    middle = (here + ahead) * (0.5 * ROOT)
                    out.append(jnp.where(active, middle, far if axis == 0 else 0.0))
                out.append(jnp.where(active, radius + 0.5 * jnp.sqrt(square + 1e-6), 1.0))
                for quantity in range(4):
                    value = out[quantity]
                    swept[half * ROBOTS_HERE + robot, quantity, 8 * group : 8 * group + 8, :] = value
                    value = pltpu.roll(value, 0, 1, stride=PART, stride_axis=0)
                    for bit in (1, 2, 4):
                        value = jnp.where(part & bit != 0, pltpu.roll(value, 8 - bit, 0), value)
                    row = (robot * GROUPS + group) * 4 + quantity
                    send[pl.ds(half * 8 * ROWS + row, 8, stride=ROWS), :] = value

    pl.semaphore_wait(barrier, ROBOT_DEVICES - 1)

    def slot_of(device):
        return (device // 8) * 8 + lax.rem(8 - lax.rem(device, 8), 8)

    def rows_of(slot):
        return pl.ds(pl.multiple_of(slot * ROWS, 8), ROWS)

    notes, copies = [], []
    for number, peer in enumerate(peers):
        copy = pltpu.make_async_remote_copy(
            src_ref=note_send,
            dst_ref=note_recv.at[me],
            send_sem=note_send_sem.at[number],
            recv_sem=note_recv_sem.at[number],
            device_id=(peer, seed),
            device_id_type=MESH,
        )
        copy.start()
        notes.append(copy)
        copy = pltpu.make_async_remote_copy(
            src_ref=send.at[rows_of(slot_of(peer))],
            dst_ref=recv_ref.at[rows_of(me)],
            send_sem=send_sem.at[number],
            recv_sem=recv_sem.at[number],
            device_id=(peer, seed),
            device_id_type=MESH,
        )
        copy.start()
        copies.append(copy)
    note_recv[me] = note_send[...]
    recv_ref[rows_of(me), :] = send[rows_of(slot_of(me)), :]

    def turn_rows(device):
        def turn_group(index, carry):
            row = pl.multiple_of(device * ROWS + index * 8, 8)
            for n in range(8):
                line = jnp.broadcast_to(recv_ref[pl.ds(row + n, 1), :], (8, LANES))
                turned_ref[row + n] = pltpu.roll(line, 0, 1, stride=PART, stride_axis=0)
            return carry

        lax.fori_loop(0, ROWS // 8, turn_group, 0)

    turn_rows(me)
    for index in range(2 * ROBOTS_HERE):
        robot = index % ROBOTS_HERE
        number = (me * ROBOTS_HERE + robot) * 64 + 1
        for quantity in range(4):
            fill = jnp.full((8, LANES), float(quantity == 3))
            if quantity == 0:
                fill = FAR * (sub + 8 * GROUPS + number).astype(jnp.float32)
            swept[index, quantity, 8 * GROUPS : 8 * GROUPS + 8, :] = fill

    def self_pairs(index, carry):
        sums = [jnp.zeros((8, LANES), jnp.float32) for _ in range(4)]
        turn = 0
        for group in range(GROUPS):
            first = [swept[index, q, 8 * group : 8 * group + 8, :] for q in range(4)]
            for apart in range(2, SPHERES - 8 * group):
                start = 8 * group + apart
                second = [swept[index, q, start : start + 8, :] for q in range(4)]
                sums[turn] = sums[turn] + pair_term(first, second)
                turn = (turn + 1) % 4
        total = jnp.sum((sums[0] + sums[1]) + (sums[2] + sums[3]), axis=0, keepdims=True)
        self_ref[pl.ds(index, 1), :] = total * (1.0 / (SPHERES * SPHERES))
        return carry

    lax.fori_loop(0, 2 * ROBOTS_HERE, self_pairs, 0)

    for copy in notes:
        copy.wait_recv()
    for device in range(ROBOT_DEVICES):
        note[ROBOTS_HERE * device : ROBOTS_HERE * (device + 1), :] = note_recv[device]
    shape = (ROBOTS, LANES)
    row, column = iota(0, shape), iota(1, shape)
    row_number = row.astype(jnp.float32)
    noted = note[...].astype(jnp.float32)
    link = jnp.where((column > row) & (column < ROBOTS) & (noted != 0.0), 1.0, 0.0)
    counts = jnp.sum(jnp.where(column == COUNT_LANE, noted, 0.0), axis=1, keepdims=True)
    groups = jnp.floor((counts + 7.0) * 0.125)

    def as_row(value):
        return jnp.sum(jnp.where(row == column, value, 0.0), axis=0, keepdims=True)

    length = link * as_row(groups)
    before = (iota(0, (LANES, LANES)) < iota(1, (LANES, LANES))).astype(jnp.float32)
    start = jnp.dot(length, before, preferred_element_type=jnp.float32)
    end = start + length
    words = jnp.zeros(shape, jnp.int32)
    for byte in range(4):
        place = (column * 4 + byte).astype(jnp.float32)
        listed = jnp.full(shape, float(ROW_IDS))
        for robot in range(1, ROBOTS):
            first, past = start[:, robot : robot + 1], end[:, robot : robot + 1]
            listed = jnp.where(
                (place >= first) & (place < past), place + (float(GROUPS * robot) - first), listed
            )
        words = words | (listed.astype(jnp.int32) << (8 * byte))
    steps = jnp.floor((jnp.sum(length, axis=1, keepdims=True) + (STEP_ROWS - 1.0)) * (1.0 / STEP_ROWS))
    words = jnp.where(column == STEPS_WORD, steps.astype(jnp.int32), words)
    note[...] = jnp.where(column < ENTRY, words, 0)
    table_ref[0:16, :] = note[pl.ds(0, 16, stride=2), :] + pltpu.roll(
        note[pl.ds(1, 16, stride=2), :], ENTRY, 1
    )
    busy = jnp.where(steps > 0.0, 1.0, 0.0)
    key = groups * 32.0 + row_number
    key_row, busy_row = as_row(key), as_row(busy)
    rank = jnp.sum(jnp.where(key_row < key, busy_row, 0.0), axis=1, keepdims=True)
    lane_number = column.astype(jnp.float32)
    last = jnp.sum(
        jnp.where((rank == lane_number) & (busy > 0.0), row_number, 0.0), axis=0, keepdims=True
    )
    line = iota(1, (1, LANES))
    for case in range(FIRST_GROUPS, GROUPS + 1):
        of_case = jnp.where(row == column, jnp.where(groups == float(case), steps, 0.0), 0.0)
        earlier = jnp.where(row == column, jnp.where(groups < float(case), busy, 0.0), 0.0)
        last = jnp.where(line == CASE_STEPS - ORDER + case - FIRST_GROUPS, jnp.sum(of_case), last)
        last = jnp.where(line == CASE_START - ORDER + case - FIRST_GROUPS, jnp.sum(earlier), last)
    table_ref[16:24, :] = jnp.broadcast_to(last, (8, LANES)).astype(jnp.int32)
    recv_ref[ROBOT_DEVICES * ROWS : ROBOT_DEVICES * ROWS + 8, :] = jnp.where(
        sub == 0, -1000.0 * FAR, jnp.where(sub == 3, 1.0, 0.0)
    )

    for number, copy in enumerate(copies):
        copy.wait_recv()
        turn_rows(lax.rem(me + ROBOT_DEVICES - 1 - number, ROBOT_DEVICES))
    for copy in notes + copies:
        copy.wait_send()


def cross_kernel(table, rows, turned, total, arguments):
    zero = jnp.zeros((8, LANES), jnp.float32)
    for slot in range(STEP_ROWS * GROUPS):
        arguments[slot] = zero

    def clear(index, carry):
        for n in range(15):
            total[index * 15 + n] = zero
        return carry

    lax.fori_loop(0, (ROW_IDS + 1) // 15, clear, 0)

    def row_ids(words):
        return [lax.shift_right_logical(word, 8 * n) & 255 for word in words for n in range(4)]

    def sum_terms(groups, n):
        terms = [jnp.exp2(arguments[n * groups + group]) for group in range(groups)]
        while len(terms) > 1:
            terms = [p + q for p, q in zip(terms[0::2], terms[1::2])] + terms[len(terms) & ~1 :]
        return terms[0]

    def add_up(ids, news):
        own = news
        while len(own) > 1:
            own = [p + q for p, q in zip(own[0::2], own[1::2])]
        olds = [total[row_id] for row_id in ids]
        for row_id, old, new in zip(ids, olds, news + own):
            total[row_id] = old + new

    def entry_of(turn, step):
        robot = jnp.minimum(table[ORDER + turn], ROBOTS - 1)
        at = robot * ENTRY + 2 * step
        return robot, table[at], table[at + 1]

    for groups in range(FIRST_GROUPS, GROUPS + 1):

        def one_step(_, state, groups=groups):
            turn, step, robot, first, second, *past_ids = state
            ids = row_ids((first, second)) + [robot * GROUPS]
            a_row = robot * (4 * GROUPS)
            news = []
            for n in range(STEP_ROWS):
                news.append(sum_terms(groups, n))
                b = [
                    jnp.broadcast_to(rows[pl.ds(ids[n] * 4 + q, 1), :], (8, LANES))
                    for q in range(4)
                ]
                for group in range(groups):
                    a = [turned[a_row + (group * 4 + q)] for q in range(4)]
                    arguments[n * groups + group] = pair_argument(a, b)
            add_up(past_ids, news)
            step = step + 1
            over = (step >= table[robot * ENTRY + STEPS_WORD]).astype(jnp.int32)
            turn, step = turn + over, step * (1 - over)
            return turn, step, *entry_of(turn, step), *ids

        case = groups - FIRST_GROUPS
        turn = table[CASE_START + case]
        nothing = [jnp.int32(ROW_IDS)] * (STEP_ROWS + 1)
        state = (turn, jnp.int32(0), *entry_of(turn, 0), *nothing)
        state = lax.fori_loop(0, table[CASE_STEPS + case], one_step, state)
        add_up(list(state[5:]), [sum_terms(groups, n) for n in range(STEP_ROWS)])


def blend_kernel(
    total,
    self_ref,
    centres_ref,
    robot_cost_ref,
    gathered,
    sums,
    cost_ref,
    cost_recv,
    weight,
    packed,
    parts,
    mine,
    other,
    cost_sems,
    part_sems,
    pair_sems,
    gather_sems,
):
    me = lax.axis_index("robot")
    seed = lax.axis_index("seed")
    x, z = seed // Z, lax.rem(seed, Z)
    peers = [lax.rem(me + step, ROBOT_DEVICES) for step in range(1, ROBOT_DEVICES)]
    z_peers = [lax.rem(z + step, Z) for step in range(1, Z)]
    opposite = (1 - x) * Z + z

    barrier = pltpu.get_barrier_semaphore()
    for peer in peers:
        pl.semaphore_signal(barrier, inc=1, device_id=(peer, seed), device_id_type=MESH)
    for peer in z_peers:
        pl.semaphore_signal(barrier, inc=1, device_id=(me, x * Z + peer), device_id_type=MESH)
    pl.semaphore_signal(barrier, inc=1, device_id=(me, opposite), device_id_type=MESH)

    for robot in range(ROBOTS):
        found = total[robot * GROUPS]
        for group in range(1, GROUPS):
            found = found + total[robot * GROUPS + group]
        sums[robot] = found
    cost = jnp.sum(sums[...], axis=1)
    for shift in (64, 32, 16):
        cost = cost + pltpu.roll(cost, shift, 1)
    cost = cost * (1.0 / (SPHERES * SPHERES))
    for device in range(ROBOT_DEVICES):
        cost_ref[device] = cost[ROBOTS_HERE * device : ROBOTS_HERE * (device + 1), :]

    pl.semaphore_wait(barrier, ROBOT_DEVICES - 1 + Z)

    def start(src, dst, sems, number, device):
        copy = pltpu.make_async_remote_copy(
            src_ref=src,
            dst_ref=dst,
            send_sem=sems.at[0, number],
            recv_sem=sems.at[1, number],
            device_id=device,
            device_id_type=MESH,
        )
        copy.start()
        return copy

    copies = [
        start(cost_ref.at[peer], cost_recv.at[me], cost_sems, number, (peer, seed))
        for number, peer in enumerate(peers)
    ]
    cost_recv[me] = cost_ref[me]
    for copy in copies:
        copy.wait_recv()
    sent = copies

    lane = iota(1, (ROBOTS_HERE, LANES))
    part = lane // PART
    for half in range(2):
        cost = self_ref[half * ROBOTS_HERE : (half + 1) * ROBOTS_HERE, :]
        for k in range(8):
            cost = cost + jnp.where(part == k, cost_recv[half * 8 + k], 0.0)
        robot_cost_ref[:, half * LANES : (half + 1) * LANES] = cost
        for bit in (1, 2, 4, 8, 16):
            cost = cost + jnp.where(
                lane & bit != 0, pltpu.roll(cost, bit, 1), pltpu.roll(cost, LANES - bit, 1)
            )
        weight[half] = 1.0 / (1.0 + cost)
    weights = weight[0] + weight[1]
    weights = weights + pltpu.roll(weights, 64, 1)
    weights = weights + pltpu.roll(weights, 32, 1)
    line = iota(1, (1, LANES))
    total_row = jnp.where(line < 64, weights[0:1, :], weights[1:2, :])

    quarter = iota(1) // W
    units = [[], []]
    for robot in range(ROBOTS_HERE):
        weights = [
            jnp.broadcast_to(weight[half, robot : robot + 1, :], (8, LANES)) for half in range(2)
        ]
        for axis in range(3):
            for group in range(GROUPS):
                value = (
                    centre_rows(centres_ref, robot, axis, group, 0) * weights[0]
                    + centre_rows(centres_ref, robot, axis, group, 1) * weights[1]
                )
                value = value + pltpu.roll(value, 64, 1)
                units[robot].append(value + pltpu.roll(value, 32, 1))
        units[robot].append(jnp.zeros((8, LANES), jnp.float32))
    for v in range(CHUNK):
        value = jnp.where(
            quarter < 2,
            jnp.where(quarter == 0, units[0][v], units[0][CHUNK + v]),
            jnp.where(quarter == 2, units[1][v], units[1][CHUNK + v]),
        )
        done = 0
        while done < 8:
            chunk, row = divmod(8 * v + done, CHUNK)
            length = min(8 - done, CHUNK - row)
            packed[chunk, row : row + length, :] = value[done : done + length, :]
            done += length
    for chunk in range(Z):
        packed[chunk, CHUNK : CHUNK + 1, :] = total_row

    copies = [
        start(packed.at[peer], parts.at[number], part_sems, number, (me, x * Z + peer))
        for number, peer in enumerate(z_peers)
    ]
    found = packed[z]
    for number, copy in enumerate(copies):
        copy.wait_recv()
        found = found + parts[number]
    sent = sent + copies

    mine[...] = found
    copy = start(mine, other, pair_sems, 0, (me, opposite))
    copy.wait_recv()
    sent = sent + [copy]
    found = mine[...] + other[...]
    gathered[z] = found / found[CHUNK : CHUNK + 1, :]

    copies = [
        start(gathered.at[z], gathered.at[z], gather_sems, number, (me, x * Z + peer))
        for number, peer in enumerate(z_peers)
    ]
    for copy in copies:
        copy.wait_recv()
    sent = sent + copies

    for copy in sent:
        copy.wait_send()


def finish_kernel(cost_in, gathered, cost_out, blended, lines):
    cost_out[...] = cost_in[...]
    for chunk in range(Z):
        lines[CHUNK * chunk : CHUNK * (chunk + 1), :] = gathered[chunk, 0:CHUNK, :]
    turned = lines[...].T
    for robot in range(ROBOTS_HERE):
        for axis in range(3):
            for quarter in range(2):
                low = max(axis * GROUPS, quarter * CHUNK)
                high = min((axis + 1) * GROUPS, (quarter + 1) * CHUNK)
                if low < high:
                    source = (robot * 2 + quarter) * W
                    lane = 8 * (low - quarter * CHUNK)
                    first = 8 * (low - axis * GROUPS)
                    width = min(8 * (high - low), SPHERES - first)
                    blended[robot, axis, :, first : first + width] = turned[
                        source : source + W, lane : lane + width
                    ]


def in_vmem(count):
    return [pl.BlockSpec(memory_space=pltpu.VMEM)] * count


IN_SMEM = pl.BlockSpec(memory_space=pltpu.SMEM)


def local(centres, sphere_radius, counts, adjacency):
    dma = pltpu.SemaphoreType.DMA
    f32 = jnp.float32
    peers = ROBOT_DEVICES - 1
    rows = centres.transpose(1, 2, 0, 3).reshape(3 * SPHERES, ROBOTS_HERE, 2, LANES)
    rows = rows.transpose(0, 2, 1, 3).reshape(3 * SPHERES * 2 * ROBOTS_HERE, LANES)
    in_hbm = pl.BlockSpec(memory_space=pltpu.HBM)
    received, turned, self_cost, table = pl.pallas_call(
        spread_kernel,
        out_shape=(
            jax.ShapeDtypeStruct((ROBOT_DEVICES * ROWS + 8, LANES), f32),
            jax.ShapeDtypeStruct((ROBOT_DEVICES * ROWS, 8, LANES), f32),
            jax.ShapeDtypeStruct((2 * ROBOTS_HERE, LANES), f32),
            jax.ShapeDtypeStruct((TABLE_ROWS, LANES), jnp.int32),
        ),
        in_specs=[in_hbm] * 4,
        out_specs=tuple(in_vmem(4)),
        scratch_shapes=[
            pltpu.SMEM((ROBOTS_HERE,), jnp.int32),
            pltpu.VMEM(rows.shape, f32),
            pltpu.VMEM((ROBOTS_HERE, SPHERES), f32),
            pltpu.VMEM((ROBOTS_HERE, ROBOTS), jnp.int32),
            pltpu.VMEM((ROBOT_DEVICES * ROWS, LANES), f32),
            pltpu.VMEM((2 * ROBOTS_HERE, 4, 64, LANES), f32),
            pltpu.VMEM((ROBOTS_HERE, LANES), jnp.int32),
            pltpu.VMEM((ROBOT_DEVICES, ROBOTS_HERE, LANES), jnp.int32),
            pltpu.VMEM((ROBOTS, LANES), jnp.int32),
            dma((9,)),
            dma((peers,)),
            dma((peers,)),
            dma((peers,)),
            dma((peers,)),
        ],
        compiler_params=pltpu.CompilerParams(
            collective_id=0, has_side_effects=True, vmem_limit_bytes=GRANT
        ),
        name="spread",
    )(*[pltpu.with_memory_space_constraint(v, pltpu.HBM) for v in (counts, rows, sphere_radius, adjacency)])
    total = pl.pallas_call(
        cross_kernel,
        out_shape=jax.ShapeDtypeStruct((ROW_IDS + 1, 8, LANES), f32),
        in_specs=[IN_SMEM] + in_vmem(2),
        out_specs=in_vmem(1)[0],
        scratch_shapes=[pltpu.VMEM((STEP_ROWS * GROUPS, 8, LANES), f32)],
        compiler_params=pltpu.CompilerParams(vmem_limit_bytes=GRANT),
        name="cross",
    )(table.reshape(TABLE_ROWS * LANES), received, turned)
    robot_cost, gathered = pl.pallas_call(
        blend_kernel,
        out_shape=(
            jax.ShapeDtypeStruct((ROBOTS_HERE, COLUMNS), f32),
            jax.ShapeDtypeStruct((Z, CHUNK + 1, LANES), f32),
        ),
        in_specs=in_vmem(3),
        out_specs=tuple(in_vmem(2)),
        scratch_shapes=[
            pltpu.VMEM((ROBOTS, 8, LANES), f32),
            pltpu.VMEM((ROBOT_DEVICES, ROBOTS_HERE, LANES), f32),
            pltpu.VMEM((ROBOT_DEVICES, ROBOTS_HERE, LANES), f32),
            pltpu.VMEM((2, ROBOTS_HERE, LANES), f32),
            pltpu.VMEM((Z, CHUNK + 1, LANES), f32),
            pltpu.VMEM((Z - 1, CHUNK + 1, LANES), f32),
            pltpu.VMEM((CHUNK + 1, LANES), f32),
            pltpu.VMEM((CHUNK + 1, LANES), f32),
            dma((2, peers)),
            dma((2, Z - 1)),
            dma((2, 1)),
            dma((2, Z - 1)),
        ],
        compiler_params=pltpu.CompilerParams(
            collective_id=1, has_side_effects=True, vmem_limit_bytes=GRANT
        ),
        name="blend",
    )(total, self_cost, rows)
    robot_cost, blended = pl.pallas_call(
        finish_kernel,
        out_shape=(
            jax.ShapeDtypeStruct((ROBOTS_HERE, COLUMNS), f32),
            jax.ShapeDtypeStruct((ROBOTS_HERE, 3, W, SPHERES), f32),
        ),
        in_specs=in_vmem(2),
        out_specs=tuple(in_vmem(2)),
        scratch_shapes=[pltpu.VMEM((LANES, LANES), f32)],
        compiler_params=pltpu.CompilerParams(vmem_limit_bytes=GRANT),
        name="finish",
    )(robot_cost, gathered)
    return robot_cost, blended.transpose(0, 1, 3, 2)


def solution(mesh):
    return jax.shard_map(
        local,
        mesh=mesh,
        in_specs=(P("robot", None, None, "seed"), P("robot", None), P("robot"), P("robot", None)),
        out_specs=(P("robot", "seed"), P("robot", None, None, None)),
        check_vma=False,
    )
```

```python
import functools
import math

import jax
import jax.numpy as jnp
from jax import lax
from jax.experimental import pallas as pl
from jax.experimental.pallas import tpu as pltpu
from jax.sharding import PartitionSpec as P

W = 32
SPHERES = 52
GROUPS = 7
FIRST_GROUPS = 4
ROBOTS_HERE = 2
ROBOT_DEVICES = 16
ROBOTS = ROBOTS_HERE * ROBOT_DEVICES
LANES = 128
COLUMNS = 256
PART = 16
ROWS = ROBOTS_HERE * GROUPS * 4
Z = 8
CHUNK = 11
COUNT_LANE = 32
ROOT = math.sqrt(math.log2(math.e))
FAR = 1.0e6
STEP_ROWS = 8
ROW_IDS = ROBOTS * GROUPS
WORDS = 56
STEPS_WORD = 56
ENTRY = 64
ORDER = ROBOTS * ENTRY
CASE_STEPS = ORDER + 32
CASE_START = ORDER + 40
TABLE_ROWS = 24
EARLY_GROUPS = 3
GRANT = 16 * 1024 * 1024
MESH = pl.DeviceIdType.MESH


def iota(axis, shape=(8, LANES)):
    return lax.broadcasted_iota(jnp.int32, shape, axis)


def pair_argument(a, b):
    dx, dy, dz = a[0] - b[0], a[1] - b[1], a[2] - b[2]
    spread = a[3] + b[3]
    return (dx * dx + dy * dy + dz * dz) / (-spread * spread)


def pair_term(a, b):
    return jnp.exp2(pair_argument(a, b))


def centre_rows(ref, robot, axis, group, half):
    first = min(8 * group, SPHERES - 8)
    row = ((axis * SPHERES + first) * 2 + half) * ROBOTS_HERE + robot
    value = ref[pl.ds(row, 8, stride=2 * ROBOTS_HERE), :]
    return value if first == 8 * group else pltpu.roll(value, 4, 0)


def spread_kernel(
    counts_hbm,
    centres_hbm,
    radius_hbm,
    adjacency_hbm,
    recv_ref,
    turned_ref,
    self_ref,
    table_ref,
    counts_ref,
    centres_ref,
    radius_ref,
    adjacency_ref,
    send,
    swept,
    note_send,
    note_recv,
    note,
    load_sem,
    send_sem,
    recv_sem,
    note_send_sem,
    note_recv_sem,
):
    me = lax.axis_index("robot")
    seed = lax.axis_index("seed")
    peers = [lax.rem(me + step, ROBOT_DEVICES) for step in range(1, ROBOT_DEVICES)]

    loads = [
        pltpu.make_async_copy(counts_hbm, counts_ref, load_sem.at[0]),
        pltpu.make_async_copy(radius_hbm, radius_ref, load_sem.at[1]),
        pltpu.make_async_copy(adjacency_hbm, adjacency_ref, load_sem.at[2]),
    ]
    per_axis, early = 4 * SPHERES, 4 * 8 * EARLY_GROUPS
    for axis in range(3):
        at = pl.ds(axis * per_axis, early)
        loads.append(pltpu.make_async_copy(centres_hbm.at[at], centres_ref.at[at], load_sem.at[3 + axis]))
    for axis in range(3):
        at = pl.ds(axis * per_axis + early, per_axis - early)
        loads.append(pltpu.make_async_copy(centres_hbm.at[at], centres_ref.at[at], load_sem.at[6 + axis]))
    for load in loads:
        load.start()

    barrier = pltpu.get_barrier_semaphore()
    for peer in peers:
        pl.semaphore_signal(barrier, inc=1, device_id=(peer, seed), device_id_type=MESH)

    for load in loads[:6]:
        load.wait()

    sub, lane = iota(0), iota(1)
    part = lane // PART
    last_waypoint = lane % W == W - 1
    radius_lane = iota(1, (8, SPHERES))
    radius_sub = iota(0, (8, SPHERES))
    note_send[...] = jnp.zeros((ROBOTS_HERE, LANES), jnp.int32)
    note_send[:, 0:ROBOTS] = adjacency_ref[...]
    for robot in range(ROBOTS_HERE):
        note_send[robot : robot + 1, COUNT_LANE : COUNT_LANE + 1] = jnp.full((1, 1), counts_ref[robot], jnp.int32)
    for group in range(GROUPS):
        if group == EARLY_GROUPS:
            for load in loads[6:]:
                load.wait()
        for robot in range(ROBOTS_HERE):
            count = counts_ref[robot]
            radius_row = jnp.broadcast_to(radius_ref[robot : robot + 1, :], (8, SPHERES))
            number = (me * ROBOTS_HERE + robot) * 64 + 1
            radius = jnp.sum(
                jnp.where(radius_lane == radius_sub + 8 * group, radius_row, 0.0),
                axis=1,
                keepdims=True,
            )
            sphere = sub + 8 * group
            active = sphere < count
            far = FAR * (sphere + number).astype(jnp.float32)
            for half in range(2):
                out, square = [], None
                for axis in range(3):
                    here = centre_rows(centres_ref, robot, axis, group, half)
                    ahead = jnp.where(last_waypoint, here, pltpu.roll(here, LANES - 1, 1))
                    step = ahead - here
                    square = step * step if square is None else square + step * step
                    middle = (here + ahead) * (0.5 * ROOT)
                    out.append(jnp.where(active, middle, far if axis == 0 else 0.0))
                out.append(jnp.where(active, radius + 0.5 * jnp.sqrt(square + 1e-6), 1.0))
                for quantity in range(4):
                    value = out[quantity]
                    swept[half * ROBOTS_HERE + robot, quantity, 8 * group : 8 * group + 8, :] = value
                    value = pltpu.roll(value, 0, 1, stride=PART, stride_axis=0)
                    for bit in (1, 2, 4):
                        value = jnp.where(part & bit != 0, pltpu.roll(value, 8 - bit, 0), value)
                    row = (robot * GROUPS + group) * 4 + quantity
                    send[pl.ds(half * 8 * ROWS + row, 8, stride=ROWS), :] = value

    pl.semaphore_wait(barrier, ROBOT_DEVICES - 1)

    def slot_of(device):
        return (device // 8) * 8 + lax.rem(8 - lax.rem(device, 8), 8)

    def rows_of(slot):
        return pl.ds(pl.multiple_of(slot * ROWS, 8), ROWS)

    def send_note(number):
        return pltpu.make_async_remote_copy(
            src_ref=note_send,
            dst_ref=note_recv.at[me],
            send_sem=note_send_sem.at[number],
            recv_sem=note_recv_sem.at[number],
            device_id=(lax.rem(me + 1 + number, ROBOT_DEVICES), seed),
            device_id_type=MESH,
        )

    def send_rows(number):
        peer = lax.rem(me + 1 + number, ROBOT_DEVICES)
        return pltpu.make_async_remote_copy(
            src_ref=send.at[rows_of(slot_of(peer))],
            dst_ref=recv_ref.at[rows_of(me)],
            send_sem=send_sem.at[number],
            recv_sem=recv_sem.at[number],
            device_id=(peer, seed),
            device_id_type=MESH,
        )

    def for_peers(act):
        def one(number, carry):
            act(number)
            return carry

        lax.fori_loop(0, ROBOT_DEVICES - 1, one, 0)

    for_peers(lambda number: send_note(number).start())
    for_peers(lambda number: send_rows(number).start())
    note_recv[me] = note_send[...]
    recv_ref[rows_of(me), :] = send[rows_of(slot_of(me)), :]

    def turn_rows(device):
        row = pl.multiple_of(device * ROWS, 8)
        for n in range(ROWS):
            line = jnp.broadcast_to(recv_ref[pl.ds(row + n, 1), :], (8, LANES))
            turned_ref[row + n] = pltpu.roll(line, 0, 1, stride=PART, stride_axis=0)

    turn_rows(me)
    for index in range(2 * ROBOTS_HERE):
        robot = index % ROBOTS_HERE
        number = (me * ROBOTS_HERE + robot) * 64 + 1
        for quantity in range(4):
            fill = jnp.full((8, LANES), float(quantity == 3))
            if quantity == 0:
                fill = FAR * (sub + 8 * GROUPS + number).astype(jnp.float32)
            swept[index, quantity, 8 * GROUPS : 8 * GROUPS + 8, :] = fill

    def self_pairs(index, carry):
        sums = [jnp.zeros((8, LANES), jnp.float32) for _ in range(4)]
        turn = 0
        for group in range(GROUPS):
            first = [swept[index, q, 8 * group : 8 * group + 8, :] for q in range(4)]
            for apart in range(2, SPHERES - 8 * group):
                start = 8 * group + apart
                second = [swept[index, q, start : start + 8, :] for q in range(4)]
                sums[turn] = sums[turn] + pair_term(first, second)
                turn = (turn + 1) % 4
        total = jnp.sum((sums[0] + sums[1]) + (sums[2] + sums[3]), axis=0, keepdims=True)
        self_ref[pl.ds(index, 1), :] = total * (1.0 / (SPHERES * SPHERES))
        return carry

    lax.fori_loop(0, 2 * ROBOTS_HERE, self_pairs, 0)

    for_peers(lambda number: send_note(number).wait_recv())
    for device in range(ROBOT_DEVICES):
        note[ROBOTS_HERE * device : ROBOTS_HERE * (device + 1), :] = note_recv[device]
    shape = (ROBOTS, LANES)
    row, column = iota(0, shape), iota(1, shape)
    row_number = row.astype(jnp.float32)
    noted = note[...].astype(jnp.float32)
    link = jnp.where((column > row) & (column < ROBOTS) & (noted != 0.0), 1.0, 0.0)
    counts = jnp.sum(jnp.where(column == COUNT_LANE, noted, 0.0), axis=1, keepdims=True)
    groups = jnp.floor((counts + 7.0) * 0.125)

    def as_row(value):
        return jnp.sum(jnp.where(row == column, value, 0.0), axis=0, keepdims=True)

    length = link * as_row(groups)
    before = (iota(0, (LANES, LANES)) < iota(1, (LANES, LANES))).astype(jnp.float32)
    start = jnp.dot(length, before, preferred_element_type=jnp.float32)
    end = start + length
    words = jnp.zeros(shape, jnp.int32)
    for byte in range(4):
        place = (column * 4 + byte).astype(jnp.float32)
        listed = jnp.full(shape, float(ROW_IDS))
        for robot in range(1, ROBOTS):
            first, past = start[:, robot : robot + 1], end[:, robot : robot + 1]
            listed = jnp.where(
                (place >= first) & (place < past), place + (float(GROUPS * robot) - first), listed
            )
        words = words | (listed.astype(jnp.int32) << (8 * byte))
    steps = jnp.floor((jnp.sum(length, axis=1, keepdims=True) + (STEP_ROWS - 1.0)) * (1.0 / STEP_ROWS))
    words = jnp.where(column == STEPS_WORD, steps.astype(jnp.int32), words)
    note[...] = jnp.where(column < ENTRY, words, 0)
    table_ref[0:16, :] = note[pl.ds(0, 16, stride=2), :] + pltpu.roll(
        note[pl.ds(1, 16, stride=2), :], ENTRY, 1
    )
    busy = jnp.where(steps > 0.0, 1.0, 0.0)
    key = groups * 32.0 + row_number
    key_row, busy_row = as_row(key), as_row(busy)
    rank = jnp.sum(jnp.where(key_row < key, busy_row, 0.0), axis=1, keepdims=True)
    lane_number = column.astype(jnp.float32)
    last = jnp.sum(
        jnp.where((rank == lane_number) & (busy > 0.0), row_number, 0.0), axis=0, keepdims=True
    )
    line = iota(1, (1, LANES))
    for case in range(FIRST_GROUPS, GROUPS + 1):
        of_case = jnp.where(row == column, jnp.where(groups == float(case), steps, 0.0), 0.0)
        earlier = jnp.where(row == column, jnp.where(groups < float(case), busy, 0.0), 0.0)
        last = jnp.where(line == CASE_STEPS - ORDER + case - FIRST_GROUPS, jnp.sum(of_case), last)
        last = jnp.where(line == CASE_START - ORDER + case - FIRST_GROUPS, jnp.sum(earlier), last)
    table_ref[16:24, :] = jnp.broadcast_to(last, (8, LANES)).astype(jnp.int32)
    recv_ref[ROBOT_DEVICES * ROWS : ROBOT_DEVICES * ROWS + 8, :] = jnp.where(
        sub == 0, -1000.0 * FAR, jnp.where(sub == 3, 1.0, 0.0)
    )

    def arrive(number):
        send_rows(number).wait_recv()
        turn_rows(lax.rem(me + ROBOT_DEVICES - 1 - number, ROBOT_DEVICES))

    for_peers(arrive)
    for_peers(lambda number: send_note(number).wait_send())
    for_peers(lambda number: send_rows(number).wait_send())


def cross_kernel(table, rows, turned, total, arguments):
    zero = jnp.zeros((8, LANES), jnp.float32)
    for slot in range(STEP_ROWS * GROUPS):
        arguments[slot] = zero

    def clear(index, carry):
        for n in range(15):
            total[index * 15 + n] = zero
        return carry

    lax.fori_loop(0, (ROW_IDS + 1) // 15, clear, 0)

    def row_ids(words):
        return [lax.shift_right_logical(word, 8 * n) & 255 for word in words for n in range(4)]

    def sum_terms(groups, n):
        terms = [jnp.exp2(arguments[n * groups + group]) for group in range(groups)]
        while len(terms) > 1:
            terms = [p + q for p, q in zip(terms[0::2], terms[1::2])] + terms[len(terms) & ~1 :]
        return terms[0]

    def add_up(ids, news):
        own = news
        while len(own) > 1:
            own = [p + q for p, q in zip(own[0::2], own[1::2])]
        olds = [total[row_id] for row_id in ids]
        for row_id, old, new in zip(ids, olds, news + own):
            total[row_id] = old + new

    def entry_of(turn, step):
        robot = jnp.minimum(table[ORDER + turn], ROBOTS - 1)
        at = robot * ENTRY + 2 * step
        return robot, table[at], table[at + 1]

    for groups in range(FIRST_GROUPS, GROUPS + 1):

        def one_step(_, state, groups=groups):
            turn, step, robot, first, second, *past_ids = state
            ids = row_ids((first, second)) + [robot * GROUPS]
            a_row = robot * (4 * GROUPS)
            news = []
            for n in range(STEP_ROWS):
                news.append(sum_terms(groups, n))
                b = [
                    jnp.broadcast_to(rows[pl.ds(ids[n] * 4 + q, 1), :], (8, LANES))
                    for q in range(4)
                ]
                for group in range(groups):
                    a = [turned[a_row + (group * 4 + q)] for q in range(4)]
                    arguments[n * groups + group] = pair_argument(a, b)
            add_up(past_ids, news)
            step = step + 1
            over = (step >= table[robot * ENTRY + STEPS_WORD]).astype(jnp.int32)
            turn, step = turn + over, step * (1 - over)
            return turn, step, *entry_of(turn, step), *ids

        case = groups - FIRST_GROUPS
        turn = table[CASE_START + case]
        nothing = [jnp.int32(ROW_IDS)] * (STEP_ROWS + 1)
        state = (turn, jnp.int32(0), *entry_of(turn, 0), *nothing)
        state = lax.fori_loop(0, table[CASE_STEPS + case], one_step, state)
        add_up(list(state[5:]), [sum_terms(groups, n) for n in range(STEP_ROWS)])


def blend_kernel(
    total,
    self_ref,
    centres_ref,
    robot_cost_ref,
    gathered,
    sums,
    cost_ref,
    cost_recv,
    weight,
    packed,
    parts,
    mine,
    other,
    cost_sems,
    part_sems,
    pair_sems,
    gather_sems,
):
    me = lax.axis_index("robot")
    seed = lax.axis_index("seed")
    x, z = seed // Z, lax.rem(seed, Z)
    peers = [lax.rem(me + step, ROBOT_DEVICES) for step in range(1, ROBOT_DEVICES)]
    z_peers = [lax.rem(z + step, Z) for step in range(1, Z)]
    opposite = (1 - x) * Z + z

    barrier = pltpu.get_barrier_semaphore()
    for peer in peers:
        pl.semaphore_signal(barrier, inc=1, device_id=(peer, seed), device_id_type=MESH)
    for peer in z_peers:
        pl.semaphore_signal(barrier, inc=1, device_id=(me, x * Z + peer), device_id_type=MESH)
    pl.semaphore_signal(barrier, inc=1, device_id=(me, opposite), device_id_type=MESH)

    for robot in range(ROBOTS):
        found = total[robot * GROUPS]
        for group in range(1, GROUPS):
            found = found + total[robot * GROUPS + group]
        sums[robot] = found
    cost = jnp.sum(sums[...], axis=1)
    for shift in (64, 32, 16):
        cost = cost + pltpu.roll(cost, shift, 1)
    cost = cost * (1.0 / (SPHERES * SPHERES))
    for device in range(ROBOT_DEVICES):
        cost_ref[device] = cost[ROBOTS_HERE * device : ROBOTS_HERE * (device + 1), :]

    pl.semaphore_wait(barrier, ROBOT_DEVICES - 1 + Z)

    def start(src, dst, sems, number, device):
        copy = pltpu.make_async_remote_copy(
            src_ref=src,
            dst_ref=dst,
            send_sem=sems.at[0, number],
            recv_sem=sems.at[1, number],
            device_id=device,
            device_id_type=MESH,
        )
        copy.start()
        return copy

    copies = [
        start(cost_ref.at[peer], cost_recv.at[me], cost_sems, number, (peer, seed))
        for number, peer in enumerate(peers)
    ]
    cost_recv[me] = cost_ref[me]
    for copy in copies:
        copy.wait_recv()
    sent = copies

    lane = iota(1, (ROBOTS_HERE, LANES))
    part = lane // PART
    for half in range(2):
        cost = self_ref[half * ROBOTS_HERE : (half + 1) * ROBOTS_HERE, :]
        for k in range(8):
            cost = cost + jnp.where(part == k, cost_recv[half * 8 + k], 0.0)
        robot_cost_ref[:, half * LANES : (half + 1) * LANES] = cost
        for bit in (1, 2, 4, 8, 16):
            cost = cost + jnp.where(
                lane & bit != 0, pltpu.roll(cost, bit, 1), pltpu.roll(cost, LANES - bit, 1)
            )
        weight[half] = 1.0 / (1.0 + cost)
    weights = weight[0] + weight[1]
    weights = weights + pltpu.roll(weights, 64, 1)
    weights = weights + pltpu.roll(weights, 32, 1)
    line = iota(1, (1, LANES))
    total_row = jnp.where(line < 64, weights[0:1, :], weights[1:2, :])

    quarter = iota(1) // W
    units = [[], []]
    for robot in range(ROBOTS_HERE):
        weights = [
            jnp.broadcast_to(weight[half, robot : robot + 1, :], (8, LANES)) for half in range(2)
        ]
        for axis in range(3):
            for group in range(GROUPS):
                value = (
                    centre_rows(centres_ref, robot, axis, group, 0) * weights[0]
                    + centre_rows(centres_ref, robot, axis, group, 1) * weights[1]
                )
                value = value + pltpu.roll(value, 64, 1)
                units[robot].append(value + pltpu.roll(value, 32, 1))
        units[robot].append(jnp.zeros((8, LANES), jnp.float32))
    for v in range(CHUNK):
        value = jnp.where(
            quarter < 2,
            jnp.where(quarter == 0, units[0][v], units[0][CHUNK + v]),
            jnp.where(quarter == 2, units[1][v], units[1][CHUNK + v]),
        )
        done = 0
        while done < 8:
            chunk, row = divmod(8 * v + done, CHUNK)
            length = min(8 - done, CHUNK - row)
            packed[chunk, row : row + length, :] = value[done : done + length, :]
            done += length
    for chunk in range(Z):
        packed[chunk, CHUNK : CHUNK + 1, :] = total_row

    copies = [
        start(packed.at[peer], parts.at[number], part_sems, number, (me, x * Z + peer))
        for number, peer in enumerate(z_peers)
    ]
    found = packed[z]
    for number, copy in enumerate(copies):
        copy.wait_recv()
        found = found + parts[number]
    sent = sent + copies

    mine[...] = found
    copy = start(mine, other, pair_sems, 0, (me, opposite))
    copy.wait_recv()
    sent = sent + [copy]
    found = mine[...] + other[...]
    gathered[z] = found / found[CHUNK : CHUNK + 1, :]

    copies = [
        start(gathered.at[z], gathered.at[z], gather_sems, number, (me, x * Z + peer))
        for number, peer in enumerate(z_peers)
    ]
    for copy in copies:
        copy.wait_recv()
    sent = sent + copies

    for copy in sent:
        copy.wait_send()


def finish_kernel(cost_in, gathered, cost_out, blended, lines):
    cost_out[...] = cost_in[...]
    for chunk in range(Z):
        lines[CHUNK * chunk : CHUNK * (chunk + 1), :] = gathered[chunk, 0:CHUNK, :]
    turned = lines[...].T
    for robot in range(ROBOTS_HERE):
        for axis in range(3):
            for quarter in range(2):
                low = max(axis * GROUPS, quarter * CHUNK)
                high = min((axis + 1) * GROUPS, (quarter + 1) * CHUNK)
                if low < high:
                    source = (robot * 2 + quarter) * W
                    lane = 8 * (low - quarter * CHUNK)
                    first = 8 * (low - axis * GROUPS)
                    width = min(8 * (high - low), SPHERES - first)
                    blended[robot, axis, :, first : first + width] = turned[
                        source : source + W, lane : lane + width
                    ]


def in_vmem(count):
    return [pl.BlockSpec(memory_space=pltpu.VMEM)] * count


IN_SMEM = pl.BlockSpec(memory_space=pltpu.SMEM)


def local(centres, sphere_radius, counts, adjacency):
    dma = pltpu.SemaphoreType.DMA
    f32 = jnp.float32
    peers = ROBOT_DEVICES - 1
    rows = centres.transpose(1, 2, 0, 3).reshape(3 * SPHERES, ROBOTS_HERE, 2, LANES)
    rows = rows.transpose(0, 2, 1, 3).reshape(3 * SPHERES * 2 * ROBOTS_HERE, LANES)
    in_hbm = pl.BlockSpec(memory_space=pltpu.HBM)
    received, turned, self_cost, table = pl.pallas_call(
        spread_kernel,
        out_shape=(
            jax.ShapeDtypeStruct((ROBOT_DEVICES * ROWS + 8, LANES), f32),
            jax.ShapeDtypeStruct((ROBOT_DEVICES * ROWS, 8, LANES), f32),
            jax.ShapeDtypeStruct((2 * ROBOTS_HERE, LANES), f32),
            jax.ShapeDtypeStruct((TABLE_ROWS, LANES), jnp.int32),
        ),
        in_specs=[in_hbm] * 4,
        out_specs=tuple(in_vmem(4)),
        scratch_shapes=[
            pltpu.SMEM((ROBOTS_HERE,), jnp.int32),
            pltpu.VMEM(rows.shape, f32),
            pltpu.VMEM((ROBOTS_HERE, SPHERES), f32),
            pltpu.VMEM((ROBOTS_HERE, ROBOTS), jnp.int32),
            pltpu.VMEM((ROBOT_DEVICES * ROWS, LANES), f32),
            pltpu.VMEM((2 * ROBOTS_HERE, 4, 64, LANES), f32),
            pltpu.VMEM((ROBOTS_HERE, LANES), jnp.int32),
            pltpu.VMEM((ROBOT_DEVICES, ROBOTS_HERE, LANES), jnp.int32),
            pltpu.VMEM((ROBOTS, LANES), jnp.int32),
            dma((9,)),
            dma((peers,)),
            dma((peers,)),
            dma((peers,)),
            dma((peers,)),
        ],
        compiler_params=pltpu.CompilerParams(
            collective_id=0, has_side_effects=True, vmem_limit_bytes=GRANT
        ),
        name="spread",
    )(*[pltpu.with_memory_space_constraint(v, pltpu.HBM) for v in (counts, rows, sphere_radius, adjacency)])
    total = pl.pallas_call(
        cross_kernel,
        out_shape=jax.ShapeDtypeStruct((ROW_IDS + 1, 8, LANES), f32),
        in_specs=[IN_SMEM] + in_vmem(2),
        out_specs=in_vmem(1)[0],
        scratch_shapes=[pltpu.VMEM((STEP_ROWS * GROUPS, 8, LANES), f32)],
        compiler_params=pltpu.CompilerParams(vmem_limit_bytes=GRANT),
        name="cross",
    )(table.reshape(TABLE_ROWS * LANES), received, turned)
    robot_cost, gathered = pl.pallas_call(
        blend_kernel,
        out_shape=(
            jax.ShapeDtypeStruct((ROBOTS_HERE, COLUMNS), f32),
            jax.ShapeDtypeStruct((Z, CHUNK + 1, LANES), f32),
        ),
        in_specs=in_vmem(3),
        out_specs=tuple(in_vmem(2)),
        scratch_shapes=[
            pltpu.VMEM((ROBOTS, 8, LANES), f32),
            pltpu.VMEM((ROBOT_DEVICES, ROBOTS_HERE, LANES), f32),
            pltpu.VMEM((ROBOT_DEVICES, ROBOTS_HERE, LANES), f32),
            pltpu.VMEM((2, ROBOTS_HERE, LANES), f32),
            pltpu.VMEM((Z, CHUNK + 1, LANES), f32),
            pltpu.VMEM((Z - 1, CHUNK + 1, LANES), f32),
            pltpu.VMEM((CHUNK + 1, LANES), f32),
            pltpu.VMEM((CHUNK + 1, LANES), f32),
            dma((2, peers)),
            dma((2, Z - 1)),
            dma((2, 1)),
            dma((2, Z - 1)),
        ],
        compiler_params=pltpu.CompilerParams(
            collective_id=1, has_side_effects=True, vmem_limit_bytes=GRANT
        ),
        name="blend",
    )(total, self_cost, rows)
    robot_cost, blended = pl.pallas_call(
        finish_kernel,
        out_shape=(
            jax.ShapeDtypeStruct((ROBOTS_HERE, COLUMNS), f32),
            jax.ShapeDtypeStruct((ROBOTS_HERE, 3, W, SPHERES), f32),
        ),
        in_specs=in_vmem(2),
        out_specs=tuple(in_vmem(2)),
        scratch_shapes=[pltpu.VMEM((LANES, LANES), f32)],
        compiler_params=pltpu.CompilerParams(vmem_limit_bytes=GRANT),
        name="finish",
    )(robot_cost, gathered)
    return robot_cost, blended.transpose(0, 1, 3, 2)


def solution(mesh):
    return jax.shard_map(
        local,
        mesh=mesh,
        in_specs=(P("robot", None, None, "seed"), P("robot", None), P("robot"), P("robot", None)),
        out_specs=(P("robot", "seed"), P("robot", None, None, None)),
        check_vma=False,
    )
```

```python
import functools
import math

import jax
import jax.numpy as jnp
from jax import lax
from jax.experimental import pallas as pl
from jax.experimental.pallas import tpu as pltpu
from jax.sharding import PartitionSpec as P

W = 32
SPHERES = 52
GROUPS = 7
FIRST_GROUPS = 4
ROBOTS_HERE = 2
ROBOT_DEVICES = 16
ROBOTS = ROBOTS_HERE * ROBOT_DEVICES
LANES = 128
COLUMNS = 256
PART = 16
ROWS = ROBOTS_HERE * GROUPS * 4
Z = 8
CHUNK = 11
COUNT_LANE = 32
ROOT = math.sqrt(math.log2(math.e))
FAR = 1.0e6
STEP_ROWS = 8
ROW_IDS = ROBOTS * GROUPS
WORDS = 56
STEPS_WORD = 56
ENTRY = 64
ORDER = ROBOTS * ENTRY
CASE_STEPS = ORDER + 32
CASE_START = ORDER + 40
TABLE_ROWS = 24
EARLY_GROUPS = 3
GRANT = 16 * 1024 * 1024
MESH = pl.DeviceIdType.MESH


def iota(axis, shape=(8, LANES)):
    return lax.broadcasted_iota(jnp.int32, shape, axis)


def pair_argument(a, b):
    dx, dy, dz = a[0] - b[0], a[1] - b[1], a[2] - b[2]
    spread = a[3] + b[3]
    return (dx * dx + dy * dy + dz * dz) / (-spread * spread)


def pair_term(a, b):
    return jnp.exp2(pair_argument(a, b))


def centre_rows(ref, robot, axis, group, half):
    first = min(8 * group, SPHERES - 8)
    row = ((axis * SPHERES + first) * 2 + half) * ROBOTS_HERE + robot
    value = ref[pl.ds(row, 8, stride=2 * ROBOTS_HERE), :]
    return value if first == 8 * group else pltpu.roll(value, 4, 0)


def spread_kernel(
    counts_hbm,
    centres_hbm,
    radius_hbm,
    adjacency_hbm,
    recv_ref,
    turned_ref,
    self_ref,
    table_ref,
    counts_ref,
    centres_ref,
    radius_ref,
    adjacency_ref,
    send,
    swept,
    note_send,
    note_recv,
    note,
    load_sem,
    send_sem,
    recv_sem,
    note_send_sem,
    note_recv_sem,
):
    me = lax.axis_index("robot")
    seed = lax.axis_index("seed")
    peers = [lax.rem(me + step, ROBOT_DEVICES) for step in range(1, ROBOT_DEVICES)]

    loads = [
        pltpu.make_async_copy(counts_hbm, counts_ref, load_sem.at[0]),
        pltpu.make_async_copy(radius_hbm, radius_ref, load_sem.at[1]),
        pltpu.make_async_copy(adjacency_hbm, adjacency_ref, load_sem.at[2]),
    ]
    per_axis, early = 4 * SPHERES, 4 * 8 * EARLY_GROUPS
    for axis in range(3):
        at = pl.ds(axis * per_axis, early)
        loads.append(pltpu.make_async_copy(centres_hbm.at[at], centres_ref.at[at], load_sem.at[3 + axis]))
    for axis in range(3):
        at = pl.ds(axis * per_axis + early, per_axis - early)
        loads.append(pltpu.make_async_copy(centres_hbm.at[at], centres_ref.at[at], load_sem.at[6 + axis]))
    for load in loads:
        load.start()

    barrier = pltpu.get_barrier_semaphore()
    for peer in peers:
        pl.semaphore_signal(barrier, inc=1, device_id=(peer, seed), device_id_type=MESH)

    for load in loads[:6]:
        load.wait()

    sub, lane = iota(0), iota(1)
    part = lane // PART
    last_waypoint = lane % W == W - 1
    radius_lane = iota(1, (8, SPHERES))
    radius_sub = iota(0, (8, SPHERES))
    note_send[...] = jnp.zeros((ROBOTS_HERE, LANES), jnp.int32)
    note_send[:, 0:ROBOTS] = adjacency_ref[...]
    for robot in range(ROBOTS_HERE):
        note_send[robot : robot + 1, COUNT_LANE : COUNT_LANE + 1] = jnp.full((1, 1), counts_ref[robot], jnp.int32)
    for group in range(GROUPS):
        if group == EARLY_GROUPS:
            for load in loads[6:]:
                load.wait()
        for robot in range(ROBOTS_HERE):
            count = counts_ref[robot]
            radius_row = jnp.broadcast_to(radius_ref[robot : robot + 1, :], (8, SPHERES))
            number = (me * ROBOTS_HERE + robot) * 64 + 1
            radius = jnp.sum(
                jnp.where(radius_lane == radius_sub + 8 * group, radius_row, 0.0),
                axis=1,
                keepdims=True,
            )
            sphere = sub + 8 * group
            active = sphere < count
            far = FAR * (sphere + number).astype(jnp.float32)
            for half in range(2):
                out, square = [], None
                for axis in range(3):
                    here = centre_rows(centres_ref, robot, axis, group, half)
                    ahead = jnp.where(last_waypoint, here, pltpu.roll(here, LANES - 1, 1))
                    step = ahead - here
                    square = step * step if square is None else square + step * step
                    middle = (here + ahead) * (0.5 * ROOT)
                    out.append(jnp.where(active, middle, far if axis == 0 else 0.0))
                out.append(jnp.where(active, radius + 0.5 * jnp.sqrt(square + 1e-6), 1.0))
                for quantity in range(4):
                    value = out[quantity]
                    swept[half * ROBOTS_HERE + robot, quantity, 8 * group : 8 * group + 8, :] = value
                    value = pltpu.roll(value, 0, 1, stride=PART, stride_axis=0)
                    for bit in (1, 2, 4):
                        value = jnp.where(part & bit != 0, pltpu.roll(value, 8 - bit, 0), value)
                    row = (robot * GROUPS + group) * 4 + quantity
                    send[pl.ds(half * 8 * ROWS + row, 8, stride=ROWS), :] = value

    pl.semaphore_wait(barrier, ROBOT_DEVICES - 1)

    def slot_of(device):
        return (device // 8) * 8 + lax.rem(8 - lax.rem(device, 8), 8)

    def rows_of(slot):
        return pl.ds(pl.multiple_of(slot * ROWS, 8), ROWS)

    def send_note(number):
        return pltpu.make_async_remote_copy(
            src_ref=note_send,
            dst_ref=note_recv.at[me],
            send_sem=note_send_sem.at[number],
            recv_sem=note_recv_sem.at[number],
            device_id=(lax.rem(me + 1 + number, ROBOT_DEVICES), seed),
            device_id_type=MESH,
        )

    def send_rows(number):
        peer = lax.rem(me + 1 + number, ROBOT_DEVICES)
        return pltpu.make_async_remote_copy(
            src_ref=send.at[rows_of(slot_of(peer))],
            dst_ref=recv_ref.at[rows_of(me)],
            send_sem=send_sem.at[number],
            recv_sem=recv_sem.at[number],
            device_id=(peer, seed),
            device_id_type=MESH,
        )

    def for_peers(act):
        def one(number, carry):
            act(number)
            return carry

        lax.fori_loop(0, ROBOT_DEVICES - 1, one, 0)

    for_peers(lambda number: send_note(number).start())
    for_peers(lambda number: send_rows(number).start())
    note_recv[me] = note_send[...]
    recv_ref[rows_of(me), :] = send[rows_of(slot_of(me)), :]

    def turn_rows(device):
        row = pl.multiple_of(device * ROWS, 8)
        for n in range(ROWS):
            line = jnp.broadcast_to(recv_ref[pl.ds(row + n, 1), :], (8, LANES))
            turned_ref[row + n] = pltpu.roll(line, 0, 1, stride=PART, stride_axis=0)

    turn_rows(me)
    for index in range(2 * ROBOTS_HERE):
        robot = index % ROBOTS_HERE
        number = (me * ROBOTS_HERE + robot) * 64 + 1
        for quantity in range(4):
            fill = jnp.full((8, LANES), float(quantity == 3))
            if quantity == 0:
                fill = FAR * (sub + 8 * GROUPS + number).astype(jnp.float32)
            swept[index, quantity, 8 * GROUPS : 8 * GROUPS + 8, :] = fill

    def self_pairs(index, carry):
        sums = [jnp.zeros((8, LANES), jnp.float32) for _ in range(4)]
        turn = 0
        for group in range(GROUPS):
            first = [swept[index, q, 8 * group : 8 * group + 8, :] for q in range(4)]
            for apart in range(2, SPHERES - 8 * group):
                start = 8 * group + apart
                second = [swept[index, q, start : start + 8, :] for q in range(4)]
                sums[turn] = sums[turn] + pair_term(first, second)
                turn = (turn + 1) % 4
        total = jnp.sum((sums[0] + sums[1]) + (sums[2] + sums[3]), axis=0, keepdims=True)
        self_ref[pl.ds(index, 1), :] = total * (1.0 / (SPHERES * SPHERES))
        return carry

    lax.fori_loop(0, 2 * ROBOTS_HERE, self_pairs, 0)

    for_peers(lambda number: send_note(number).wait_recv())
    for device in range(ROBOT_DEVICES):
        note[ROBOTS_HERE * device : ROBOTS_HERE * (device + 1), :] = note_recv[device]
    shape = (ROBOTS, LANES)
    row, column = iota(0, shape), iota(1, shape)
    row_number = row.astype(jnp.float32)
    noted = note[...].astype(jnp.float32)
    link = jnp.where((column > row) & (column < ROBOTS) & (noted != 0.0), 1.0, 0.0)
    counts = jnp.sum(jnp.where(column == COUNT_LANE, noted, 0.0), axis=1, keepdims=True)
    groups = jnp.floor((counts + 7.0) * 0.125)

    def as_row(value):
        return jnp.sum(jnp.where(row == column, value, 0.0), axis=0, keepdims=True)

    length = link * as_row(groups)
    before = (iota(0, (LANES, LANES)) < iota(1, (LANES, LANES))).astype(jnp.float32)
    start = jnp.dot(length, before, preferred_element_type=jnp.float32)
    end = start + length
    words = jnp.zeros(shape, jnp.int32)
    for byte in range(4):
        place = (column * 4 + byte).astype(jnp.float32)
        listed = jnp.full(shape, float(ROW_IDS))
        for robot in range(1, ROBOTS):
            first, past = start[:, robot : robot + 1], end[:, robot : robot + 1]
            listed = jnp.where(
                (place >= first) & (place < past), place + (float(GROUPS * robot) - first), listed
            )
        words = words | (listed.astype(jnp.int32) << (8 * byte))
    steps = jnp.floor((jnp.sum(length, axis=1, keepdims=True) + (STEP_ROWS - 1.0)) * (1.0 / STEP_ROWS))
    words = jnp.where(column == STEPS_WORD, steps.astype(jnp.int32), words)
    note[...] = jnp.where(column < ENTRY, words, 0)
    table_ref[0:16, :] = note[pl.ds(0, 16, stride=2), :] + pltpu.roll(
        note[pl.ds(1, 16, stride=2), :], ENTRY, 1
    )
    busy = jnp.where(steps > 0.0, 1.0, 0.0)
    key = groups * 32.0 + row_number
    key_row, busy_row = as_row(key), as_row(busy)
    rank = jnp.sum(jnp.where(key_row < key, busy_row, 0.0), axis=1, keepdims=True)
    lane_number = column.astype(jnp.float32)
    last = jnp.sum(
        jnp.where((rank == lane_number) & (busy > 0.0), row_number, 0.0), axis=0, keepdims=True
    )
    line = iota(1, (1, LANES))
    for case in range(FIRST_GROUPS, GROUPS + 1):
        of_case = jnp.where(row == column, jnp.where(groups == float(case), steps, 0.0), 0.0)
        earlier = jnp.where(row == column, jnp.where(groups < float(case), busy, 0.0), 0.0)
        last = jnp.where(line == CASE_STEPS - ORDER + case - FIRST_GROUPS, jnp.sum(of_case), last)
        last = jnp.where(line == CASE_START - ORDER + case - FIRST_GROUPS, jnp.sum(earlier), last)
    table_ref[16:24, :] = jnp.broadcast_to(last, (8, LANES)).astype(jnp.int32)
    recv_ref[ROBOT_DEVICES * ROWS : ROBOT_DEVICES * ROWS + 8, :] = jnp.where(
        sub == 0, -1000.0 * FAR, jnp.where(sub == 3, 1.0, 0.0)
    )

    def arrive(number):
        send_rows(number).wait_recv()
        turn_rows(lax.rem(me + ROBOT_DEVICES - 1 - number, ROBOT_DEVICES))

    for_peers(arrive)
    for_peers(lambda number: send_note(number).wait_send())
    for_peers(lambda number: send_rows(number).wait_send())


def cross_kernel(table, rows, turned, total):
    zero = jnp.zeros((8, LANES), jnp.float32)

    def clear(index, carry):
        for n in range(15):
            total[index * 15 + n] = zero
        return carry

    lax.fori_loop(0, (ROW_IDS + 1) // 15, clear, 0)

    def pair_sums(groups, robot, ids):
        a_row = robot * (4 * GROUPS)
        sums = []
        for row_id in ids:
            b = [
                jnp.broadcast_to(rows[pl.ds(row_id * 4 + q, 1), :], (8, LANES)) for q in range(4)
            ]
            terms = []
            for group in range(groups):
                a = [turned[a_row + (group * 4 + q)] for q in range(4)]
                terms.append(pair_term(a, b))
            while len(terms) > 1:
                terms = [p + q for p, q in zip(terms[0::2], terms[1::2])] + terms[len(terms) & ~1 :]
            sums.append(terms[0])
        return sums

    def add_up(robot, ids, found):
        own = found
        while len(own) > 1:
            own = [p + q for p, q in zip(own[0::2], own[1::2])]
        ids = ids + [robot * GROUPS]
        olds = [total[row_id] for row_id in ids]
        for row_id, old, new in zip(ids, olds, found + own):
            total[row_id] = old + new

    nothing = ROW_IDS * 0x01010101 - (1 << 32)

    def step_of(turn, step, there):
        robot = jnp.minimum(table[ORDER + turn], ROBOTS - 1)
        entry = robot * ENTRY
        words = [
            jnp.where(there, table[entry + 2 * step + n], jnp.int32(nothing)) for n in range(2)
        ]
        ids = [lax.shift_right_logical(word, 8 * n) & 255 for word in words for n in range(4)]
        step = step + 1
        over = (step >= table[entry + STEPS_WORD]).astype(jnp.int32)
        return robot, ids, jnp.minimum(turn + over, ROBOTS - 1), step * (1 - over)

    for groups in range(FIRST_GROUPS, GROUPS + 1):
        steps = table[CASE_STEPS + groups - FIRST_GROUPS]

        def two_steps_of(index, turn, step):
            robot, ids, turn, step = step_of(turn, step, 2 * index < steps)
            other, other_ids, turn, step = step_of(turn, step, 2 * index + 1 < steps)
            return turn, step, robot, other, *ids, *other_ids

        def two_steps(index, state, groups=groups, two_steps_of=two_steps_of):
            turn, step, robot, other, *ids = state
            ids, other_ids = ids[:STEP_ROWS], ids[STEP_ROWS:]
            found = pair_sums(groups, robot, ids)
            other_found = pair_sums(groups, other, other_ids)
            add_up(robot, ids, found)
            add_up(other, other_ids, other_found)
            return two_steps_of(index + 1, turn, step)

        start = jnp.minimum(table[CASE_START + groups - FIRST_GROUPS], ROBOTS - 1)
        lax.fori_loop(0, (steps + 1) >> 1, two_steps, two_steps_of(0, start, jnp.int32(0)))


def blend_kernel(
    total,
    self_ref,
    centres_ref,
    robot_cost_ref,
    gathered,
    sums,
    cost_ref,
    cost_recv,
    weight,
    packed,
    parts,
    cost_sems,
    part_sems,
    gather_sems,
):
    me = lax.axis_index("robot")
    seed = lax.axis_index("seed")
    x, z = seed // Z, lax.rem(seed, Z)
    peers = [lax.rem(me + step, ROBOT_DEVICES) for step in range(1, ROBOT_DEVICES)]
    z_peers = [lax.rem(z + step, Z) for step in (4, 3, 5, 2, 6, 1, 7)]
    seed_peers = [lax.rem((1 - x) * Z + lax.rem(z + 4, Z), 2 * Z)] + [p for step in (3, 5, 2, 6, 1, 7, 0) for p in ([(1 - x) * Z + lax.rem(z + step, Z)])]
    seed_peers = seed_peers[:3] + [x * Z + lax.rem(z + 4, Z)] + seed_peers[3:5] + [x * Z + lax.rem(z + 3, Z), x * Z + lax.rem(z + 5, Z)] + seed_peers[5:7] + [x * Z + lax.rem(z + 2, Z), x * Z + lax.rem(z + 6, Z)] + seed_peers[7:] + [x * Z + lax.rem(z + 1, Z), x * Z + lax.rem(z + 7, Z)]

    barrier = pltpu.get_barrier_semaphore()
    for peer in peers:
        pl.semaphore_signal(barrier, inc=1, device_id=(peer, seed), device_id_type=MESH)
    for peer in seed_peers:
        pl.semaphore_signal(barrier, inc=1, device_id=(me, peer), device_id_type=MESH)

    for robot in range(ROBOTS):
        found = total[robot * GROUPS]
        for group in range(1, GROUPS):
            found = found + total[robot * GROUPS + group]
        sums[robot] = found
    cost = jnp.sum(sums[...], axis=1)
    for shift in (64, 32, 16):
        cost = cost + pltpu.roll(cost, shift, 1)
    cost = cost * (1.0 / (SPHERES * SPHERES))
    for device in range(ROBOT_DEVICES):
        cost_ref[device] = cost[ROBOTS_HERE * device : ROBOTS_HERE * (device + 1), :]

    pl.semaphore_wait(barrier, ROBOT_DEVICES - 1 + 2 * Z - 1)

    def start(src, dst, sems, number, device):
        copy = pltpu.make_async_remote_copy(
            src_ref=src,
            dst_ref=dst,
            send_sem=sems.at[0, number],
            recv_sem=sems.at[1, number],
            device_id=device,
            device_id_type=MESH,
        )
        copy.start()
        return copy

    copies = [
        start(cost_ref.at[peer], cost_recv.at[me], cost_sems, number, (peer, seed))
        for number, peer in enumerate(peers)
    ]
    cost_recv[me] = cost_ref[me]
    for copy in copies:
        copy.wait_recv()
    sent = copies

    lane = iota(1, (ROBOTS_HERE, LANES))
    part = lane // PART
    for half in range(2):
        cost = self_ref[half * ROBOTS_HERE : (half + 1) * ROBOTS_HERE, :]
        for k in range(8):
            cost = cost + jnp.where(part == k, cost_recv[half * 8 + k], 0.0)
        robot_cost_ref[:, half * LANES : (half + 1) * LANES] = cost
        for bit in (1, 2, 4, 8, 16):
            cost = cost + jnp.where(
                lane & bit != 0, pltpu.roll(cost, bit, 1), pltpu.roll(cost, LANES - bit, 1)
            )
        weight[half] = 1.0 / (1.0 + cost)
    weights = weight[0] + weight[1]
    weights = weights + pltpu.roll(weights, 64, 1)
    weights = weights + pltpu.roll(weights, 32, 1)
    line = iota(1, (1, LANES))
    total_row = jnp.where(line < 64, weights[0:1, :], weights[1:2, :])

    quarter = iota(1) // W
    units = [[], []]
    for robot in range(ROBOTS_HERE):
        weights = [
            jnp.broadcast_to(weight[half, robot : robot + 1, :], (8, LANES)) for half in range(2)
        ]
        for axis in range(3):
            for group in range(GROUPS):
                value = (
                    centre_rows(centres_ref, robot, axis, group, 0) * weights[0]
                    + centre_rows(centres_ref, robot, axis, group, 1) * weights[1]
                )
                value = value + pltpu.roll(value, 64, 1)
                units[robot].append(value + pltpu.roll(value, 32, 1))
        units[robot].append(jnp.zeros((8, LANES), jnp.float32))
    for v in range(CHUNK):
        value = jnp.where(
            quarter < 2,
            jnp.where(quarter == 0, units[0][v], units[0][CHUNK + v]),
            jnp.where(quarter == 2, units[1][v], units[1][CHUNK + v]),
        )
        done = 0
        while done < 8:
            chunk, row = divmod(8 * v + done, CHUNK)
            length = min(8 - done, CHUNK - row)
            packed[chunk, row : row + length, :] = value[done : done + length, :]
            done += length
    for chunk in range(Z):
        packed[chunk, CHUNK : CHUNK + 1, :] = total_row

    copies = [
        start(packed.at[peer], parts.at[number], part_sems, number, (me, x * Z + peer))
        for number, peer in enumerate(z_peers)
    ]
    found = packed[z]
    for number, copy in enumerate(copies):
        copy.wait_recv()
        found = found + parts[number]
    sent = sent + copies

    gathered[seed] = found
    copies = [
        start(gathered.at[seed], gathered.at[seed], gather_sems, number, (me, peer))
        for number, peer in enumerate(seed_peers)
    ]
    for copy in copies:
        copy.wait_recv()
    sent = sent + copies

    for copy in sent:
        copy.wait_send()


def finish_kernel(cost_in, gathered, cost_out, blended, lines):
    cost_out[...] = cost_in[...]
    for chunk in range(Z):
        found = gathered[chunk] + gathered[Z + chunk]
        found = found / found[CHUNK : CHUNK + 1, :]
        lines[CHUNK * chunk : CHUNK * (chunk + 1), :] = found[0:CHUNK, :]
    turned = lines[...].T
    for robot in range(ROBOTS_HERE):
        for axis in range(3):
            for quarter in range(2):
                low = max(axis * GROUPS, quarter * CHUNK)
                high = min((axis + 1) * GROUPS, (quarter + 1) * CHUNK)
                if low < high:
                    source = (robot * 2 + quarter) * W
                    lane = 8 * (low - quarter * CHUNK)
                    first = 8 * (low - axis * GROUPS)
                    width = min(8 * (high - low), SPHERES - first)
                    blended[robot, axis, :, first : first + width] = turned[
                        source : source + W, lane : lane + width
                    ]


def in_vmem(count):
    return [pl.BlockSpec(memory_space=pltpu.VMEM)] * count


IN_SMEM = pl.BlockSpec(memory_space=pltpu.SMEM)


def local(centres, sphere_radius, counts, adjacency):
    dma = pltpu.SemaphoreType.DMA
    f32 = jnp.float32
    peers = ROBOT_DEVICES - 1
    rows = centres.transpose(1, 2, 0, 3).reshape(3 * SPHERES, ROBOTS_HERE, 2, LANES)
    rows = rows.transpose(0, 2, 1, 3).reshape(3 * SPHERES * 2 * ROBOTS_HERE, LANES)
    in_hbm = pl.BlockSpec(memory_space=pltpu.HBM)
    received, turned, self_cost, table = pl.pallas_call(
        spread_kernel,
        out_shape=(
            jax.ShapeDtypeStruct((ROBOT_DEVICES * ROWS + 8, LANES), f32),
            jax.ShapeDtypeStruct((ROBOT_DEVICES * ROWS, 8, LANES), f32),
            jax.ShapeDtypeStruct((2 * ROBOTS_HERE, LANES), f32),
            jax.ShapeDtypeStruct((TABLE_ROWS, LANES), jnp.int32),
        ),
        in_specs=[in_hbm] * 4,
        out_specs=tuple(in_vmem(4)),
        scratch_shapes=[
            pltpu.SMEM((ROBOTS_HERE,), jnp.int32),
            pltpu.VMEM(rows.shape, f32),
            pltpu.VMEM((ROBOTS_HERE, SPHERES), f32),
            pltpu.VMEM((ROBOTS_HERE, ROBOTS), jnp.int32),
            pltpu.VMEM((ROBOT_DEVICES * ROWS, LANES), f32),
            pltpu.VMEM((2 * ROBOTS_HERE, 4, 64, LANES), f32),
            pltpu.VMEM((ROBOTS_HERE, LANES), jnp.int32),
            pltpu.VMEM((ROBOT_DEVICES, ROBOTS_HERE, LANES), jnp.int32),
            pltpu.VMEM((ROBOTS, LANES), jnp.int32),
            dma((9,)),
            dma((peers,)),
            dma((peers,)),
            dma((peers,)),
            dma((peers,)),
        ],
        compiler_params=pltpu.CompilerParams(
            collective_id=0, has_side_effects=True, vmem_limit_bytes=GRANT
        ),
        name="spread",
    )(*[pltpu.with_memory_space_constraint(v, pltpu.HBM) for v in (counts, rows, sphere_radius, adjacency)])
    total = pl.pallas_call(
        cross_kernel,
        out_shape=jax.ShapeDtypeStruct((ROW_IDS + 1, 8, LANES), f32),
        in_specs=[IN_SMEM] + in_vmem(2),
        out_specs=in_vmem(1)[0],
        compiler_params=pltpu.CompilerParams(vmem_limit_bytes=GRANT),
        name="cross",
    )(table.reshape(TABLE_ROWS * LANES), received, turned)
    robot_cost, gathered = pl.pallas_call(
        blend_kernel,
        out_shape=(
            jax.ShapeDtypeStruct((ROBOTS_HERE, COLUMNS), f32),
            jax.ShapeDtypeStruct((2 * Z, CHUNK + 1, LANES), f32),
        ),
        in_specs=in_vmem(3),
        out_specs=tuple(in_vmem(2)),
        scratch_shapes=[
            pltpu.VMEM((ROBOTS, 8, LANES), f32),
            pltpu.VMEM((ROBOT_DEVICES, ROBOTS_HERE, LANES), f32),
            pltpu.VMEM((ROBOT_DEVICES, ROBOTS_HERE, LANES), f32),
            pltpu.VMEM((2, ROBOTS_HERE, LANES), f32),
            pltpu.VMEM((Z, CHUNK + 1, LANES), f32),
            pltpu.VMEM((Z - 1, CHUNK + 1, LANES), f32),
            dma((2, peers)),
            dma((2, Z - 1)),
            dma((2, 2 * Z - 1)),
        ],
        compiler_params=pltpu.CompilerParams(
            collective_id=1, has_side_effects=True, vmem_limit_bytes=GRANT
        ),
        name="blend",
    )(total, self_cost, rows)
    robot_cost, blended = pl.pallas_call(
        finish_kernel,
        out_shape=(
            jax.ShapeDtypeStruct((ROBOTS_HERE, COLUMNS), f32),
            jax.ShapeDtypeStruct((ROBOTS_HERE, 3, W, SPHERES), f32),
        ),
        in_specs=in_vmem(2),
        out_specs=tuple(in_vmem(2)),
        scratch_shapes=[pltpu.VMEM((LANES, LANES), f32)],
        compiler_params=pltpu.CompilerParams(vmem_limit_bytes=GRANT),
        name="finish",
    )(robot_cost, gathered)
    return robot_cost, blended.transpose(0, 1, 3, 2)


def solution(mesh):
    return jax.shard_map(
        local,
        mesh=mesh,
        in_specs=(P("robot", None, None, "seed"), P("robot", None), P("robot"), P("robot", None)),
        out_specs=(P("robot", "seed"), P("robot", None, None, None)),
        check_vma=False,
    )
```

```python
import functools
import math

import jax
import jax.numpy as jnp
from jax import lax
from jax.experimental import pallas as pl
from jax.experimental.pallas import tpu as pltpu
from jax.sharding import PartitionSpec as P

W = 32
SPHERES = 52
GROUPS = 7
FIRST_GROUPS = 4
ROBOTS_HERE = 2
ROBOT_DEVICES = 16
ROBOTS = ROBOTS_HERE * ROBOT_DEVICES
LANES = 128
COLUMNS = 256
PART = 16
ROWS = ROBOTS_HERE * GROUPS * 4
Z = 8
CHUNK = 11
COUNT_LANE = 32
ROOT = math.sqrt(math.log2(math.e))
FAR = 1.0e6
STEP_ROWS = 8
ROW_IDS = ROBOTS * GROUPS
WORDS = 56
STEPS_WORD = 56
ENTRY = 64
ORDER = ROBOTS * ENTRY
CASE_STEPS = ORDER + 32
CASE_START = ORDER + 40
LATE = ORDER + 48
LATE_STEPS = 12
LATE_SLOTS = 112
TABLE_ROWS = 24
EARLY_GROUPS = 3
GRANT = 16 * 1024 * 1024
MESH = pl.DeviceIdType.MESH


def iota(axis, shape=(8, LANES)):
    return lax.broadcasted_iota(jnp.int32, shape, axis)


def pair_argument(a, b):
    dx, dy, dz = a[0] - b[0], a[1] - b[1], a[2] - b[2]
    spread = a[3] + b[3]
    return (dx * dx + dy * dy + dz * dz) / (-spread * spread)


def pair_term(a, b):
    return jnp.exp2(pair_argument(a, b))


def centre_rows(ref, robot, axis, group, half):
    first = min(8 * group, SPHERES - 8)
    row = ((axis * SPHERES + first) * 2 + half) * ROBOTS_HERE + robot
    value = ref[pl.ds(row, 8, stride=2 * ROBOTS_HERE), :]
    return value if first == 8 * group else pltpu.roll(value, 4, 0)


def spread_kernel(
    counts_hbm,
    centres_hbm,
    radius_hbm,
    adjacency_hbm,
    recv_ref,
    turned_ref,
    self_ref,
    table_ref,
    counts_ref,
    centres_ref,
    radius_ref,
    adjacency_ref,
    send,
    swept,
    note_send,
    note_recv,
    note,
    load_sem,
    send_sem,
    recv_sem,
    note_send_sem,
    note_recv_sem,
):
    me = lax.axis_index("robot")
    seed = lax.axis_index("seed")
    peers = [lax.rem(me + step, ROBOT_DEVICES) for step in range(1, ROBOT_DEVICES)]

    loads = [
        pltpu.make_async_copy(counts_hbm, counts_ref, load_sem.at[0]),
        pltpu.make_async_copy(radius_hbm, radius_ref, load_sem.at[1]),
        pltpu.make_async_copy(adjacency_hbm, adjacency_ref, load_sem.at[2]),
    ]
    per_axis, early = 4 * SPHERES, 4 * 8 * EARLY_GROUPS
    for axis in range(3):
        at = pl.ds(axis * per_axis, early)
        loads.append(pltpu.make_async_copy(centres_hbm.at[at], centres_ref.at[at], load_sem.at[3 + axis]))
    for axis in range(3):
        at = pl.ds(axis * per_axis + early, per_axis - early)
        loads.append(pltpu.make_async_copy(centres_hbm.at[at], centres_ref.at[at], load_sem.at[6 + axis]))
    for load in loads:
        load.start()

    barrier = pltpu.get_barrier_semaphore()
    for peer in peers:
        pl.semaphore_signal(barrier, inc=1, device_id=(peer, seed), device_id_type=MESH)

    for load in loads[:6]:
        load.wait()

    sub, lane = iota(0), iota(1)
    part = lane // PART
    last_waypoint = lane % W == W - 1
    radius_lane = iota(1, (8, SPHERES))
    radius_sub = iota(0, (8, SPHERES))
    note_send[...] = jnp.zeros((ROBOTS_HERE, LANES), jnp.int32)
    note_send[:, 0:ROBOTS] = adjacency_ref[...]
    for robot in range(ROBOTS_HERE):
        note_send[robot : robot + 1, COUNT_LANE : COUNT_LANE + 1] = jnp.full((1, 1), counts_ref[robot], jnp.int32)
    for group in range(GROUPS):
        if group == EARLY_GROUPS:
            for load in loads[6:]:
                load.wait()
        for robot in range(ROBOTS_HERE):
            count = counts_ref[robot]
            radius_row = jnp.broadcast_to(radius_ref[robot : robot + 1, :], (8, SPHERES))
            number = (me * ROBOTS_HERE + robot) * 64 + 1
            radius = jnp.sum(
                jnp.where(radius_lane == radius_sub + 8 * group, radius_row, 0.0),
                axis=1,
                keepdims=True,
            )
            sphere = sub + 8 * group
            active = sphere < count
            far = FAR * (sphere + number).astype(jnp.float32)
            for half in range(2):
                out, square = [], None
                for axis in range(3):
                    here = centre_rows(centres_ref, robot, axis, group, half)
                    ahead = jnp.where(last_waypoint, here, pltpu.roll(here, LANES - 1, 1))
                    step = ahead - here
                    square = step * step if square is None else square + step * step
                    middle = (here + ahead) * (0.5 * ROOT)
                    out.append(jnp.where(active, middle, far if axis == 0 else 0.0))
                out.append(jnp.where(active, radius + 0.5 * jnp.sqrt(square + 1e-6), 1.0))
                for quantity in range(4):
                    value = out[quantity]
                    swept[half * ROBOTS_HERE + robot, quantity, 8 * group : 8 * group + 8, :] = value
                    value = pltpu.roll(value, 0, 1, stride=PART, stride_axis=0)
                    for bit in (1, 2, 4):
                        value = jnp.where(part & bit != 0, pltpu.roll(value, 8 - bit, 0), value)
                    row = (robot * GROUPS + group) * 4 + quantity
                    send[pl.ds(half * 8 * ROWS + row, 8, stride=ROWS), :] = value

    pl.semaphore_wait(barrier, ROBOT_DEVICES - 1)

    def slot_of(device):
        return (device // 8) * 8 + lax.rem(8 - lax.rem(device, 8), 8)

    def rows_of(slot):
        return pl.ds(pl.multiple_of(slot * ROWS, 8), ROWS)

    def send_note(number):
        return pltpu.make_async_remote_copy(
            src_ref=note_send,
            dst_ref=note_recv.at[me],
            send_sem=note_send_sem.at[number],
            recv_sem=note_recv_sem.at[number],
            device_id=(lax.rem(me + 1 + number, ROBOT_DEVICES), seed),
            device_id_type=MESH,
        )

    def send_rows(number):
        peer = lax.rem(me + 1 + number, ROBOT_DEVICES)
        return pltpu.make_async_remote_copy(
            src_ref=send.at[rows_of(slot_of(peer))],
            dst_ref=recv_ref.at[rows_of(me)],
            send_sem=send_sem.at[number],
            recv_sem=recv_sem.at[number],
            device_id=(peer, seed),
            device_id_type=MESH,
        )

    def for_peers(act):
        def one(number, carry):
            act(number)
            return carry

        lax.fori_loop(0, ROBOT_DEVICES - 1, one, 0)

    for_peers(lambda number: send_note(number).start())
    for_peers(lambda number: send_rows(number).start())
    note_recv[me] = note_send[...]
    recv_ref[rows_of(me), :] = send[rows_of(slot_of(me)), :]

    def turn_rows(device):
        row = pl.multiple_of(device * ROWS, 8)
        for n in range(ROWS):
            line = jnp.broadcast_to(recv_ref[pl.ds(row + n, 1), :], (8, LANES))
            turned_ref[row + n] = pltpu.roll(line, 0, 1, stride=PART, stride_axis=0)

    turn_rows(me)
    for index in range(2 * ROBOTS_HERE):
        robot = index % ROBOTS_HERE
        number = (me * ROBOTS_HERE + robot) * 64 + 1
        for quantity in range(4):
            fill = jnp.full((8, LANES), float(quantity == 3))
            if quantity == 0:
                fill = FAR * (sub + 8 * GROUPS + number).astype(jnp.float32)
            swept[index, quantity, 8 * GROUPS : 8 * GROUPS + 8, :] = fill

    def self_pairs(index, carry):
        sums = [jnp.zeros((8, LANES), jnp.float32) for _ in range(4)]
        turn = 0
        for group in range(GROUPS):
            first = [swept[index, q, 8 * group : 8 * group + 8, :] for q in range(4)]
            for apart in range(2, SPHERES - 8 * group):
                start = 8 * group + apart
                second = [swept[index, q, start : start + 8, :] for q in range(4)]
                sums[turn] = sums[turn] + pair_term(first, second)
                turn = (turn + 1) % 4
        total = jnp.sum((sums[0] + sums[1]) + (sums[2] + sums[3]), axis=0, keepdims=True)
        self_ref[pl.ds(index, 1), :] = total * (1.0 / (SPHERES * SPHERES))
        return carry

    lax.fori_loop(0, 2 * ROBOTS_HERE, self_pairs, 0)

    for_peers(lambda number: send_note(number).wait_recv())
    for device in range(ROBOT_DEVICES):
        note[ROBOTS_HERE * device : ROBOTS_HERE * (device + 1), :] = note_recv[device]
    shape = (ROBOTS, LANES)
    row, column = iota(0, shape), iota(1, shape)
    row_number = row.astype(jnp.float32)
    noted = note[...].astype(jnp.float32)
    link = jnp.where((column > row) & (column < ROBOTS) & (noted != 0.0), 1.0, 0.0)
    counts = jnp.sum(jnp.where(column == COUNT_LANE, noted, 0.0), axis=1, keepdims=True)
    groups = jnp.floor((counts + 7.0) * 0.125)

    def as_row(value):
        return jnp.sum(jnp.where(row == column, value, 0.0), axis=0, keepdims=True)

    length = link * as_row(groups)
    before = (iota(0, (LANES, LANES)) < iota(1, (LANES, LANES))).astype(jnp.float32)
    start = jnp.dot(length, before, preferred_element_type=jnp.float32)
    end = start + length
    words = jnp.zeros(shape, jnp.int32)
    for byte in range(4):
        place = (column * 4 + byte).astype(jnp.float32)
        listed = jnp.full(shape, float(ROW_IDS))
        for robot in range(1, ROBOTS):
            first, past = start[:, robot : robot + 1], end[:, robot : robot + 1]
            listed = jnp.where(
                (place >= first) & (place < past), place + (float(GROUPS * robot) - first), listed
            )
        words = words | (listed.astype(jnp.int32) << (8 * byte))
    steps = jnp.floor((jnp.sum(length, axis=1, keepdims=True) + (STEP_ROWS - 1.0)) * (1.0 / STEP_ROWS))
    words = jnp.where(column == STEPS_WORD, steps.astype(jnp.int32), words)
    note[...] = jnp.where(column < ENTRY, words, 0)
    table_ref[0:16, :] = note[pl.ds(0, 16, stride=2), :] + pltpu.roll(
        note[pl.ds(1, 16, stride=2), :], ENTRY, 1
    )
    busy = jnp.where(steps > 0.0, 1.0, 0.0)
    key = groups * 32.0 + row_number
    key_row, busy_row = as_row(key), as_row(busy)
    rank = jnp.sum(jnp.where(key_row < key, busy_row, 0.0), axis=1, keepdims=True)
    lane_number = column.astype(jnp.float32)
    last = jnp.sum(
        jnp.where((rank == lane_number) & (busy > 0.0), row_number, 0.0), axis=0, keepdims=True
    )
    steps_row = as_row(steps)
    rank_row = as_row(rank)
    done_before = jnp.sum(
        jnp.where((rank_row < rank) & (busy_row > 0.0), steps_row, 0.0), axis=1, keepdims=True
    )
    all_steps = jnp.sum(steps_row, axis=1, keepdims=True)
    late_start = jnp.maximum(all_steps - float(LATE_STEPS), 0.0)
    holds = (busy > 0.0) & (done_before <= late_start) & (late_start < done_before + steps)

    def held(value):
        return jnp.sum(jnp.where(holds, value, 0.0), axis=0, keepdims=True)

    line = iota(1, (1, LANES))
    for n, value in enumerate((held(rank), held(late_start - done_before), all_steps - late_start)):
        last = jnp.where(line == LATE - ORDER + n, value, last)
    for case in range(FIRST_GROUPS, GROUPS + 1):
        of_case = jnp.sum(jnp.where(groups == float(case), steps, 0.0), axis=0, keepdims=True)
        before_case = jnp.sum(jnp.where(groups < float(case), steps, 0.0), axis=0, keepdims=True)
        earlier = jnp.sum(jnp.where(groups < float(case), busy, 0.0), axis=0, keepdims=True)
        of_case = jnp.minimum(jnp.maximum(late_start - before_case, 0.0), of_case)
        last = jnp.where(line == CASE_STEPS - ORDER + case - FIRST_GROUPS, of_case, last)
        last = jnp.where(line == CASE_START - ORDER + case - FIRST_GROUPS, earlier, last)
    table_ref[16:24, :] = jnp.broadcast_to(last, (8, LANES)).astype(jnp.int32)
    recv_ref[ROBOT_DEVICES * ROWS : ROBOT_DEVICES * ROWS + 8, :] = jnp.where(
        sub == 0, -1000.0 * FAR, jnp.where(sub == 3, 1.0, 0.0)
    )

    def arrive(number):
        send_rows(number).wait_recv()
        turn_rows(lax.rem(me + ROBOT_DEVICES - 1 - number, ROBOT_DEVICES))

    for_peers(arrive)
    for_peers(lambda number: send_note(number).wait_send())
    for_peers(lambda number: send_rows(number).wait_send())


def pair_sums(rows, turned, groups, robot, ids):
    a_row = robot * (4 * GROUPS)
    sums = []
    for row_id in ids:
        b = [jnp.broadcast_to(rows[pl.ds(row_id * 4 + q, 1), :], (8, LANES)) for q in range(4)]
        terms = []
        for group in range(groups):
            a = [turned[a_row + (group * 4 + q)] for q in range(4)]
            terms.append(pair_term(a, b))
        while len(terms) > 1:
            terms = [p + q for p, q in zip(terms[0::2], terms[1::2])] + terms[len(terms) & ~1 :]
        sums.append(terms[0])
    own = sums
    while len(own) > 1:
        own = [p + q for p, q in zip(own[0::2], own[1::2])]
    return sums + own


def step_of(table, turn, step, there):
    robot = jnp.minimum(table[ORDER + turn], ROBOTS - 1)
    entry = robot * ENTRY
    nothing = jnp.int32(ROW_IDS * 0x01010101 - (1 << 32))
    words = [jnp.where(there, table[entry + 2 * step + n], nothing) for n in range(2)]
    ids = [lax.shift_right_logical(word, 8 * n) & 255 for word in words for n in range(4)]
    step = step + 1
    over = (step >= table[entry + STEPS_WORD]).astype(jnp.int32)
    return robot, ids, jnp.minimum(turn + over, ROBOTS - 1), step * (1 - over)


def cross_kernel(table, rows, turned, total):
    zero = jnp.zeros((8, LANES), jnp.float32)

    def clear(index, carry):
        for n in range(15):
            total[index * 15 + n] = zero
        return carry

    lax.fori_loop(0, (ROW_IDS + 1) // 15, clear, 0)

    def add_up(robot, ids, found):
        ids = ids + [robot * GROUPS]
        olds = [total[row_id] for row_id in ids]
        for row_id, old, new in zip(ids, olds, found):
            total[row_id] = old + new

    for groups in range(FIRST_GROUPS, GROUPS + 1):
        steps = table[CASE_STEPS + groups - FIRST_GROUPS]

        def two_steps_of(index, turn, step):
            robot, ids, turn, step = step_of(table, turn, step, 2 * index < steps)
            other, other_ids, turn, step = step_of(table, turn, step, 2 * index + 1 < steps)
            return turn, step, robot, other, *ids, *other_ids

        def two_steps(index, state, groups=groups, two_steps_of=two_steps_of):
            turn, step, robot, other, *ids = state
            ids, other_ids = ids[:STEP_ROWS], ids[STEP_ROWS:]
            found = pair_sums(rows, turned, groups, robot, ids)
            other_found = pair_sums(rows, turned, groups, other, other_ids)
            add_up(robot, ids, found)
            add_up(other, other_ids, other_found)
            return two_steps_of(index + 1, turn, step)

        start = jnp.minimum(table[CASE_START + groups - FIRST_GROUPS], ROBOTS - 1)
        lax.fori_loop(0, (steps + 1) >> 1, two_steps, two_steps_of(0, start, jnp.int32(0)))


def blend_kernel(
    table_ref,
    rows,
    turned,
    total,
    self_ref,
    centres_ref,
    robot_cost_ref,
    gathered,
    table,
    late,
    late_robot,
    sums,
    cost_ref,
    cost_recv,
    weight,
    packed,
    parts,
    table_sem,
    cost_sems,
    part_sems,
    gather_sems,
):
    me = lax.axis_index("robot")
    seed = lax.axis_index("seed")
    x, z = seed // Z, lax.rem(seed, Z)
    peers = [lax.rem(me + step, ROBOT_DEVICES) for step in range(1, ROBOT_DEVICES)]
    z_peers = [lax.rem(z + step, Z) for step in (4, 3, 5, 2, 6, 1, 7)]
    seed_peers = [lax.rem((1 - x) * Z + lax.rem(z + 4, Z), 2 * Z)] + [p for step in (3, 5, 2, 6, 1, 7, 0) for p in ([(1 - x) * Z + lax.rem(z + step, Z)])]
    seed_peers = seed_peers[:3] + [x * Z + lax.rem(z + 4, Z)] + seed_peers[3:5] + [x * Z + lax.rem(z + 3, Z), x * Z + lax.rem(z + 5, Z)] + seed_peers[5:7] + [x * Z + lax.rem(z + 2, Z), x * Z + lax.rem(z + 6, Z)] + seed_peers[7:] + [x * Z + lax.rem(z + 1, Z), x * Z + lax.rem(z + 7, Z)]

    barrier = pltpu.get_barrier_semaphore()
    for peer in peers:
        pl.semaphore_signal(barrier, inc=1, device_id=(peer, seed), device_id_type=MESH)
    for peer in seed_peers:
        pl.semaphore_signal(barrier, inc=1, device_id=(me, peer), device_id_type=MESH)

    load = pltpu.make_async_copy(table_ref, table, table_sem)
    load.start()
    line = iota(1, (1, LANES))
    for robot in range(ROBOTS):
        found = total[robot * GROUPS]
        for group in range(1, GROUPS):
            found = found + total[robot * GROUPS + group]
        sums[robot] = found
    for slot in range(9 * LATE_STEPS, LATE_SLOTS):
        late[slot] = jnp.zeros((8, LANES), jnp.float32)
        late_robot[slot : slot + 1, :] = jnp.zeros((1, LANES), jnp.float32)
    load.wait()
    late_count = table[LATE + 2]

    def two_steps(index, place):
        turn, step = place
        first = step_of(table, turn, step, 2 * index < late_count)
        second = step_of(table, *first[2:], 2 * index + 1 < late_count)
        slot = 2 * (STEP_ROWS + 1) * index
        for robot, ids, _, _ in (first, second):
            found = pair_sums(rows, turned, GROUPS, robot, ids)
            for value, holder in zip(found, [row_id // GROUPS for row_id in ids] + [robot]):
                late[slot] = value
                late_robot[pl.ds(slot, 1), :] = jnp.where(line == holder, 1.0, 0.0)
                slot = slot + 1
        return second[2:]

    lax.fori_loop(0, LATE_STEPS // 2, two_steps, (table[LATE], table[LATE + 1]))
    late_cost = lax.dot_general(
        late_robot[...],
        jnp.sum(late[...], axis=1),
        (((0,), (0,)), ((), ())),
        precision=lax.Precision.HIGHEST,
        preferred_element_type=jnp.float32,
    )
    cost = jnp.sum(sums[...], axis=1) + late_cost[0:ROBOTS, :]
    for shift in (64, 32, 16):
        cost = cost + pltpu.roll(cost, shift, 1)
    cost = cost * (1.0 / (SPHERES * SPHERES))
    for device in range(ROBOT_DEVICES):
        cost_ref[device] = cost[ROBOTS_HERE * device : ROBOTS_HERE * (device + 1), :]

    pl.semaphore_wait(barrier, ROBOT_DEVICES - 1 + 2 * Z - 1)

    def start(src, dst, sems, number, device):
        copy = pltpu.make_async_remote_copy(
            src_ref=src,
            dst_ref=dst,
            send_sem=sems.at[0, number],
            recv_sem=sems.at[1, number],
            device_id=device,
            device_id_type=MESH,
        )
        copy.start()
        return copy

    copies = [
        start(cost_ref.at[peer], cost_recv.at[me], cost_sems, number, (peer, seed))
        for number, peer in enumerate(peers)
    ]
    cost_recv[me] = cost_ref[me]
    for copy in copies:
        copy.wait_recv()
    sent = copies

    lane = iota(1, (ROBOTS_HERE, LANES))
    part = lane // PART
    for half in range(2):
        cost = self_ref[half * ROBOTS_HERE : (half + 1) * ROBOTS_HERE, :]
        for k in range(8):
            cost = cost + jnp.where(part == k, cost_recv[half * 8 + k], 0.0)
        robot_cost_ref[:, half * LANES : (half + 1) * LANES] = cost
        for bit in (1, 2, 4, 8, 16):
            cost = cost + jnp.where(
                lane & bit != 0, pltpu.roll(cost, bit, 1), pltpu.roll(cost, LANES - bit, 1)
            )
        weight[half] = 1.0 / (1.0 + cost)
    weights = weight[0] + weight[1]
    weights = weights + pltpu.roll(weights, 64, 1)
    weights = weights + pltpu.roll(weights, 32, 1)
    total_row = jnp.where(line < 64, weights[0:1, :], weights[1:2, :])

    quarter = iota(1) // W
    units = [[], []]
    for robot in range(ROBOTS_HERE):
        weights = [
            jnp.broadcast_to(weight[half, robot : robot + 1, :], (8, LANES)) for half in range(2)
        ]
        for axis in range(3):
            for group in range(GROUPS):
                value = (
                    centre_rows(centres_ref, robot, axis, group, 0) * weights[0]
                    + centre_rows(centres_ref, robot, axis, group, 1) * weights[1]
                )
                value = value + pltpu.roll(value, 64, 1)
                units[robot].append(value + pltpu.roll(value, 32, 1))
        units[robot].append(jnp.zeros((8, LANES), jnp.float32))
    for v in range(CHUNK):
        value = jnp.where(
            quarter < 2,
            jnp.where(quarter == 0, units[0][v], units[0][CHUNK + v]),
            jnp.where(quarter == 2, units[1][v], units[1][CHUNK + v]),
        )
        done = 0
        while done < 8:
            chunk, row = divmod(8 * v + done, CHUNK)
            length = min(8 - done, CHUNK - row)
            packed[chunk, row : row + length, :] = value[done : done + length, :]
            done += length
    for chunk in range(Z):
        packed[chunk, CHUNK : CHUNK + 1, :] = total_row

    copies = [
        start(packed.at[peer], parts.at[number], part_sems, number, (me, x * Z + peer))
        for number, peer in enumerate(z_peers)
    ]
    found = packed[z]
    for number, copy in enumerate(copies):
        copy.wait_recv()
        found = found + parts[number]
    sent = sent + copies

    gathered[seed] = found
    copies = [
        start(gathered.at[seed], gathered.at[seed], gather_sems, number, (me, peer))
        for number, peer in enumerate(seed_peers)
    ]
    for copy in copies:
        copy.wait_recv()
    sent = sent + copies

    for copy in sent:
        copy.wait_send()


def finish_kernel(cost_in, gathered, cost_out, blended, lines):
    cost_out[...] = cost_in[...]
    for chunk in range(Z):
        found = gathered[chunk] + gathered[Z + chunk]
        found = found / found[CHUNK : CHUNK + 1, :]
        lines[CHUNK * chunk : CHUNK * (chunk + 1), :] = found[0:CHUNK, :]
    turned = lines[...].T
    for robot in range(ROBOTS_HERE):
        for axis in range(3):
            for quarter in range(2):
                low = max(axis * GROUPS, quarter * CHUNK)
                high = min((axis + 1) * GROUPS, (quarter + 1) * CHUNK)
                if low < high:
                    source = (robot * 2 + quarter) * W
                    lane = 8 * (low - quarter * CHUNK)
                    first = 8 * (low - axis * GROUPS)
                    width = min(8 * (high - low), SPHERES - first)
                    blended[robot, axis, :, first : first + width] = turned[
                        source : source + W, lane : lane + width
                    ]


def in_vmem(count):
    return [pl.BlockSpec(memory_space=pltpu.VMEM)] * count


IN_SMEM = pl.BlockSpec(memory_space=pltpu.SMEM)


def local(centres, sphere_radius, counts, adjacency):
    dma = pltpu.SemaphoreType.DMA
    f32 = jnp.float32
    peers = ROBOT_DEVICES - 1
    rows = centres.transpose(1, 2, 0, 3).reshape(3 * SPHERES, ROBOTS_HERE, 2, LANES)
    rows = rows.transpose(0, 2, 1, 3).reshape(3 * SPHERES * 2 * ROBOTS_HERE, LANES)
    in_hbm = pl.BlockSpec(memory_space=pltpu.HBM)
    received, turned, self_cost, table = pl.pallas_call(
        spread_kernel,
        out_shape=(
            jax.ShapeDtypeStruct((ROBOT_DEVICES * ROWS + 8, LANES), f32),
            jax.ShapeDtypeStruct((ROBOT_DEVICES * ROWS, 8, LANES), f32),
            jax.ShapeDtypeStruct((2 * ROBOTS_HERE, LANES), f32),
            jax.ShapeDtypeStruct((TABLE_ROWS, LANES), jnp.int32),
        ),
        in_specs=[in_hbm] * 4,
        out_specs=tuple(in_vmem(4)),
        scratch_shapes=[
            pltpu.SMEM((ROBOTS_HERE,), jnp.int32),
            pltpu.VMEM(rows.shape, f32),
            pltpu.VMEM((ROBOTS_HERE, SPHERES), f32),
            pltpu.VMEM((ROBOTS_HERE, ROBOTS), jnp.int32),
            pltpu.VMEM((ROBOT_DEVICES * ROWS, LANES), f32),
            pltpu.VMEM((2 * ROBOTS_HERE, 4, 64, LANES), f32),
            pltpu.VMEM((ROBOTS_HERE, LANES), jnp.int32),
            pltpu.VMEM((ROBOT_DEVICES, ROBOTS_HERE, LANES), jnp.int32),
            pltpu.VMEM((ROBOTS, LANES), jnp.int32),
            dma((9,)),
            dma((peers,)),
            dma((peers,)),
            dma((peers,)),
            dma((peers,)),
        ],
        compiler_params=pltpu.CompilerParams(
            collective_id=0, has_side_effects=True, vmem_limit_bytes=GRANT
        ),
        name="spread",
    )(*[pltpu.with_memory_space_constraint(v, pltpu.HBM) for v in (counts, rows, sphere_radius, adjacency)])
    flat_table = table.reshape(TABLE_ROWS * LANES)
    total = pl.pallas_call(
        cross_kernel,
        out_shape=jax.ShapeDtypeStruct((ROW_IDS + 1, 8, LANES), f32),
        in_specs=[IN_SMEM] + in_vmem(2),
        out_specs=in_vmem(1)[0],
        compiler_params=pltpu.CompilerParams(vmem_limit_bytes=GRANT),
        name="cross",
    )(flat_table, received, turned)
    robot_cost, gathered = pl.pallas_call(
        blend_kernel,
        out_shape=(
            jax.ShapeDtypeStruct((ROBOTS_HERE, COLUMNS), f32),
            jax.ShapeDtypeStruct((2 * Z, CHUNK + 1, LANES), f32),
        ),
        in_specs=in_vmem(6),
        out_specs=tuple(in_vmem(2)),
        scratch_shapes=[
            pltpu.SMEM((TABLE_ROWS * LANES,), jnp.int32),
            pltpu.VMEM((LATE_SLOTS, 8, LANES), f32),
            pltpu.VMEM((LATE_SLOTS, LANES), f32),
            pltpu.VMEM((ROBOTS, 8, LANES), f32),
            pltpu.VMEM((ROBOT_DEVICES, ROBOTS_HERE, LANES), f32),
            pltpu.VMEM((ROBOT_DEVICES, ROBOTS_HERE, LANES), f32),
            pltpu.VMEM((2, ROBOTS_HERE, LANES), f32),
            pltpu.VMEM((Z, CHUNK + 1, LANES), f32),
            pltpu.VMEM((Z - 1, CHUNK + 1, LANES), f32),
            dma,
            dma((2, peers)),
            dma((2, Z - 1)),
            dma((2, 2 * Z - 1)),
        ],
        compiler_params=pltpu.CompilerParams(
            collective_id=1, has_side_effects=True, vmem_limit_bytes=GRANT
        ),
        name="blend",
    )(flat_table, received, turned, total, self_cost, rows)
    robot_cost, blended = pl.pallas_call(
        finish_kernel,
        out_shape=(
            jax.ShapeDtypeStruct((ROBOTS_HERE, COLUMNS), f32),
            jax.ShapeDtypeStruct((ROBOTS_HERE, 3, W, SPHERES), f32),
        ),
        in_specs=in_vmem(2),
        out_specs=tuple(in_vmem(2)),
        scratch_shapes=[pltpu.VMEM((LANES, LANES), f32)],
        compiler_params=pltpu.CompilerParams(vmem_limit_bytes=GRANT),
        name="finish",
    )(robot_cost, gathered)
    return robot_cost, blended.transpose(0, 1, 3, 2)


def solution(mesh):
    return jax.shard_map(
        local,
        mesh=mesh,
        in_specs=(P("robot", None, None, "seed"), P("robot", None), P("robot"), P("robot", None)),
        out_specs=(P("robot", "seed"), P("robot", None, None, None)),
        check_vma=False,
    )
```

```python
import functools
import math

import jax
import jax.numpy as jnp
from jax import lax
from jax.experimental import pallas as pl
from jax.experimental.pallas import tpu as pltpu
from jax.sharding import PartitionSpec as P

W = 32
SPHERES = 52
GROUPS = 7
FIRST_GROUPS = 4
ROBOTS_HERE = 2
ROBOT_DEVICES = 16
ROBOTS = ROBOTS_HERE * ROBOT_DEVICES
LANES = 128
COLUMNS = 256
PART = 16
ROWS = ROBOTS_HERE * GROUPS * 4
Z = 8
CHUNK = 11
COUNT_LANE = 32
ROOT = math.sqrt(math.log2(math.e))
FAR = 1.0e6
STEP_ROWS = 8
ROW_IDS = ROBOTS * GROUPS
WORDS = 56
STEPS_WORD = 56
ENTRY = 64
ORDER = ROBOTS * ENTRY
CASE_STEPS = ORDER + 32
CASE_START = ORDER + 40
LATE = ORDER + 48
LATE_STEPS = 24
LATE_SLOTS = 216
TABLE_ROWS = 24
EARLY_GROUPS = 3
GRANT = 16 * 1024 * 1024
MESH = pl.DeviceIdType.MESH


def iota(axis, shape=(8, LANES)):
    return lax.broadcasted_iota(jnp.int32, shape, axis)


def pair_argument(a, b):
    dx, dy, dz = a[0] - b[0], a[1] - b[1], a[2] - b[2]
    spread = a[3] + b[3]
    return (dx * dx + dy * dy + dz * dz) / (-spread * spread)


def pair_term(a, b):
    return jnp.exp2(pair_argument(a, b))


def centre_rows(ref, robot, axis, group, half):
    first = min(8 * group, SPHERES - 8)
    row = ((axis * SPHERES + first) * 2 + half) * ROBOTS_HERE + robot
    value = ref[pl.ds(row, 8, stride=2 * ROBOTS_HERE), :]
    return value if first == 8 * group else pltpu.roll(value, 4, 0)


def spread_kernel(
    counts_hbm,
    centres_hbm,
    radius_hbm,
    adjacency_hbm,
    recv_ref,
    turned_ref,
    self_ref,
    table_ref,
    counts_ref,
    centres_ref,
    radius_ref,
    adjacency_ref,
    send,
    swept,
    note_send,
    note_recv,
    note,
    load_sem,
    send_sem,
    recv_sem,
    note_send_sem,
    note_recv_sem,
):
    me = lax.axis_index("robot")
    seed = lax.axis_index("seed")
    peers = [lax.rem(me + step, ROBOT_DEVICES) for step in range(1, ROBOT_DEVICES)]

    loads = [
        pltpu.make_async_copy(counts_hbm, counts_ref, load_sem.at[0]),
        pltpu.make_async_copy(radius_hbm, radius_ref, load_sem.at[1]),
        pltpu.make_async_copy(adjacency_hbm, adjacency_ref, load_sem.at[2]),
    ]
    per_axis, early = 4 * SPHERES, 4 * 8 * EARLY_GROUPS
    for axis in range(3):
        at = pl.ds(axis * per_axis, early)
        loads.append(pltpu.make_async_copy(centres_hbm.at[at], centres_ref.at[at], load_sem.at[3 + axis]))
    for axis in range(3):
        at = pl.ds(axis * per_axis + early, per_axis - early)
        loads.append(pltpu.make_async_copy(centres_hbm.at[at], centres_ref.at[at], load_sem.at[6 + axis]))
    for load in loads:
        load.start()

    barrier = pltpu.get_barrier_semaphore()
    for peer in peers:
        pl.semaphore_signal(barrier, inc=1, device_id=(peer, seed), device_id_type=MESH)

    for load in loads[:6]:
        load.wait()

    sub, lane = iota(0), iota(1)
    part = lane // PART
    last_waypoint = lane % W == W - 1
    radius_lane = iota(1, (8, SPHERES))
    radius_sub = iota(0, (8, SPHERES))
    note_send[...] = jnp.zeros((ROBOTS_HERE, LANES), jnp.int32)
    note_send[:, 0:ROBOTS] = adjacency_ref[...]
    for robot in range(ROBOTS_HERE):
        note_send[robot : robot + 1, COUNT_LANE : COUNT_LANE + 1] = jnp.full((1, 1), counts_ref[robot], jnp.int32)
    for group in range(GROUPS):
        if group == EARLY_GROUPS:
            for load in loads[6:]:
                load.wait()
        for robot in range(ROBOTS_HERE):
            count = counts_ref[robot]
            radius_row = jnp.broadcast_to(radius_ref[robot : robot + 1, :], (8, SPHERES))
            number = (me * ROBOTS_HERE + robot) * 64 + 1
            radius = jnp.sum(
                jnp.where(radius_lane == radius_sub + 8 * group, radius_row, 0.0),
                axis=1,
                keepdims=True,
            )
            sphere = sub + 8 * group
            active = sphere < count
            far = FAR * (sphere + number).astype(jnp.float32)
            for half in range(2):
                out, square = [], None
                for axis in range(3):
                    here = centre_rows(centres_ref, robot, axis, group, half)
                    ahead = jnp.where(last_waypoint, here, pltpu.roll(here, LANES - 1, 1))
                    step = ahead - here
                    square = step * step if square is None else square + step * step
                    middle = (here + ahead) * (0.5 * ROOT)
                    out.append(jnp.where(active, middle, far if axis == 0 else 0.0))
                out.append(jnp.where(active, radius + 0.5 * jnp.sqrt(square + 1e-6), 1.0))
                for quantity in range(4):
                    value = out[quantity]
                    swept[half * ROBOTS_HERE + robot, quantity, 8 * group : 8 * group + 8, :] = value
                    value = pltpu.roll(value, 0, 1, stride=PART, stride_axis=0)
                    for bit in (1, 2, 4):
                        value = jnp.where(part & bit != 0, pltpu.roll(value, 8 - bit, 0), value)
                    row = (robot * GROUPS + group) * 4 + quantity
                    send[pl.ds(half * 8 * ROWS + row, 8, stride=ROWS), :] = value

    pl.semaphore_wait(barrier, ROBOT_DEVICES - 1)

    def slot_of(device):
        return (device // 8) * 8 + lax.rem(8 - lax.rem(device, 8), 8)

    def rows_of(slot):
        return pl.ds(pl.multiple_of(slot * ROWS, 8), ROWS)

    def send_note(number):
        return pltpu.make_async_remote_copy(
            src_ref=note_send,
            dst_ref=note_recv.at[me],
            send_sem=note_send_sem.at[number],
            recv_sem=note_recv_sem.at[number],
            device_id=(lax.rem(me + 1 + number, ROBOT_DEVICES), seed),
            device_id_type=MESH,
        )

    def send_rows(number):
        peer = lax.rem(me + 1 + number, ROBOT_DEVICES)
        return pltpu.make_async_remote_copy(
            src_ref=send.at[rows_of(slot_of(peer))],
            dst_ref=recv_ref.at[rows_of(me)],
            send_sem=send_sem.at[number],
            recv_sem=recv_sem.at[number],
            device_id=(peer, seed),
            device_id_type=MESH,
        )

    def for_peers(act):
        def one(number, carry):
            act(number)
            return carry

        lax.fori_loop(0, ROBOT_DEVICES - 1, one, 0)

    for_peers(lambda number: send_note(number).start())
    for_peers(lambda number: send_rows(number).start())
    note_recv[me] = note_send[...]
    recv_ref[rows_of(me), :] = send[rows_of(slot_of(me)), :]

    def turn_rows(device):
        row = pl.multiple_of(device * ROWS, 8)
        for n in range(ROWS):
            line = jnp.broadcast_to(recv_ref[pl.ds(row + n, 1), :], (8, LANES))
            turned_ref[row + n] = pltpu.roll(line, 0, 1, stride=PART, stride_axis=0)

    turn_rows(me)
    for index in range(2 * ROBOTS_HERE):
        robot = index % ROBOTS_HERE
        number = (me * ROBOTS_HERE + robot) * 64 + 1
        for quantity in range(4):
            fill = jnp.full((8, LANES), float(quantity == 3))
            if quantity == 0:
                fill = FAR * (sub + 8 * GROUPS + number).astype(jnp.float32)
            swept[index, quantity, 8 * GROUPS : 8 * GROUPS + 8, :] = fill

    def self_pairs(index, carry):
        sums = [jnp.zeros((8, LANES), jnp.float32) for _ in range(4)]
        turn = 0
        for group in range(GROUPS):
            first = [swept[index, q, 8 * group : 8 * group + 8, :] for q in range(4)]
            for apart in range(2, SPHERES - 8 * group):
                start = 8 * group + apart
                second = [swept[index, q, start : start + 8, :] for q in range(4)]
                sums[turn] = sums[turn] + pair_term(first, second)
                turn = (turn + 1) % 4
        total = jnp.sum((sums[0] + sums[1]) + (sums[2] + sums[3]), axis=0, keepdims=True)
        self_ref[pl.ds(index, 1), :] = total * (1.0 / (SPHERES * SPHERES))
        return carry

    lax.fori_loop(0, 2 * ROBOTS_HERE, self_pairs, 0)

    for_peers(lambda number: send_note(number).wait_recv())
    for device in range(ROBOT_DEVICES):
        note[ROBOTS_HERE * device : ROBOTS_HERE * (device + 1), :] = note_recv[device]
    shape = (ROBOTS, LANES)
    row, column = iota(0, shape), iota(1, shape)
    row_number = row.astype(jnp.float32)
    noted = note[...].astype(jnp.float32)
    link = jnp.where((column > row) & (column < ROBOTS) & (noted != 0.0), 1.0, 0.0)
    counts = jnp.sum(jnp.where(column == COUNT_LANE, noted, 0.0), axis=1, keepdims=True)
    groups = jnp.floor((counts + 7.0) * 0.125)

    def as_row(value):
        return jnp.sum(jnp.where(row == column, value, 0.0), axis=0, keepdims=True)

    length = link * as_row(groups)
    before = (iota(0, (LANES, LANES)) < iota(1, (LANES, LANES))).astype(jnp.float32)
    start = jnp.dot(length, before, preferred_element_type=jnp.float32)
    end = start + length
    words = jnp.zeros(shape, jnp.int32)
    for byte in range(4):
        place = (column * 4 + byte).astype(jnp.float32)
        listed = jnp.full(shape, float(ROW_IDS))
        for robot in range(1, ROBOTS):
            first, past = start[:, robot : robot + 1], end[:, robot : robot + 1]
            listed = jnp.where(
                (place >= first) & (place < past), place + (float(GROUPS * robot) - first), listed
            )
        words = words | (listed.astype(jnp.int32) << (8 * byte))
    steps = jnp.floor((jnp.sum(length, axis=1, keepdims=True) + (STEP_ROWS - 1.0)) * (1.0 / STEP_ROWS))
    words = jnp.where(column == STEPS_WORD, steps.astype(jnp.int32), words)
    note[...] = jnp.where(column < ENTRY, words, 0)
    table_ref[0:16, :] = note[pl.ds(0, 16, stride=2), :] + pltpu.roll(
        note[pl.ds(1, 16, stride=2), :], ENTRY, 1
    )
    busy = jnp.where(steps > 0.0, 1.0, 0.0)
    key = groups * 32.0 + row_number
    key_row, busy_row = as_row(key), as_row(busy)
    rank = jnp.sum(jnp.where(key_row < key, busy_row, 0.0), axis=1, keepdims=True)
    lane_number = column.astype(jnp.float32)
    last = jnp.sum(
        jnp.where((rank == lane_number) & (busy > 0.0), row_number, 0.0), axis=0, keepdims=True
    )
    steps_row = as_row(steps)
    rank_row = as_row(rank)
    done_before = jnp.sum(
        jnp.where((rank_row < rank) & (busy_row > 0.0), steps_row, 0.0), axis=1, keepdims=True
    )
    all_steps = jnp.sum(steps_row, axis=1, keepdims=True)
    late_start = jnp.maximum(all_steps - float(LATE_STEPS), 0.0)
    holds = (busy > 0.0) & (done_before <= late_start) & (late_start < done_before + steps)

    def held(value):
        return jnp.sum(jnp.where(holds, value, 0.0), axis=0, keepdims=True)

    line = iota(1, (1, LANES))
    for n, value in enumerate((held(rank), held(late_start - done_before), all_steps - late_start)):
        last = jnp.where(line == LATE - ORDER + n, value, last)
    for case in range(FIRST_GROUPS, GROUPS + 1):
        of_case = jnp.sum(jnp.where(groups == float(case), steps, 0.0), axis=0, keepdims=True)
        before_case = jnp.sum(jnp.where(groups < float(case), steps, 0.0), axis=0, keepdims=True)
        earlier = jnp.sum(jnp.where(groups < float(case), busy, 0.0), axis=0, keepdims=True)
        of_case = jnp.minimum(jnp.maximum(late_start - before_case, 0.0), of_case)
        last = jnp.where(line == CASE_STEPS - ORDER + case - FIRST_GROUPS, of_case, last)
        last = jnp.where(line == CASE_START - ORDER + case - FIRST_GROUPS, earlier, last)
    table_ref[16:24, :] = jnp.broadcast_to(last, (8, LANES)).astype(jnp.int32)
    recv_ref[ROBOT_DEVICES * ROWS : ROBOT_DEVICES * ROWS + 8, :] = jnp.where(
        sub == 0, -1000.0 * FAR, jnp.where(sub == 3, 1.0, 0.0)
    )

    def arrive(number):
        send_rows(number).wait_recv()
        turn_rows(lax.rem(me + ROBOT_DEVICES - 1 - number, ROBOT_DEVICES))

    for_peers(arrive)
    for_peers(lambda number: send_note(number).wait_send())
    for_peers(lambda number: send_rows(number).wait_send())


def pair_sums(rows, turned, groups, robot, ids):
    a_row = robot * (4 * GROUPS)
    sums = []
    for row_id in ids:
        b = [jnp.broadcast_to(rows[pl.ds(row_id * 4 + q, 1), :], (8, LANES)) for q in range(4)]
        terms = []
        for group in range(groups):
            a = [turned[a_row + (group * 4 + q)] for q in range(4)]
            terms.append(pair_term(a, b))
        while len(terms) > 1:
            terms = [p + q for p, q in zip(terms[0::2], terms[1::2])] + terms[len(terms) & ~1 :]
        sums.append(terms[0])
    own = sums
    while len(own) > 1:
        own = [p + q for p, q in zip(own[0::2], own[1::2])]
    return sums + own


def step_of(table, turn, step, there):
    robot = jnp.minimum(table[ORDER + turn], ROBOTS - 1)
    entry = robot * ENTRY
    nothing = jnp.int32(ROW_IDS * 0x01010101 - (1 << 32))
    words = [jnp.where(there, table[entry + 2 * step + n], nothing) for n in range(2)]
    ids = [lax.shift_right_logical(word, 8 * n) & 255 for word in words for n in range(4)]
    step = step + 1
    over = (step >= table[entry + STEPS_WORD]).astype(jnp.int32)
    return robot, ids, jnp.minimum(turn + over, ROBOTS - 1), step * (1 - over)


def cross_kernel(table, rows, turned, total):
    zero = jnp.zeros((8, LANES), jnp.float32)

    def clear(index, carry):
        for n in range(15):
            total[index * 15 + n] = zero
        return carry

    lax.fori_loop(0, (ROW_IDS + 1) // 15, clear, 0)

    def add_up(robot, ids, found):
        ids = ids + [robot * GROUPS]
        olds = [total[row_id] for row_id in ids]
        for row_id, old, new in zip(ids, olds, found):
            total[row_id] = old + new

    for groups in range(FIRST_GROUPS, GROUPS + 1):
        steps = table[CASE_STEPS + groups - FIRST_GROUPS]

        def two_steps_of(index, turn, step):
            robot, ids, turn, step = step_of(table, turn, step, 2 * index < steps)
            other, other_ids, turn, step = step_of(table, turn, step, 2 * index + 1 < steps)
            return turn, step, robot, other, *ids, *other_ids

        def two_steps(index, state, groups=groups, two_steps_of=two_steps_of):
            turn, step, robot, other, *ids = state
            ids, other_ids = ids[:STEP_ROWS], ids[STEP_ROWS:]
            found = pair_sums(rows, turned, groups, robot, ids)
            other_found = pair_sums(rows, turned, groups, other, other_ids)
            add_up(robot, ids, found)
            add_up(other, other_ids, other_found)
            return two_steps_of(index + 1, turn, step)

        start = jnp.minimum(table[CASE_START + groups - FIRST_GROUPS], ROBOTS - 1)
        lax.fori_loop(0, (steps + 1) >> 1, two_steps, two_steps_of(0, start, jnp.int32(0)))


def blend_kernel(
    table_ref,
    rows,
    turned,
    total,
    self_ref,
    centres_ref,
    robot_cost_ref,
    gathered,
    table,
    late,
    late_robot,
    sums,
    cost_ref,
    cost_recv,
    weight,
    packed,
    parts,
    table_sem,
    cost_sems,
    part_sems,
    gather_sems,
):
    me = lax.axis_index("robot")
    seed = lax.axis_index("seed")
    x, z = seed // Z, lax.rem(seed, Z)
    peers = [lax.rem(me + step, ROBOT_DEVICES) for step in range(1, ROBOT_DEVICES)]
    z_peers = [lax.rem(z + step, Z) for step in (4, 3, 5, 2, 6, 1, 7)]
    seed_peers = [lax.rem((1 - x) * Z + lax.rem(z + 4, Z), 2 * Z)] + [p for step in (3, 5, 2, 6, 1, 7, 0) for p in ([(1 - x) * Z + lax.rem(z + step, Z)])]
    seed_peers = seed_peers[:3] + [x * Z + lax.rem(z + 4, Z)] + seed_peers[3:5] + [x * Z + lax.rem(z + 3, Z), x * Z + lax.rem(z + 5, Z)] + seed_peers[5:7] + [x * Z + lax.rem(z + 2, Z), x * Z + lax.rem(z + 6, Z)] + seed_peers[7:] + [x * Z + lax.rem(z + 1, Z), x * Z + lax.rem(z + 7, Z)]

    barrier = pltpu.get_barrier_semaphore()

    def greet(number, carry):
        peer = lax.rem(me + 1 + lax.rem(number + 7, ROBOT_DEVICES - 1), ROBOT_DEVICES)
        pl.semaphore_signal(barrier, inc=1, device_id=(peer, seed), device_id_type=MESH)
        return carry

    lax.fori_loop(0, ROBOT_DEVICES - 1, greet, 0)

    def greet_seed(number, carry):
        peer = lax.rem(seed + 1 + number, 2 * Z)
        pl.semaphore_signal(barrier, inc=1, device_id=(me, peer), device_id_type=MESH)
        return carry

    lax.fori_loop(0, 2 * Z - 1, greet_seed, 0)

    load = pltpu.make_async_copy(table_ref, table, table_sem)
    load.start()
    line = iota(1, (1, LANES))
    for robot in range(ROBOTS):
        found = total[robot * GROUPS]
        for group in range(1, GROUPS):
            found = found + total[robot * GROUPS + group]
        sums[robot] = found
    for slot in range(9 * LATE_STEPS, LATE_SLOTS):
        late[slot] = jnp.zeros((8, LANES), jnp.float32)
        late_robot[slot : slot + 1, :] = jnp.zeros((1, LANES), jnp.float32)
    load.wait()
    late_count = table[LATE + 2]

    def two_steps(index, place):
        turn, step = place
        first = step_of(table, turn, step, 2 * index < late_count)
        second = step_of(table, *first[2:], 2 * index + 1 < late_count)
        slot = 2 * (STEP_ROWS + 1) * index
        for robot, ids, _, _ in (first, second):
            found = pair_sums(rows, turned, GROUPS, robot, ids)
            for value, holder in zip(found, [row_id // GROUPS for row_id in ids] + [robot]):
                late[slot] = value
                late_robot[pl.ds(slot, 1), :] = jnp.where(line == holder, 1.0, 0.0)
                slot = slot + 1
        return second[2:]

    lax.fori_loop(0, LATE_STEPS // 2, two_steps, (table[LATE], table[LATE + 1]))
    late_cost = lax.dot_general(
        late_robot[...],
        jnp.sum(late[...], axis=1),
        (((0,), (0,)), ((), ())),
        precision=lax.Precision.HIGHEST,
        preferred_element_type=jnp.float32,
    )
    cost = jnp.sum(sums[...], axis=1) + late_cost[0:ROBOTS, :]
    for shift in (64, 32, 16):
        cost = cost + pltpu.roll(cost, shift, 1)
    cost = cost * (1.0 / (SPHERES * SPHERES))
    for device in range(ROBOT_DEVICES):
        cost_ref[device] = cost[ROBOTS_HERE * device : ROBOTS_HERE * (device + 1), :]

    pl.semaphore_wait(barrier, ROBOT_DEVICES - 1 + 2 * Z - 1)

    def start(src, dst, sems, number, device):
        copy = pltpu.make_async_remote_copy(
            src_ref=src,
            dst_ref=dst,
            send_sem=sems.at[0, number],
            recv_sem=sems.at[1, number],
            device_id=device,
            device_id_type=MESH,
        )
        copy.start()
        return copy

    copies = [
        start(cost_ref.at[peer], cost_recv.at[me], cost_sems, number, (peer, seed))
        for number, peer in enumerate(peers)
    ]
    cost_recv[me] = cost_ref[me]
    for copy in copies:
        copy.wait_recv()
    sent = copies

    lane = iota(1, (ROBOTS_HERE, LANES))
    part = lane // PART
    for half in range(2):
        cost = self_ref[half * ROBOTS_HERE : (half + 1) * ROBOTS_HERE, :]
        for k in range(8):
            cost = cost + jnp.where(part == k, cost_recv[half * 8 + k], 0.0)
        robot_cost_ref[:, half * LANES : (half + 1) * LANES] = cost
        for bit in (1, 2, 4, 8, 16):
            cost = cost + jnp.where(
                lane & bit != 0, pltpu.roll(cost, bit, 1), pltpu.roll(cost, LANES - bit, 1)
            )
        weight[half] = 1.0 / (1.0 + cost)
    weights = weight[0] + weight[1]
    weights = weights + pltpu.roll(weights, 64, 1)
    weights = weights + pltpu.roll(weights, 32, 1)
    total_row = jnp.where(line < 64, weights[0:1, :], weights[1:2, :])

    quarter = iota(1) // W
    units = [[], []]
    for robot in range(ROBOTS_HERE):
        weights = [
            jnp.broadcast_to(weight[half, robot : robot + 1, :], (8, LANES)) for half in range(2)
        ]
        for axis in range(3):
            for group in range(GROUPS):
                value = (
                    centre_rows(centres_ref, robot, axis, group, 0) * weights[0]
                    + centre_rows(centres_ref, robot, axis, group, 1) * weights[1]
                )
                value = value + pltpu.roll(value, 64, 1)
                units[robot].append(value + pltpu.roll(value, 32, 1))
        units[robot].append(jnp.zeros((8, LANES), jnp.float32))
    for v in range(CHUNK):
        value = jnp.where(
            quarter < 2,
            jnp.where(quarter == 0, units[0][v], units[0][CHUNK + v]),
            jnp.where(quarter == 2, units[1][v], units[1][CHUNK + v]),
        )
        done = 0
        while done < 8:
            chunk, row = divmod(8 * v + done, CHUNK)
            length = min(8 - done, CHUNK - row)
            packed[chunk, row : row + length, :] = value[done : done + length, :]
            done += length
    for chunk in range(Z):
        packed[chunk, CHUNK : CHUNK + 1, :] = total_row

    copies = [
        start(packed.at[peer], parts.at[number], part_sems, number, (me, x * Z + peer))
        for number, peer in enumerate(z_peers)
    ]
    found = packed[z]
    for number, copy in enumerate(copies):
        copy.wait_recv()
        found = found + parts[number]
    sent = sent + copies

    gathered[seed] = found
    copies = [
        start(gathered.at[seed], gathered.at[seed], gather_sems, number, (me, peer))
        for number, peer in enumerate(seed_peers)
    ]
    for copy in copies:
        copy.wait_recv()
    sent = sent + copies

    for copy in sent:
        copy.wait_send()


def finish_kernel(cost_in, gathered, cost_out, blended, lines):
    cost_out[...] = cost_in[...]
    for chunk in range(Z):
        found = gathered[chunk] + gathered[Z + chunk]
        found = found / found[CHUNK : CHUNK + 1, :]
        lines[CHUNK * chunk : CHUNK * (chunk + 1), :] = found[0:CHUNK, :]
    turned = lines[...].T
    for robot in range(ROBOTS_HERE):
        for axis in range(3):
            for quarter in range(2):
                low = max(axis * GROUPS, quarter * CHUNK)
                high = min((axis + 1) * GROUPS, (quarter + 1) * CHUNK)
                if low < high:
                    source = (robot * 2 + quarter) * W
                    lane = 8 * (low - quarter * CHUNK)
                    first = 8 * (low - axis * GROUPS)
                    width = min(8 * (high - low), SPHERES - first)
                    blended[robot, axis, :, first : first + width] = turned[
                        source : source + W, lane : lane + width
                    ]


def in_vmem(count):
    return [pl.BlockSpec(memory_space=pltpu.VMEM)] * count


IN_SMEM = pl.BlockSpec(memory_space=pltpu.SMEM)


def local(centres, sphere_radius, counts, adjacency):
    dma = pltpu.SemaphoreType.DMA
    f32 = jnp.float32
    peers = ROBOT_DEVICES - 1
    rows = centres.transpose(1, 2, 0, 3).reshape(3 * SPHERES, ROBOTS_HERE, 2, LANES)
    rows = rows.transpose(0, 2, 1, 3).reshape(3 * SPHERES * 2 * ROBOTS_HERE, LANES)
    in_hbm = pl.BlockSpec(memory_space=pltpu.HBM)
    received, turned, self_cost, table = pl.pallas_call(
        spread_kernel,
        out_shape=(
            jax.ShapeDtypeStruct((ROBOT_DEVICES * ROWS + 8, LANES), f32),
            jax.ShapeDtypeStruct((ROBOT_DEVICES * ROWS, 8, LANES), f32),
            jax.ShapeDtypeStruct((2 * ROBOTS_HERE, LANES), f32),
            jax.ShapeDtypeStruct((TABLE_ROWS, LANES), jnp.int32),
        ),
        in_specs=[in_hbm] * 4,
        out_specs=tuple(in_vmem(4)),
        scratch_shapes=[
            pltpu.SMEM((ROBOTS_HERE,), jnp.int32),
            pltpu.VMEM(rows.shape, f32),
            pltpu.VMEM((ROBOTS_HERE, SPHERES), f32),
            pltpu.VMEM((ROBOTS_HERE, ROBOTS), jnp.int32),
            pltpu.VMEM((ROBOT_DEVICES * ROWS, LANES), f32),
            pltpu.VMEM((2 * ROBOTS_HERE, 4, 64, LANES), f32),
            pltpu.VMEM((ROBOTS_HERE, LANES), jnp.int32),
            pltpu.VMEM((ROBOT_DEVICES, ROBOTS_HERE, LANES), jnp.int32),
            pltpu.VMEM((ROBOTS, LANES), jnp.int32),
            dma((9,)),
            dma((peers,)),
            dma((peers,)),
            dma((peers,)),
            dma((peers,)),
        ],
        compiler_params=pltpu.CompilerParams(
            collective_id=0, has_side_effects=True, vmem_limit_bytes=GRANT
        ),
        name="spread",
    )(*[pltpu.with_memory_space_constraint(v, pltpu.HBM) for v in (counts, rows, sphere_radius, adjacency)])
    flat_table = table.reshape(TABLE_ROWS * LANES)
    total = pl.pallas_call(
        cross_kernel,
        out_shape=jax.ShapeDtypeStruct((ROW_IDS + 1, 8, LANES), f32),
        in_specs=[IN_SMEM] + in_vmem(2),
        out_specs=in_vmem(1)[0],
        compiler_params=pltpu.CompilerParams(vmem_limit_bytes=GRANT),
        name="cross",
    )(flat_table, received, turned)
    robot_cost, gathered = pl.pallas_call(
        blend_kernel,
        out_shape=(
            jax.ShapeDtypeStruct((ROBOTS_HERE, COLUMNS), f32),
            jax.ShapeDtypeStruct((2 * Z, CHUNK + 1, LANES), f32),
        ),
        in_specs=in_vmem(6),
        out_specs=tuple(in_vmem(2)),
        scratch_shapes=[
            pltpu.SMEM((TABLE_ROWS * LANES,), jnp.int32),
            pltpu.VMEM((LATE_SLOTS, 8, LANES), f32),
            pltpu.VMEM((LATE_SLOTS, LANES), f32),
            pltpu.VMEM((ROBOTS, 8, LANES), f32),
            pltpu.VMEM((ROBOT_DEVICES, ROBOTS_HERE, LANES), f32),
            pltpu.VMEM((ROBOT_DEVICES, ROBOTS_HERE, LANES), f32),
            pltpu.VMEM((2, ROBOTS_HERE, LANES), f32),
            pltpu.VMEM((Z, CHUNK + 1, LANES), f32),
            pltpu.VMEM((Z - 1, CHUNK + 1, LANES), f32),
            dma,
            dma((2, peers)),
            dma((2, Z - 1)),
            dma((2, 2 * Z - 1)),
        ],
        compiler_params=pltpu.CompilerParams(
            collective_id=1, has_side_effects=True, vmem_limit_bytes=GRANT
        ),
        name="blend",
    )(flat_table, received, turned, total, self_cost, rows)
    robot_cost, blended = pl.pallas_call(
        finish_kernel,
        out_shape=(
            jax.ShapeDtypeStruct((ROBOTS_HERE, COLUMNS), f32),
            jax.ShapeDtypeStruct((ROBOTS_HERE, 3, W, SPHERES), f32),
        ),
        in_specs=in_vmem(2),
        out_specs=tuple(in_vmem(2)),
        scratch_shapes=[pltpu.VMEM((LANES, LANES), f32)],
        compiler_params=pltpu.CompilerParams(vmem_limit_bytes=GRANT),
        name="finish",
    )(robot_cost, gathered)
    return robot_cost, blended.transpose(0, 1, 3, 2)


def solution(mesh):
    return jax.shard_map(
        local,
        mesh=mesh,
        in_specs=(P("robot", None, None, "seed"), P("robot", None), P("robot"), P("robot", None)),
        out_specs=(P("robot", "seed"), P("robot", None, None, None)),
        check_vma=False,
    )
```

```python
import functools
import math

import jax
import jax.numpy as jnp
from jax import lax
from jax.experimental import pallas as pl
from jax.experimental.pallas import tpu as pltpu
from jax.sharding import PartitionSpec as P

W = 32
SPHERES = 52
GROUPS = 7
FIRST_GROUPS = 4
ROBOTS_HERE = 2
ROBOT_DEVICES = 16
ROBOTS = ROBOTS_HERE * ROBOT_DEVICES
LANES = 128
COLUMNS = 256
PART = 16
ROWS = ROBOTS_HERE * GROUPS * 4
AXIS_ROWS = 14
SHARED, NEXT = 6, 7
RADII = 3 * AXIS_ROWS
MESSAGE = RADII + 2
Z = 8
CHUNK = 11
COUNT_LANE = 32
ROOT = math.sqrt(math.log2(math.e))
FAR = 1.0e6
STEP_ROWS = 8
ROW_IDS = ROBOTS * GROUPS
WORDS = 56
STEPS_WORD = 56
ENTRY = 64
ORDER = ROBOTS * ENTRY
CASE_STEPS = ORDER + 32
CASE_START = ORDER + 40
LATE = ORDER + 48
LATE_STEPS = 24
LATE_SLOTS = 216
TABLE_ROWS = 24
EARLY_GROUPS = 3
GRANT = 16 * 1024 * 1024
MESH = pl.DeviceIdType.MESH


def iota(axis, shape=(8, LANES)):
    return lax.broadcasted_iota(jnp.int32, shape, axis)


def pair_argument(a, b):
    dx, dy, dz = a[0] - b[0], a[1] - b[1], a[2] - b[2]
    spread = a[3] + b[3]
    return (dx * dx + dy * dy + dz * dz) / (-spread * spread)


def pair_term(a, b):
    return jnp.exp2(pair_argument(a, b))


def centre_rows(ref, robot, axis, group, half):
    first = min(8 * group, SPHERES - 8)
    row = ((axis * SPHERES + first) * 2 + half) * ROBOTS_HERE + robot
    value = ref[pl.ds(row, 8, stride=2 * ROBOTS_HERE), :]
    return value if first == 8 * group else pltpu.roll(value, 4, 0)


def spread_kernel(
    counts_hbm,
    centres_hbm,
    radius_hbm,
    adjacency_hbm,
    recv_ref,
    turned_ref,
    self_ref,
    table_ref,
    counts_ref,
    centres_ref,
    radius_ref,
    adjacency_ref,
    send,
    recv,
    swept,
    note_send,
    note_recv,
    note,
    load_sem,
    send_sem,
    recv_sem,
    note_send_sem,
    note_recv_sem,
):
    me = lax.axis_index("robot")
    seed = lax.axis_index("seed")
    peers = [lax.rem(me + step, ROBOT_DEVICES) for step in range(1, ROBOT_DEVICES)]

    loads = [
        pltpu.make_async_copy(counts_hbm, counts_ref, load_sem.at[0]),
        pltpu.make_async_copy(radius_hbm, radius_ref, load_sem.at[1]),
        pltpu.make_async_copy(adjacency_hbm, adjacency_ref, load_sem.at[2]),
    ]
    per_axis, early = 4 * SPHERES, 4 * 8 * EARLY_GROUPS
    for axis in range(3):
        at = pl.ds(axis * per_axis, early)
        loads.append(pltpu.make_async_copy(centres_hbm.at[at], centres_ref.at[at], load_sem.at[3 + axis]))
    for axis in range(3):
        at = pl.ds(axis * per_axis + early, per_axis - early)
        loads.append(pltpu.make_async_copy(centres_hbm.at[at], centres_ref.at[at], load_sem.at[6 + axis]))
    for load in loads:
        load.start()

    barrier = pltpu.get_barrier_semaphore()
    for peer in peers:
        pl.semaphore_signal(barrier, inc=1, device_id=(peer, seed), device_id_type=MESH)

    for load in loads[:6]:
        load.wait()

    sub, lane = iota(0), iota(1)
    part = lane // PART
    spot = lane % PART
    last_waypoint = lane % W == W - 1
    radius_lane = iota(1, (8, SPHERES))
    radius_sub = iota(0, (8, SPHERES))
    numbers = [(me * ROBOTS_HERE + robot) * 64 + 1 for robot in range(ROBOTS_HERE)]

    def ahead_of(here):
        return jnp.where(last_waypoint, here, pltpu.roll(here, LANES - 1, 1))

    def radius_column(robot, group):
        row = jnp.broadcast_to(radius_ref[robot : robot + 1, :], (8, SPHERES))
        return jnp.sum(jnp.where(radius_lane == radius_sub + 8 * group, row, 0.0), axis=1, keepdims=True)

    def by_part(value):
        value = pltpu.roll(value, 0, 1, stride=PART, stride_axis=0)
        for bit in (1, 2, 4):
            value = jnp.where(part & bit != 0, pltpu.roll(value, 8 - bit, 0), value)
        return value

    note_send[...] = jnp.zeros((ROBOTS_HERE, LANES), jnp.int32)
    note_send[:, 0:ROBOTS] = adjacency_ref[...]
    for robot in range(ROBOTS_HERE):
        note_send[robot : robot + 1, COUNT_LANE : COUNT_LANE + 1] = jnp.full((1, 1), counts_ref[robot], jnp.int32)
    def raw(robot, axis, group, half):
        here = centre_rows(centres_ref, robot, axis, group, half)
        sphere = sub + 8 * group
        far = FAR * (sphere + numbers[robot]).astype(jnp.float32) if axis == 0 else 0.0
        return jnp.where(sphere < counts_ref[robot], here, far)

    groups_of = [(0, g) for g in range(6)] + [None, None] + [(1, g) for g in range(6)]
    next_columns = [[jnp.zeros((8, LANES), jnp.float32) for _ in range(3)] for _ in range(2)]
    radii = jnp.zeros((8, LANES), jnp.float32)
    for place in sorted((p for p in range(AXIS_ROWS) if p != NEXT), key=lambda p: p % 8):
        if place == EARLY_GROUPS:
            for load in loads[6:]:
                load.wait()
        if place == SHARED:
            column = jnp.where(
                sub < 4,
                radius_column(0, GROUPS - 1),
                pltpu.roll(jnp.broadcast_to(radius_column(1, GROUPS - 1), (8, LANES)), 4, 0),
            )
        else:
            column = radius_column(*groups_of[place])
        radii = jnp.where(spot == PART - 1 - place, column, radii)
        for half in range(2):
            for axis in range(3):
                if place == SHARED:
                    value = jnp.where(
                        sub < 4,
                        raw(0, axis, GROUPS - 1, half),
                        pltpu.roll(raw(1, axis, GROUPS - 1, half), 4, 0),
                    )
                else:
                    robot, group = groups_of[place]
                    value = raw(robot, axis, group, half)
                send[half * 8 : half * 8 + 8, axis * AXIS_ROWS + place, :] = by_part(value)
                value = pltpu.roll(ahead_of(value), (LANES - place) % LANES, 1)
                next_columns[half][axis] = jnp.where(
                    spot == PART - 1 - place, value, next_columns[half][axis]
                )
    radii = by_part(radii)
    for half in range(2):
        for axis in range(3):
            send[half * 8 : half * 8 + 8, axis * AXIS_ROWS + NEXT, :] = by_part(next_columns[half][axis])
        send[half * 8 : half * 8 + 8, RADII, :] = radii
        send[half * 8 : half * 8 + 8, RADII + 1, :] = radii

    pl.semaphore_wait(barrier, ROBOT_DEVICES - 1)

    def slot_of(device):
        return (device // 8) * 8 + lax.rem(8 - lax.rem(device, 8), 8)

    def send_note(number):
        return pltpu.make_async_remote_copy(
            src_ref=note_send,
            dst_ref=note_recv.at[me],
            send_sem=note_send_sem.at[number],
            recv_sem=note_recv_sem.at[number],
            device_id=(lax.rem(me + 1 + number, ROBOT_DEVICES), seed),
            device_id_type=MESH,
        )

    def send_rows(number):
        peer = lax.rem(me + 1 + number, ROBOT_DEVICES)
        return pltpu.make_async_remote_copy(
            src_ref=send.at[slot_of(peer)],
            dst_ref=recv.at[me],
            send_sem=send_sem.at[number],
            recv_sem=recv_sem.at[number],
            device_id=(peer, seed),
            device_id_type=MESH,
        )

    def for_peers(act):
        def one(number, carry):
            act(number)
            return carry

        lax.fori_loop(0, ROBOT_DEVICES - 1, one, 0)

    for_peers(lambda number: send_note(number).start())
    for_peers(lambda number: send_rows(number).start())
    note_recv[me] = note_send[...]
    recv[me] = send[slot_of(me)]
    shared_first = ((part + (8 - lax.rem(me, 8))) & 7) < 4

    def take(device):
        base = device * ROWS
        square = [None, None]
        values = [[], []]
        for axis in range(3):
            following = jnp.broadcast_to(
                recv[device, axis * AXIS_ROWS + NEXT : axis * AXIS_ROWS + NEXT + 1, :], (8, LANES)
            )
            for n in range(2):
                first = axis * AXIS_ROWS + 8 * n
                here = recv[device, first : first + 8, :]
                end = pltpu.roll(following, 8 * n, 1, stride=1, stride_axis=0)
                ahead = jnp.where(spot == PART - 1, end, pltpu.roll(here, LANES - 1, 1))
                step = ahead - here
                square[n] = step * step if axis == 0 else square[n] + step * step
                values[n].append((here + ahead) * (0.5 * ROOT))
        radii = jnp.broadcast_to(recv[device, RADII : RADII + 1, :], (8, LANES))
        for n in range(2):
            radius = pltpu.roll(radii, 8 * n, 1, stride=1, stride_axis=0)
            radius = jnp.where(spot == PART - 1, radius, 0.0)
            for shift in (1, 2, 4, 8):
                radius = radius + pltpu.roll(radius, LANES - shift, 1)
            values[n].append(radius + 0.5 * jnp.sqrt(square[n] + 1e-6))
        for quantity in range(4):
            for robot in range(ROBOTS_HERE):
                start = base + robot * (4 * GROUPS) + quantity
                recv_ref[pl.ds(start, 6, stride=4), :] = values[robot][quantity][0:6, :]
                shared = values[0][quantity][SHARED : SHARED + 1, :]
                if quantity == 0:
                    number = (device * ROBOTS_HERE + robot) * 64 + 61
                    filling = (FAR * ROOT) * jnp.full((1, LANES), number, jnp.int32).astype(jnp.float32)
                    mine = shared_first[0:1, :] if robot == 0 else ~shared_first[0:1, :]
                    shared = jnp.where(mine, shared, filling)
                recv_ref[pl.ds(start + 24, 1), :] = shared
        for n in range(ROWS):
            line = jnp.broadcast_to(recv_ref[pl.ds(base + n, 1), :], (8, LANES))
            turned_ref[base + n] = pltpu.roll(line, 0, 1, stride=PART, stride_axis=0)

    take(me)

    for group in range(GROUPS):
        sphere = sub + 8 * group
        for robot in range(ROBOTS_HERE):
            active = sphere < counts_ref[robot]
            radius = radius_column(robot, group)
            far = FAR * (sphere + numbers[robot]).astype(jnp.float32)
            for half in range(2):
                out, square = [], None
                for axis in range(3):
                    here = centre_rows(centres_ref, robot, axis, group, half)
                    ahead = ahead_of(here)
                    step = ahead - here
                    square = step * step if square is None else square + step * step
                    middle = (here + ahead) * (0.5 * ROOT)
                    out.append(jnp.where(active, middle, far if axis == 0 else 0.0))
                out.append(jnp.where(active, radius + 0.5 * jnp.sqrt(square + 1e-6), 1.0))
                for quantity in range(4):
                    swept[half * ROBOTS_HERE + robot, quantity, 8 * group : 8 * group + 8, :] = out[quantity]
    for index in range(2 * ROBOTS_HERE):
        robot = index % ROBOTS_HERE
        number = (me * ROBOTS_HERE + robot) * 64 + 1
        for quantity in range(4):
            fill = jnp.full((8, LANES), float(quantity == 3))
            if quantity == 0:
                fill = FAR * (sub + 8 * GROUPS + number).astype(jnp.float32)
            swept[index, quantity, 8 * GROUPS : 8 * GROUPS + 8, :] = fill

    def self_pairs(index, carry):
        sums = [jnp.zeros((8, LANES), jnp.float32) for _ in range(4)]
        turn = 0
        for group in range(GROUPS):
            first = [swept[index, q, 8 * group : 8 * group + 8, :] for q in range(4)]
            for apart in range(2, SPHERES - 8 * group):
                start = 8 * group + apart
                second = [swept[index, q, start : start + 8, :] for q in range(4)]
                sums[turn] = sums[turn] + pair_term(first, second)
                turn = (turn + 1) % 4
        total = jnp.sum((sums[0] + sums[1]) + (sums[2] + sums[3]), axis=0, keepdims=True)
        self_ref[pl.ds(index, 1), :] = total * (1.0 / (SPHERES * SPHERES))
        return carry

    lax.fori_loop(0, 2 * ROBOTS_HERE, self_pairs, 0)

    for_peers(lambda number: send_note(number).wait_recv())
    for device in range(ROBOT_DEVICES):
        note[ROBOTS_HERE * device : ROBOTS_HERE * (device + 1), :] = note_recv[device]
    shape = (ROBOTS, LANES)
    row, column = iota(0, shape), iota(1, shape)
    row_number = row.astype(jnp.float32)
    noted = note[...].astype(jnp.float32)
    link = jnp.where((column > row) & (column < ROBOTS) & (noted != 0.0), 1.0, 0.0)
    counts = jnp.sum(jnp.where(column == COUNT_LANE, noted, 0.0), axis=1, keepdims=True)
    groups = jnp.floor((counts + 7.0) * 0.125)

    def as_row(value):
        return jnp.sum(jnp.where(row == column, value, 0.0), axis=0, keepdims=True)

    length = link * as_row(groups)
    before = (iota(0, (LANES, LANES)) < iota(1, (LANES, LANES))).astype(jnp.float32)
    start = jnp.dot(length, before, preferred_element_type=jnp.float32)
    end = start + length
    words = jnp.zeros(shape, jnp.int32)
    for byte in range(4):
        place = (column * 4 + byte).astype(jnp.float32)
        listed = jnp.full(shape, float(ROW_IDS))
        for robot in range(1, ROBOTS):
            first, past = start[:, robot : robot + 1], end[:, robot : robot + 1]
            listed = jnp.where(
                (place >= first) & (place < past), place + (float(GROUPS * robot) - first), listed
            )
        words = words | (listed.astype(jnp.int32) << (8 * byte))
    steps = jnp.floor((jnp.sum(length, axis=1, keepdims=True) + (STEP_ROWS - 1.0)) * (1.0 / STEP_ROWS))
    words = jnp.where(column == STEPS_WORD, steps.astype(jnp.int32), words)
    note[...] = jnp.where(column < ENTRY, words, 0)
    table_ref[0:16, :] = note[pl.ds(0, 16, stride=2), :] + pltpu.roll(
        note[pl.ds(1, 16, stride=2), :], ENTRY, 1
    )
    busy = jnp.where(steps > 0.0, 1.0, 0.0)
    key = groups * 32.0 + row_number
    key_row, busy_row = as_row(key), as_row(busy)
    rank = jnp.sum(jnp.where(key_row < key, busy_row, 0.0), axis=1, keepdims=True)
    lane_number = column.astype(jnp.float32)
    last = jnp.sum(
        jnp.where((rank == lane_number) & (busy > 0.0), row_number, 0.0), axis=0, keepdims=True
    )
    steps_row = as_row(steps)
    rank_row = as_row(rank)
    done_before = jnp.sum(
        jnp.where((rank_row < rank) & (busy_row > 0.0), steps_row, 0.0), axis=1, keepdims=True
    )
    all_steps = jnp.sum(steps_row, axis=1, keepdims=True)
    late_start = jnp.maximum(all_steps - float(LATE_STEPS), 0.0)
    holds = (busy > 0.0) & (done_before <= late_start) & (late_start < done_before + steps)

    def held(value):
        return jnp.sum(jnp.where(holds, value, 0.0), axis=0, keepdims=True)

    line = iota(1, (1, LANES))
    for n, value in enumerate((held(rank), held(late_start - done_before), all_steps - late_start)):
        last = jnp.where(line == LATE - ORDER + n, value, last)
    for case in range(FIRST_GROUPS, GROUPS + 1):
        of_case = jnp.sum(jnp.where(groups == float(case), steps, 0.0), axis=0, keepdims=True)
        before_case = jnp.sum(jnp.where(groups < float(case), steps, 0.0), axis=0, keepdims=True)
        earlier = jnp.sum(jnp.where(groups < float(case), busy, 0.0), axis=0, keepdims=True)
        of_case = jnp.minimum(jnp.maximum(late_start - before_case, 0.0), of_case)
        last = jnp.where(line == CASE_STEPS - ORDER + case - FIRST_GROUPS, of_case, last)
        last = jnp.where(line == CASE_START - ORDER + case - FIRST_GROUPS, earlier, last)
    table_ref[16:24, :] = jnp.broadcast_to(last, (8, LANES)).astype(jnp.int32)
    recv_ref[ROBOT_DEVICES * ROWS : ROBOT_DEVICES * ROWS + 8, :] = jnp.where(
        sub == 0, -1000.0 * FAR, jnp.where(sub == 3, 1.0, 0.0)
    )

    def arrive(number):
        send_rows(number).wait_recv()
        take(lax.rem(me + ROBOT_DEVICES - 1 - number, ROBOT_DEVICES))

    for_peers(arrive)
    for_peers(lambda number: send_note(number).wait_send())
    for_peers(lambda number: send_rows(number).wait_send())


def pair_sums(rows, turned, groups, robot, ids):
    a_row = robot * (4 * GROUPS)
    sums = []
    for row_id in ids:
        b = [jnp.broadcast_to(rows[pl.ds(row_id * 4 + q, 1), :], (8, LANES)) for q in range(4)]
        terms = []
        for group in range(groups):
            a = [turned[a_row + (group * 4 + q)] for q in range(4)]
            terms.append(pair_term(a, b))
        while len(terms) > 1:
            terms = [p + q for p, q in zip(terms[0::2], terms[1::2])] + terms[len(terms) & ~1 :]
        sums.append(terms[0])
    own = sums
    while len(own) > 1:
        own = [p + q for p, q in zip(own[0::2], own[1::2])]
    return sums + own


def step_of(table, turn, step, there):
    robot = jnp.minimum(table[ORDER + turn], ROBOTS - 1)
    entry = robot * ENTRY
    nothing = jnp.int32(ROW_IDS * 0x01010101 - (1 << 32))
    words = [jnp.where(there, table[entry + 2 * step + n], nothing) for n in range(2)]
    ids = [lax.shift_right_logical(word, 8 * n) & 255 for word in words for n in range(4)]
    step = step + 1
    over = (step >= table[entry + STEPS_WORD]).astype(jnp.int32)
    return robot, ids, jnp.minimum(turn + over, ROBOTS - 1), step * (1 - over)


def cross_kernel(table, rows, turned, total):
    zero = jnp.zeros((8, LANES), jnp.float32)

    def clear(index, carry):
        for n in range(15):
            total[index * 15 + n] = zero
        return carry

    lax.fori_loop(0, (ROW_IDS + 1) // 15, clear, 0)

    def add_up(robot, ids, found):
        ids = ids + [robot * GROUPS]
        olds = [total[row_id] for row_id in ids]
        for row_id, old, new in zip(ids, olds, found):
            total[row_id] = old + new

    for groups in range(FIRST_GROUPS, GROUPS + 1):
        steps = table[CASE_STEPS + groups - FIRST_GROUPS]

        def two_steps_of(index, turn, step):
            robot, ids, turn, step = step_of(table, turn, step, 2 * index < steps)
            other, other_ids, turn, step = step_of(table, turn, step, 2 * index + 1 < steps)
            return turn, step, robot, other, *ids, *other_ids

        def two_steps(index, state, groups=groups, two_steps_of=two_steps_of):
            turn, step, robot, other, *ids = state
            ids, other_ids = ids[:STEP_ROWS], ids[STEP_ROWS:]
            found = pair_sums(rows, turned, groups, robot, ids)
            other_found = pair_sums(rows, turned, groups, other, other_ids)
            add_up(robot, ids, found)
            add_up(other, other_ids, other_found)
            return two_steps_of(index + 1, turn, step)

        start = jnp.minimum(table[CASE_START + groups - FIRST_GROUPS], ROBOTS - 1)
        lax.fori_loop(0, (steps + 1) >> 1, two_steps, two_steps_of(0, start, jnp.int32(0)))


def blend_kernel(
    table_ref,
    rows,
    turned,
    total,
    self_ref,
    centres_ref,
    robot_cost_ref,
    gathered,
    table,
    late,
    late_robot,
    sums,
    cost_ref,
    cost_recv,
    weight,
    packed,
    parts,
    table_sem,
    cost_sems,
    part_sems,
    gather_sems,
):
    me = lax.axis_index("robot")
    seed = lax.axis_index("seed")
    x, z = seed // Z, lax.rem(seed, Z)
    peers = [lax.rem(me + step, ROBOT_DEVICES) for step in range(1, ROBOT_DEVICES)]
    z_peers = [lax.rem(z + step, Z) for step in (4, 3, 5, 2, 6, 1, 7)]
    seed_peers = [lax.rem((1 - x) * Z + lax.rem(z + 4, Z), 2 * Z)] + [p for step in (3, 5, 2, 6, 1, 7, 0) for p in ([(1 - x) * Z + lax.rem(z + step, Z)])]
    seed_peers = seed_peers[:3] + [x * Z + lax.rem(z + 4, Z)] + seed_peers[3:5] + [x * Z + lax.rem(z + 3, Z), x * Z + lax.rem(z + 5, Z)] + seed_peers[5:7] + [x * Z + lax.rem(z + 2, Z), x * Z + lax.rem(z + 6, Z)] + seed_peers[7:] + [x * Z + lax.rem(z + 1, Z), x * Z + lax.rem(z + 7, Z)]

    barrier = pltpu.get_barrier_semaphore()

    def greet(number, carry):
        peer = lax.rem(me + 1 + lax.rem(number + 7, ROBOT_DEVICES - 1), ROBOT_DEVICES)
        pl.semaphore_signal(barrier, inc=1, device_id=(peer, seed), device_id_type=MESH)
        return carry

    lax.fori_loop(0, ROBOT_DEVICES - 1, greet, 0)

    def greet_seed(number, carry):
        peer = lax.rem(seed + 1 + number, 2 * Z)
        pl.semaphore_signal(barrier, inc=1, device_id=(me, peer), device_id_type=MESH)
        return carry

    lax.fori_loop(0, 2 * Z - 1, greet_seed, 0)

    load = pltpu.make_async_copy(table_ref, table, table_sem)
    load.start()
    line = iota(1, (1, LANES))
    for robot in range(ROBOTS):
        found = total[robot * GROUPS]
        for group in range(1, GROUPS):
            found = found + total[robot * GROUPS + group]
        sums[robot] = found
    for slot in range(9 * LATE_STEPS, LATE_SLOTS):
        late[slot] = jnp.zeros((8, LANES), jnp.float32)
        late_robot[slot : slot + 1, :] = jnp.zeros((1, LANES), jnp.float32)
    load.wait()
    late_count = table[LATE + 2]

    def two_steps(index, place):
        turn, step = place
        first = step_of(table, turn, step, 2 * index < late_count)
        second = step_of(table, *first[2:], 2 * index + 1 < late_count)
        slot = 2 * (STEP_ROWS + 1) * index
        for robot, ids, _, _ in (first, second):
            found = pair_sums(rows, turned, GROUPS, robot, ids)
            for value, holder in zip(found, [row_id // GROUPS for row_id in ids] + [robot]):
                late[slot] = value
                late_robot[pl.ds(slot, 1), :] = jnp.where(line == holder, 1.0, 0.0)
                slot = slot + 1
        return second[2:]

    lax.fori_loop(0, LATE_STEPS // 2, two_steps, (table[LATE], table[LATE + 1]))
    late_cost = lax.dot_general(
        late_robot[...],
        jnp.sum(late[...], axis=1),
        (((0,), (0,)), ((), ())),
        precision=lax.Precision.HIGHEST,
        preferred_element_type=jnp.float32,
    )
    cost = jnp.sum(sums[...], axis=1) + late_cost[0:ROBOTS, :]
    for shift in (64, 32, 16):
        cost = cost + pltpu.roll(cost, shift, 1)
    cost = cost * (1.0 / (SPHERES * SPHERES))
    for device in range(ROBOT_DEVICES):
        cost_ref[device] = cost[ROBOTS_HERE * device : ROBOTS_HERE * (device + 1), :]

    pl.semaphore_wait(barrier, ROBOT_DEVICES - 1 + 2 * Z - 1)

    def start(src, dst, sems, number, device):
        copy = pltpu.make_async_remote_copy(
            src_ref=src,
            dst_ref=dst,
            send_sem=sems.at[0, number],
            recv_sem=sems.at[1, number],
            device_id=device,
            device_id_type=MESH,
        )
        copy.start()
        return copy

    copies = [
        start(cost_ref.at[peer], cost_recv.at[me], cost_sems, number, (peer, seed))
        for number, peer in enumerate(peers)
    ]
    cost_recv[me] = cost_ref[me]
    for copy in copies:
        copy.wait_recv()
    sent = copies

    lane = iota(1, (ROBOTS_HERE, LANES))
    part = lane // PART
    for half in range(2):
        cost = self_ref[half * ROBOTS_HERE : (half + 1) * ROBOTS_HERE, :]
        for k in range(8):
            cost = cost + jnp.where(part == k, cost_recv[half * 8 + k], 0.0)
        robot_cost_ref[:, half * LANES : (half + 1) * LANES] = cost
        for bit in (1, 2, 4, 8, 16):
            cost = cost + jnp.where(
                lane & bit != 0, pltpu.roll(cost, bit, 1), pltpu.roll(cost, LANES - bit, 1)
            )
        weight[half] = 1.0 / (1.0 + cost)
    weights = weight[0] + weight[1]
    weights = weights + pltpu.roll(weights, 64, 1)
    weights = weights + pltpu.roll(weights, 32, 1)
    total_row = jnp.where(line < 64, weights[0:1, :], weights[1:2, :])

    quarter = iota(1) // W
    units = [[], []]
    for robot in range(ROBOTS_HERE):
        weights = [
            jnp.broadcast_to(weight[half, robot : robot + 1, :], (8, LANES)) for half in range(2)
        ]
        for axis in range(3):
            for group in range(GROUPS):
                value = (
                    centre_rows(centres_ref, robot, axis, group, 0) * weights[0]
                    + centre_rows(centres_ref, robot, axis, group, 1) * weights[1]
                )
                value = value + pltpu.roll(value, 64, 1)
                units[robot].append(value + pltpu.roll(value, 32, 1))
        units[robot].append(jnp.zeros((8, LANES), jnp.float32))
    for v in range(CHUNK):
        value = jnp.where(
            quarter < 2,
            jnp.where(quarter == 0, units[0][v], units[0][CHUNK + v]),
            jnp.where(quarter == 2, units[1][v], units[1][CHUNK + v]),
        )
        done = 0
        while done < 8:
            chunk, row = divmod(8 * v + done, CHUNK)
            length = min(8 - done, CHUNK - row)
            packed[chunk, row : row + length, :] = value[done : done + length, :]
            done += length
    for chunk in range(Z):
        packed[chunk, CHUNK : CHUNK + 1, :] = total_row

    copies = [
        start(packed.at[peer], parts.at[number], part_sems, number, (me, x * Z + peer))
        for number, peer in enumerate(z_peers)
    ]
    found = packed[z]
    for number, copy in enumerate(copies):
        copy.wait_recv()
        found = found + parts[number]
    sent = sent + copies

    gathered[seed] = found
    copies = [
        start(gathered.at[seed], gathered.at[seed], gather_sems, number, (me, peer))
        for number, peer in enumerate(seed_peers)
    ]
    for copy in copies:
        copy.wait_recv()
    sent = sent + copies

    for copy in sent:
        copy.wait_send()


def finish_kernel(cost_in, gathered, cost_out, blended, lines):
    cost_out[...] = cost_in[...]
    for chunk in range(Z):
        found = gathered[chunk] + gathered[Z + chunk]
        found = found / found[CHUNK : CHUNK + 1, :]
        lines[CHUNK * chunk : CHUNK * (chunk + 1), :] = found[0:CHUNK, :]
    turned = lines[...].T
    for robot in range(ROBOTS_HERE):
        for axis in range(3):
            for quarter in range(2):
                low = max(axis * GROUPS, quarter * CHUNK)
                high = min((axis + 1) * GROUPS, (quarter + 1) * CHUNK)
                if low < high:
                    source = (robot * 2 + quarter) * W
                    lane = 8 * (low - quarter * CHUNK)
                    first = 8 * (low - axis * GROUPS)
                    width = min(8 * (high - low), SPHERES - first)
                    blended[robot, axis, :, first : first + width] = turned[
                        source : source + W, lane : lane + width
                    ]


def in_vmem(count):
    return [pl.BlockSpec(memory_space=pltpu.VMEM)] * count


IN_SMEM = pl.BlockSpec(memory_space=pltpu.SMEM)


def local(centres, sphere_radius, counts, adjacency):
    dma = pltpu.SemaphoreType.DMA
    f32 = jnp.float32
    peers = ROBOT_DEVICES - 1
    rows = centres.transpose(1, 2, 0, 3).reshape(3 * SPHERES, ROBOTS_HERE, 2, LANES)
    rows = rows.transpose(0, 2, 1, 3).reshape(3 * SPHERES * 2 * ROBOTS_HERE, LANES)
    in_hbm = pl.BlockSpec(memory_space=pltpu.HBM)
    received, turned, self_cost, table = pl.pallas_call(
        spread_kernel,
        out_shape=(
            jax.ShapeDtypeStruct((ROBOT_DEVICES * ROWS + 8, LANES), f32),
            jax.ShapeDtypeStruct((ROBOT_DEVICES * ROWS, 8, LANES), f32),
            jax.ShapeDtypeStruct((2 * ROBOTS_HERE, LANES), f32),
            jax.ShapeDtypeStruct((TABLE_ROWS, LANES), jnp.int32),
        ),
        in_specs=[in_hbm] * 4,
        out_specs=tuple(in_vmem(4)),
        scratch_shapes=[
            pltpu.SMEM((ROBOTS_HERE,), jnp.int32),
            pltpu.VMEM(rows.shape, f32),
            pltpu.VMEM((ROBOTS_HERE, SPHERES), f32),
            pltpu.VMEM((ROBOTS_HERE, ROBOTS), jnp.int32),
            pltpu.VMEM((ROBOT_DEVICES, MESSAGE, LANES), f32),
            pltpu.VMEM((ROBOT_DEVICES, MESSAGE, LANES), f32),
            pltpu.VMEM((2 * ROBOTS_HERE, 4, 64, LANES), f32),
            pltpu.VMEM((ROBOTS_HERE, LANES), jnp.int32),
            pltpu.VMEM((ROBOT_DEVICES, ROBOTS_HERE, LANES), jnp.int32),
            pltpu.VMEM((ROBOTS, LANES), jnp.int32),
            dma((9,)),
            dma((peers,)),
            dma((peers,)),
            dma((peers,)),
            dma((peers,)),
        ],
        compiler_params=pltpu.CompilerParams(
            collective_id=0, has_side_effects=True, vmem_limit_bytes=GRANT
        ),
        name="spread",
    )(*[pltpu.with_memory_space_constraint(v, pltpu.HBM) for v in (counts, rows, sphere_radius, adjacency)])
    flat_table = table.reshape(TABLE_ROWS * LANES)
    total = pl.pallas_call(
        cross_kernel,
        out_shape=jax.ShapeDtypeStruct((ROW_IDS + 1, 8, LANES), f32),
        in_specs=[IN_SMEM] + in_vmem(2),
        out_specs=in_vmem(1)[0],
        compiler_params=pltpu.CompilerParams(vmem_limit_bytes=GRANT),
        name="cross",
    )(flat_table, received, turned)
    robot_cost, gathered = pl.pallas_call(
        blend_kernel,
        out_shape=(
            jax.ShapeDtypeStruct((ROBOTS_HERE, COLUMNS), f32),
            jax.ShapeDtypeStruct((2 * Z, CHUNK + 1, LANES), f32),
        ),
        in_specs=in_vmem(6),
        out_specs=tuple(in_vmem(2)),
        scratch_shapes=[
            pltpu.SMEM((TABLE_ROWS * LANES,), jnp.int32),
            pltpu.VMEM((LATE_SLOTS, 8, LANES), f32),
            pltpu.VMEM((LATE_SLOTS, LANES), f32),
            pltpu.VMEM((ROBOTS, 8, LANES), f32),
            pltpu.VMEM((ROBOT_DEVICES, ROBOTS_HERE, LANES), f32),
            pltpu.VMEM((ROBOT_DEVICES, ROBOTS_HERE, LANES), f32),
            pltpu.VMEM((2, ROBOTS_HERE, LANES), f32),
            pltpu.VMEM((Z, CHUNK + 1, LANES), f32),
            pltpu.VMEM((Z - 1, CHUNK + 1, LANES), f32),
            dma,
            dma((2, peers)),
            dma((2, Z - 1)),
            dma((2, 2 * Z - 1)),
        ],
        compiler_params=pltpu.CompilerParams(
            collective_id=1, has_side_effects=True, vmem_limit_bytes=GRANT
        ),
        name="blend",
    )(flat_table, received, turned, total, self_cost, rows)
    robot_cost, blended = pl.pallas_call(
        finish_kernel,
        out_shape=(
            jax.ShapeDtypeStruct((ROBOTS_HERE, COLUMNS), f32),
            jax.ShapeDtypeStruct((ROBOTS_HERE, 3, W, SPHERES), f32),
        ),
        in_specs=in_vmem(2),
        out_specs=tuple(in_vmem(2)),
        scratch_shapes=[pltpu.VMEM((LANES, LANES), f32)],
        compiler_params=pltpu.CompilerParams(vmem_limit_bytes=GRANT),
        name="finish",
    )(robot_cost, gathered)
    return robot_cost, blended.transpose(0, 1, 3, 2)


def solution(mesh):
    return jax.shard_map(
        local,
        mesh=mesh,
        in_specs=(P("robot", None, None, "seed"), P("robot", None), P("robot"), P("robot", None)),
        out_specs=(P("robot", "seed"), P("robot", None, None, None)),
        check_vma=False,
    )
```

```python
import functools
import math

import jax
import jax.numpy as jnp
from jax import lax
from jax.experimental import pallas as pl
from jax.experimental.pallas import tpu as pltpu
from jax.sharding import PartitionSpec as P

W = 32
SPHERES = 52
GROUPS = 7
FIRST_GROUPS = 4
ROBOTS_HERE = 2
ROBOT_DEVICES = 16
ROBOTS = ROBOTS_HERE * ROBOT_DEVICES
LANES = 128
COLUMNS = 256
PART = 16
ROWS = ROBOTS_HERE * GROUPS * 4
SHARED = 4 * (GROUPS - 1)
MESSAGE = ROWS - 4
Z = 8
CHUNK = 11
COUNT_LANE = 32
ROOT = math.sqrt(math.log2(math.e))
FAR = 1.0e6
STEP_ROWS = 8
ROW_IDS = ROBOTS * GROUPS
WORDS = 56
STEPS_WORD = 56
ENTRY = 64
ORDER = ROBOTS * ENTRY
CASE_STEPS = ORDER + 32
CASE_START = ORDER + 40
LATE = ORDER + 48
LATE_STEPS = 28
LATE_SLOTS = 256
TABLE_ROWS = 24
EARLY_GROUPS = 3
GRANT = 16 * 1024 * 1024
MESH = pl.DeviceIdType.MESH


def iota(axis, shape=(8, LANES)):
    return lax.broadcasted_iota(jnp.int32, shape, axis)


def pair_argument(a, b):
    dx, dy, dz = a[0] - b[0], a[1] - b[1], a[2] - b[2]
    spread = a[3] + b[3]
    return (dx * dx + dy * dy + dz * dz) / (-spread * spread)


def pair_term(a, b):
    return jnp.exp2(pair_argument(a, b))


def centre_rows(ref, robot, axis, group, half):
    first = min(8 * group, SPHERES - 8)
    row = ((axis * SPHERES + first) * 2 + half) * ROBOTS_HERE + robot
    value = ref[pl.ds(row, 8, stride=2 * ROBOTS_HERE), :]
    return value if first == 8 * group else pltpu.roll(value, 4, 0)


def spread_kernel(
    counts_hbm,
    centres_hbm,
    radius_hbm,
    adjacency_hbm,
    recv_ref,
    turned_ref,
    self_ref,
    table_ref,
    counts_ref,
    centres_ref,
    radius_ref,
    adjacency_ref,
    send,
    swept,
    note_send,
    note_recv,
    note,
    load_sem,
    send_sem,
    recv_sem,
    note_send_sem,
    note_recv_sem,
):
    me = lax.axis_index("robot")
    seed = lax.axis_index("seed")
    peers = [lax.rem(me + step, ROBOT_DEVICES) for step in range(1, ROBOT_DEVICES)]

    loads = [
        pltpu.make_async_copy(counts_hbm, counts_ref, load_sem.at[0]),
        pltpu.make_async_copy(radius_hbm, radius_ref, load_sem.at[1]),
        pltpu.make_async_copy(adjacency_hbm, adjacency_ref, load_sem.at[2]),
    ]
    per_axis, early = 4 * SPHERES, 4 * 8 * EARLY_GROUPS
    for axis in range(3):
        at = pl.ds(axis * per_axis, early)
        loads.append(pltpu.make_async_copy(centres_hbm.at[at], centres_ref.at[at], load_sem.at[3 + axis]))
    for axis in range(3):
        at = pl.ds(axis * per_axis + early, per_axis - early)
        loads.append(pltpu.make_async_copy(centres_hbm.at[at], centres_ref.at[at], load_sem.at[6 + axis]))
    for load in loads:
        load.start()

    barrier = pltpu.get_barrier_semaphore()
    for peer in peers:
        pl.semaphore_signal(barrier, inc=1, device_id=(peer, seed), device_id_type=MESH)

    for load in loads[:6]:
        load.wait()

    sub, lane = iota(0), iota(1)
    part = lane // PART
    last_waypoint = lane % W == W - 1
    radius_lane = iota(1, (8, SPHERES))
    radius_sub = iota(0, (8, SPHERES))
    note_send[...] = jnp.zeros((ROBOTS_HERE, LANES), jnp.int32)
    note_send[:, 0:ROBOTS] = adjacency_ref[...]
    for robot in range(ROBOTS_HERE):
        note_send[robot : robot + 1, COUNT_LANE : COUNT_LANE + 1] = jnp.full((1, 1), counts_ref[robot], jnp.int32)
    ends = {}
    for group in range(GROUPS):
        if group == EARLY_GROUPS:
            for load in loads[6:]:
                load.wait()
        for robot in range(ROBOTS_HERE):
            count = counts_ref[robot]
            radius_row = jnp.broadcast_to(radius_ref[robot : robot + 1, :], (8, SPHERES))
            number = (me * ROBOTS_HERE + robot) * 64 + 1
            radius = jnp.sum(
                jnp.where(radius_lane == radius_sub + 8 * group, radius_row, 0.0),
                axis=1,
                keepdims=True,
            )
            sphere = sub + 8 * group
            active = sphere < count
            far = FAR * (sphere + number).astype(jnp.float32)
            for half in range(2):
                out, square = [], None
                for axis in range(3):
                    here = centre_rows(centres_ref, robot, axis, group, half)
                    ahead = jnp.where(last_waypoint, here, pltpu.roll(here, LANES - 1, 1))
                    step = ahead - here
                    square = step * step if square is None else square + step * step
                    middle = (here + ahead) * (0.5 * ROOT)
                    out.append(jnp.where(active, middle, far if axis == 0 else 0.0))
                out.append(jnp.where(active, radius + 0.5 * jnp.sqrt(square + 1e-6), 1.0))
                for quantity in range(4):
                    value = out[quantity]
                    swept[half * ROBOTS_HERE + robot, quantity, 8 * group : 8 * group + 8, :] = value
                    if group == GROUPS - 1:
                        if robot == 0:
                            ends[half, quantity] = value
                            continue
                        value = jnp.where(sub < 4, ends[half, quantity], pltpu.roll(value, 4, 0))
                    value = pltpu.roll(value, 0, 1, stride=PART, stride_axis=0)
                    for bit in (1, 2, 4):
                        value = jnp.where(part & bit != 0, pltpu.roll(value, 8 - bit, 0), value)
                    row = (robot * GROUPS + group) * 4 + quantity
                    if group == GROUPS - 1:
                        row = SHARED + quantity
                    send[pl.ds(half * 8 * ROWS + row, 8, stride=ROWS), :] = value

    pl.semaphore_wait(barrier, ROBOT_DEVICES - 1)

    def slot_of(device):
        return (device // 8) * 8 + lax.rem(8 - lax.rem(device, 8), 8)

    def sent_of(slot):
        return pl.ds(pl.multiple_of(slot * ROWS, 8), MESSAGE)

    def send_note(number):
        return pltpu.make_async_remote_copy(
            src_ref=note_send,
            dst_ref=note_recv.at[me],
            send_sem=note_send_sem.at[number],
            recv_sem=note_recv_sem.at[number],
            device_id=(lax.rem(me + 1 + number, ROBOT_DEVICES), seed),
            device_id_type=MESH,
        )

    def send_rows(number):
        peer = lax.rem(me + 1 + number, ROBOT_DEVICES)
        return pltpu.make_async_remote_copy(
            src_ref=send.at[sent_of(slot_of(peer))],
            dst_ref=recv_ref.at[sent_of(me)],
            send_sem=send_sem.at[number],
            recv_sem=recv_sem.at[number],
            device_id=(peer, seed),
            device_id_type=MESH,
        )

    def for_peers(act):
        def one(number, carry):
            act(number)
            return carry

        lax.fori_loop(0, ROBOT_DEVICES - 1, one, 0)

    for_peers(lambda number: send_note(number).start())
    for_peers(lambda number: send_rows(number).start())
    note_recv[me] = note_send[...]
    recv_ref[sent_of(me), :] = send[sent_of(slot_of(me)), :]
    first_robot = ((part[0:1, :] + (8 - lax.rem(me, 8))) & 7) < 4

    def turn_rows(device):
        row = pl.multiple_of(device * ROWS, 8)
        for quantity in range(4):
            shared = recv_ref[pl.ds(row + SHARED + quantity, 1), :]
            second = shared
            if quantity == 0:
                number = (device * ROBOTS_HERE) * 64 + 61
                far = FAR * jnp.full((1, LANES), number, jnp.int32).astype(jnp.float32)
                second = jnp.where(first_robot, far + 64.0 * FAR, shared)
                recv_ref[pl.ds(row + SHARED, 1), :] = jnp.where(first_robot, shared, far)
            recv_ref[pl.ds(row + MESSAGE + quantity, 1), :] = second
        for n in range(ROWS):
            line = jnp.broadcast_to(recv_ref[pl.ds(row + n, 1), :], (8, LANES))
            turned_ref[row + n] = pltpu.roll(line, 0, 1, stride=PART, stride_axis=0)

    turn_rows(me)
    for index in range(2 * ROBOTS_HERE):
        robot = index % ROBOTS_HERE
        number = (me * ROBOTS_HERE + robot) * 64 + 1
        for quantity in range(4):
            fill = jnp.full((8, LANES), float(quantity == 3))
            if quantity == 0:
                fill = FAR * (sub + 8 * GROUPS + number).astype(jnp.float32)
            swept[index, quantity, 8 * GROUPS : 8 * GROUPS + 8, :] = fill

    def self_pairs(index, carry):
        sums = [jnp.zeros((8, LANES), jnp.float32) for _ in range(4)]
        turn = 0
        for group in range(GROUPS):
            first = [swept[index, q, 8 * group : 8 * group + 8, :] for q in range(4)]
            for apart in range(2, SPHERES - 8 * group):
                start = 8 * group + apart
                second = [swept[index, q, start : start + 8, :] for q in range(4)]
                sums[turn] = sums[turn] + pair_term(first, second)
                turn = (turn + 1) % 4
        total = jnp.sum((sums[0] + sums[1]) + (sums[2] + sums[3]), axis=0, keepdims=True)
        self_ref[pl.ds(index, 1), :] = total * (1.0 / (SPHERES * SPHERES))
        return carry

    lax.fori_loop(0, 2 * ROBOTS_HERE, self_pairs, 0)

    for_peers(lambda number: send_note(number).wait_recv())
    for device in range(ROBOT_DEVICES):
        note[ROBOTS_HERE * device : ROBOTS_HERE * (device + 1), :] = note_recv[device]
    shape = (ROBOTS, LANES)
    row, column = iota(0, shape), iota(1, shape)
    row_number = row.astype(jnp.float32)
    noted = note[...].astype(jnp.float32)
    link = jnp.where((column > row) & (column < ROBOTS) & (noted != 0.0), 1.0, 0.0)
    counts = jnp.sum(jnp.where(column == COUNT_LANE, noted, 0.0), axis=1, keepdims=True)
    groups = jnp.floor((counts + 7.0) * 0.125)

    def as_row(value):
        return jnp.sum(jnp.where(row == column, value, 0.0), axis=0, keepdims=True)

    length = link * as_row(groups)
    before = (iota(0, (LANES, LANES)) < iota(1, (LANES, LANES))).astype(jnp.float32)
    start = jnp.dot(length, before, preferred_element_type=jnp.float32)
    end = start + length
    words = jnp.zeros(shape, jnp.int32)
    for byte in range(4):
        place = (column * 4 + byte).astype(jnp.float32)
        listed = jnp.full(shape, float(ROW_IDS))
        for robot in range(1, ROBOTS):
            first, past = start[:, robot : robot + 1], end[:, robot : robot + 1]
            listed = jnp.where(
                (place >= first) & (place < past), place + (float(GROUPS * robot) - first), listed
            )
        words = words | (listed.astype(jnp.int32) << (8 * byte))
    steps = jnp.floor((jnp.sum(length, axis=1, keepdims=True) + (STEP_ROWS - 1.0)) * (1.0 / STEP_ROWS))
    words = jnp.where(column == STEPS_WORD, steps.astype(jnp.int32), words)
    note[...] = jnp.where(column < ENTRY, words, 0)
    table_ref[0:16, :] = note[pl.ds(0, 16, stride=2), :] + pltpu.roll(
        note[pl.ds(1, 16, stride=2), :], ENTRY, 1
    )
    busy = jnp.where(steps > 0.0, 1.0, 0.0)
    key = groups * 32.0 + row_number
    key_row, busy_row = as_row(key), as_row(busy)
    rank = jnp.sum(jnp.where(key_row < key, busy_row, 0.0), axis=1, keepdims=True)
    lane_number = column.astype(jnp.float32)
    last = jnp.sum(
        jnp.where((rank == lane_number) & (busy > 0.0), row_number, 0.0), axis=0, keepdims=True
    )
    steps_row = as_row(steps)
    rank_row = as_row(rank)
    done_before = jnp.sum(
        jnp.where((rank_row < rank) & (busy_row > 0.0), steps_row, 0.0), axis=1, keepdims=True
    )
    all_steps = jnp.sum(steps_row, axis=1, keepdims=True)
    late_start = jnp.maximum(all_steps - float(LATE_STEPS), 0.0)
    holds = (busy > 0.0) & (done_before <= late_start) & (late_start < done_before + steps)

    def held(value):
        return jnp.sum(jnp.where(holds, value, 0.0), axis=0, keepdims=True)

    line = iota(1, (1, LANES))
    for n, value in enumerate((held(rank), held(late_start - done_before), all_steps - late_start)):
        last = jnp.where(line == LATE - ORDER + n, value, last)
    for case in range(FIRST_GROUPS, GROUPS + 1):
        of_case = jnp.sum(jnp.where(groups == float(case), steps, 0.0), axis=0, keepdims=True)
        before_case = jnp.sum(jnp.where(groups < float(case), steps, 0.0), axis=0, keepdims=True)
        earlier = jnp.sum(jnp.where(groups < float(case), busy, 0.0), axis=0, keepdims=True)
        of_case = jnp.minimum(jnp.maximum(late_start - before_case, 0.0), of_case)
        last = jnp.where(line == CASE_STEPS - ORDER + case - FIRST_GROUPS, of_case, last)
        last = jnp.where(line == CASE_START - ORDER + case - FIRST_GROUPS, earlier, last)
    table_ref[16:24, :] = jnp.broadcast_to(last, (8, LANES)).astype(jnp.int32)
    recv_ref[ROBOT_DEVICES * ROWS : ROBOT_DEVICES * ROWS + 8, :] = jnp.where(
        sub == 0, -1000.0 * FAR, jnp.where(sub == 3, 1.0, 0.0)
    )

    def arrive(number):
        send_rows(number).wait_recv()
        turn_rows(lax.rem(me + ROBOT_DEVICES - 1 - number, ROBOT_DEVICES))

    for_peers(arrive)
    for_peers(lambda number: send_note(number).wait_send())
    for_peers(lambda number: send_rows(number).wait_send())


def pair_sums(rows, turned, groups, robot, ids):
    a_row = robot * (4 * GROUPS)
    sums = []
    for row_id in ids:
        b = [jnp.broadcast_to(rows[pl.ds(row_id * 4 + q, 1), :], (8, LANES)) for q in range(4)]
        terms = []
        for group in range(groups):
            a = [turned[a_row + (group * 4 + q)] for q in range(4)]
            terms.append(pair_term(a, b))
        while len(terms) > 1:
            terms = [p + q for p, q in zip(terms[0::2], terms[1::2])] + terms[len(terms) & ~1 :]
        sums.append(terms[0])
    own = sums
    while len(own) > 1:
        own = [p + q for p, q in zip(own[0::2], own[1::2])]
    return sums + own


def step_of(table, turn, step, there):
    robot = jnp.minimum(table[ORDER + turn], ROBOTS - 1)
    entry = robot * ENTRY
    nothing = jnp.int32(ROW_IDS * 0x01010101 - (1 << 32))
    words = [jnp.where(there, table[entry + 2 * step + n], nothing) for n in range(2)]
    ids = [lax.shift_right_logical(word, 8 * n) & 255 for word in words for n in range(4)]
    step = step + 1
    over = (step >= table[entry + STEPS_WORD]).astype(jnp.int32)
    return robot, ids, jnp.minimum(turn + over, ROBOTS - 1), step * (1 - over)


def cross_kernel(table, rows, turned, total):
    zero = jnp.zeros((8, LANES), jnp.float32)

    def clear(index, carry):
        for n in range(15):
            total[index * 15 + n] = zero
        return carry

    lax.fori_loop(0, (ROW_IDS + 1) // 15, clear, 0)

    def add_up(robot, ids, found):
        ids = ids + [robot * GROUPS]
        olds = [total[row_id] for row_id in ids]
        for row_id, old, new in zip(ids, olds, found):
            total[row_id] = old + new

    for groups in range(FIRST_GROUPS, GROUPS + 1):
        steps = table[CASE_STEPS + groups - FIRST_GROUPS]

        def two_steps_of(index, turn, step):
            robot, ids, turn, step = step_of(table, turn, step, 2 * index < steps)
            other, other_ids, turn, step = step_of(table, turn, step, 2 * index + 1 < steps)
            return turn, step, robot, other, *ids, *other_ids

        def two_steps(index, state, groups=groups, two_steps_of=two_steps_of):
            turn, step, robot, other, *ids = state
            ids, other_ids = ids[:STEP_ROWS], ids[STEP_ROWS:]
            found = pair_sums(rows, turned, groups, robot, ids)
            other_found = pair_sums(rows, turned, groups, other, other_ids)
            add_up(robot, ids, found)
            add_up(other, other_ids, other_found)
            return two_steps_of(index + 1, turn, step)

        start = jnp.minimum(table[CASE_START + groups - FIRST_GROUPS], ROBOTS - 1)
        lax.fori_loop(0, (steps + 1) >> 1, two_steps, two_steps_of(0, start, jnp.int32(0)))


def blend_kernel(
    table_ref,
    rows,
    turned,
    total,
    self_ref,
    centres_ref,
    robot_cost_ref,
    gathered,
    table,
    late,
    late_robot,
    sums,
    cost_ref,
    cost_recv,
    weight,
    packed,
    parts,
    table_sem,
    cost_sems,
    part_sems,
    gather_sems,
):
    me = lax.axis_index("robot")
    seed = lax.axis_index("seed")
    x, z = seed // Z, lax.rem(seed, Z)
    peers = [lax.rem(me + step, ROBOT_DEVICES) for step in range(1, ROBOT_DEVICES)]
    z_peers = [lax.rem(z + step, Z) for step in (4, 3, 5, 2, 6, 1, 7)]
    seed_peers = [lax.rem((1 - x) * Z + lax.rem(z + 4, Z), 2 * Z)] + [p for step in (3, 5, 2, 6, 1, 7, 0) for p in ([(1 - x) * Z + lax.rem(z + step, Z)])]
    seed_peers = seed_peers[:3] + [x * Z + lax.rem(z + 4, Z)] + seed_peers[3:5] + [x * Z + lax.rem(z + 3, Z), x * Z + lax.rem(z + 5, Z)] + seed_peers[5:7] + [x * Z + lax.rem(z + 2, Z), x * Z + lax.rem(z + 6, Z)] + seed_peers[7:] + [x * Z + lax.rem(z + 1, Z), x * Z + lax.rem(z + 7, Z)]

    barrier = pltpu.get_barrier_semaphore()

    def greet(number, carry):
        peer = lax.rem(me + 1 + lax.rem(number + 7, ROBOT_DEVICES - 1), ROBOT_DEVICES)
        pl.semaphore_signal(barrier, inc=1, device_id=(peer, seed), device_id_type=MESH)
        return carry

    lax.fori_loop(0, ROBOT_DEVICES - 1, greet, 0)

    def greet_seed(number, carry):
        peer = lax.rem(seed + 1 + number, 2 * Z)
        pl.semaphore_signal(barrier, inc=1, device_id=(me, peer), device_id_type=MESH)
        return carry

    lax.fori_loop(0, 2 * Z - 1, greet_seed, 0)

    load = pltpu.make_async_copy(table_ref, table, table_sem)
    load.start()
    line = iota(1, (1, LANES))
    for robot in range(ROBOTS):
        found = total[robot * GROUPS]
        for group in range(1, GROUPS):
            found = found + total[robot * GROUPS + group]
        sums[robot] = found
    for slot in range(9 * LATE_STEPS, LATE_SLOTS):
        late[slot] = jnp.zeros((8, LANES), jnp.float32)
        late_robot[slot : slot + 1, :] = jnp.zeros((1, LANES), jnp.float32)
    load.wait()
    late_count = table[LATE + 2]

    def late_steps(index, place):
        turn, step = place
        jobs = []
        for n in range(4):
            jobs.append(step_of(table, turn, step, 4 * index + n < late_count))
            turn, step = jobs[-1][2:]
        slot = 4 * (STEP_ROWS + 1) * index
        for robot, ids, _, _ in jobs:
            found = pair_sums(rows, turned, GROUPS, robot, ids)
            for value, holder in zip(found, [row_id // GROUPS for row_id in ids] + [robot]):
                late[slot] = value
                late_robot[pl.ds(slot, 1), :] = jnp.where(line == holder, 1.0, 0.0)
                slot = slot + 1
        return turn, step

    lax.fori_loop(0, LATE_STEPS // 4, late_steps, (table[LATE], table[LATE + 1]))
    late_cost = lax.dot_general(
        late_robot[...],
        jnp.sum(late[...], axis=1),
        (((0,), (0,)), ((), ())),
        precision=lax.Precision.HIGHEST,
        preferred_element_type=jnp.float32,
    )
    cost = jnp.sum(sums[...], axis=1) + late_cost[0:ROBOTS, :]
    for shift in (64, 32, 16):
        cost = cost + pltpu.roll(cost, shift, 1)
    cost = cost * (1.0 / (SPHERES * SPHERES))
    for device in range(ROBOT_DEVICES):
        cost_ref[device] = cost[ROBOTS_HERE * device : ROBOTS_HERE * (device + 1), :]

    pl.semaphore_wait(barrier, ROBOT_DEVICES - 1 + 2 * Z - 1)

    def start(src, dst, sems, number, device):
        copy = pltpu.make_async_remote_copy(
            src_ref=src,
            dst_ref=dst,
            send_sem=sems.at[0, number],
            recv_sem=sems.at[1, number],
            device_id=device,
            device_id_type=MESH,
        )
        copy.start()
        return copy

    copies = [
        start(cost_ref.at[peer], cost_recv.at[me], cost_sems, number, (peer, seed))
        for number, peer in enumerate(peers)
    ]
    cost_recv[me] = cost_ref[me]
    for copy in copies:
        copy.wait_recv()
    sent = copies

    lane = iota(1, (ROBOTS_HERE, LANES))
    part = lane // PART
    square = (LANES, LANES)
    same_seed = jnp.where(iota(0, square) // W == iota(1, square) // W, 1.0, 0.0)
    for half in range(2):
        cost = self_ref[half * ROBOTS_HERE : (half + 1) * ROBOTS_HERE, :]
        for k in range(8):
            cost = cost + jnp.where(part == k, cost_recv[half * 8 + k], 0.0)
        robot_cost_ref[:, half * LANES : (half + 1) * LANES] = cost
        cost = jnp.dot(
            cost, same_seed, precision=lax.Precision.HIGHEST, preferred_element_type=jnp.float32
        )
        weight[half] = 1.0 / (1.0 + cost)
    weights = weight[0] + weight[1]
    weights = weights + pltpu.roll(weights, 64, 1)
    weights = weights + pltpu.roll(weights, 32, 1)
    total_row = jnp.where(line < 64, weights[0:1, :], weights[1:2, :])

    quarter = iota(1) // W
    units = [[], []]
    for robot in range(ROBOTS_HERE):
        weights = [
            jnp.broadcast_to(weight[half, robot : robot + 1, :], (8, LANES)) for half in range(2)
        ]
        for axis in range(3):
            for group in range(GROUPS):
                value = (
                    centre_rows(centres_ref, robot, axis, group, 0) * weights[0]
                    + centre_rows(centres_ref, robot, axis, group, 1) * weights[1]
                )
                value = value + pltpu.roll(value, 64, 1)
                units[robot].append(value + pltpu.roll(value, 32, 1))
        units[robot].append(jnp.zeros((8, LANES), jnp.float32))
    for v in range(CHUNK):
        value = jnp.where(
            quarter < 2,
            jnp.where(quarter == 0, units[0][v], units[0][CHUNK + v]),
            jnp.where(quarter == 2, units[1][v], units[1][CHUNK + v]),
        )
        done = 0
        while done < 8:
            chunk, row = divmod(8 * v + done, CHUNK)
            length = min(8 - done, CHUNK - row)
            packed[chunk, row : row + length, :] = value[done : done + length, :]
            done += length
    for chunk in range(Z):
        packed[chunk, CHUNK : CHUNK + 1, :] = total_row

    copies = [
        start(packed.at[peer], parts.at[number], part_sems, number, (me, x * Z + peer))
        for number, peer in enumerate(z_peers)
    ]
    found = packed[z]
    for number, copy in enumerate(copies):
        copy.wait_recv()
        found = found + parts[number]
    sent = sent + copies

    gathered[seed] = found
    copies = [
        start(gathered.at[seed], gathered.at[seed], gather_sems, number, (me, peer))
        for number, peer in enumerate(seed_peers)
    ]
    for copy in copies:
        copy.wait_recv()
    sent = sent + copies

    for copy in sent:
        copy.wait_send()


def finish_kernel(cost_in, gathered, cost_out, blended, lines):
    cost_out[...] = cost_in[...]
    for chunk in range(Z):
        found = gathered[chunk] + gathered[Z + chunk]
        found = found / found[CHUNK : CHUNK + 1, :]
        lines[CHUNK * chunk : CHUNK * (chunk + 1), :] = found[0:CHUNK, :]
    turned = lines[...].T
    for robot in range(ROBOTS_HERE):
        for axis in range(3):
            for quarter in range(2):
                low = max(axis * GROUPS, quarter * CHUNK)
                high = min((axis + 1) * GROUPS, (quarter + 1) * CHUNK)
                if low < high:
                    source = (robot * 2 + quarter) * W
                    lane = 8 * (low - quarter * CHUNK)
                    first = 8 * (low - axis * GROUPS)
                    width = min(8 * (high - low), SPHERES - first)
                    blended[robot, axis, :, first : first + width] = turned[
                        source : source + W, lane : lane + width
                    ]


def in_vmem(count):
    return [pl.BlockSpec(memory_space=pltpu.VMEM)] * count


IN_SMEM = pl.BlockSpec(memory_space=pltpu.SMEM)


def local(centres, sphere_radius, counts, adjacency):
    dma = pltpu.SemaphoreType.DMA
    f32 = jnp.float32
    peers = ROBOT_DEVICES - 1
    rows = centres.transpose(1, 2, 0, 3).reshape(3 * SPHERES, ROBOTS_HERE, 2, LANES)
    rows = rows.transpose(0, 2, 1, 3).reshape(3 * SPHERES * 2 * ROBOTS_HERE, LANES)
    in_hbm = pl.BlockSpec(memory_space=pltpu.HBM)
    received, turned, self_cost, table = pl.pallas_call(
        spread_kernel,
        out_shape=(
            jax.ShapeDtypeStruct((ROBOT_DEVICES * ROWS + 8, LANES), f32),
            jax.ShapeDtypeStruct((ROBOT_DEVICES * ROWS, 8, LANES), f32),
            jax.ShapeDtypeStruct((2 * ROBOTS_HERE, LANES), f32),
            jax.ShapeDtypeStruct((TABLE_ROWS, LANES), jnp.int32),
        ),
        in_specs=[in_hbm] * 4,
        out_specs=tuple(in_vmem(4)),
        scratch_shapes=[
            pltpu.SMEM((ROBOTS_HERE,), jnp.int32),
            pltpu.VMEM(rows.shape, f32),
            pltpu.VMEM((ROBOTS_HERE, SPHERES), f32),
            pltpu.VMEM((ROBOTS_HERE, ROBOTS), jnp.int32),
            pltpu.VMEM((ROBOT_DEVICES * ROWS, LANES), f32),
            pltpu.VMEM((2 * ROBOTS_HERE, 4, 64, LANES), f32),
            pltpu.VMEM((ROBOTS_HERE, LANES), jnp.int32),
            pltpu.VMEM((ROBOT_DEVICES, ROBOTS_HERE, LANES), jnp.int32),
            pltpu.VMEM((ROBOTS, LANES), jnp.int32),
            dma((9,)),
            dma((peers,)),
            dma((peers,)),
            dma((peers,)),
            dma((peers,)),
        ],
        compiler_params=pltpu.CompilerParams(
            collective_id=0, has_side_effects=True, vmem_limit_bytes=GRANT
        ),
        name="spread",
    )(*[pltpu.with_memory_space_constraint(v, pltpu.HBM) for v in (counts, rows, sphere_radius, adjacency)])
    flat_table = table.reshape(TABLE_ROWS * LANES)
    total = pl.pallas_call(
        cross_kernel,
        out_shape=jax.ShapeDtypeStruct((ROW_IDS + 1, 8, LANES), f32),
        in_specs=[IN_SMEM] + in_vmem(2),
        out_specs=in_vmem(1)[0],
        compiler_params=pltpu.CompilerParams(vmem_limit_bytes=GRANT),
        name="cross",
    )(flat_table, received, turned)
    robot_cost, gathered = pl.pallas_call(
        blend_kernel,
        out_shape=(
            jax.ShapeDtypeStruct((ROBOTS_HERE, COLUMNS), f32),
            jax.ShapeDtypeStruct((2 * Z, CHUNK + 1, LANES), f32),
        ),
        in_specs=in_vmem(6),
        out_specs=tuple(in_vmem(2)),
        scratch_shapes=[
            pltpu.SMEM((TABLE_ROWS * LANES,), jnp.int32),
            pltpu.VMEM((LATE_SLOTS, 8, LANES), f32),
            pltpu.VMEM((LATE_SLOTS, LANES), f32),
            pltpu.VMEM((ROBOTS, 8, LANES), f32),
            pltpu.VMEM((ROBOT_DEVICES, ROBOTS_HERE, LANES), f32),
            pltpu.VMEM((ROBOT_DEVICES, ROBOTS_HERE, LANES), f32),
            pltpu.VMEM((2, ROBOTS_HERE, LANES), f32),
            pltpu.VMEM((Z, CHUNK + 1, LANES), f32),
            pltpu.VMEM((Z - 1, CHUNK + 1, LANES), f32),
            dma,
            dma((2, peers)),
            dma((2, Z - 1)),
            dma((2, 2 * Z - 1)),
        ],
        compiler_params=pltpu.CompilerParams(
            collective_id=1, has_side_effects=True, vmem_limit_bytes=GRANT
        ),
        name="blend",
    )(flat_table, received, turned, total, self_cost, rows)
    robot_cost, blended = pl.pallas_call(
        finish_kernel,
        out_shape=(
            jax.ShapeDtypeStruct((ROBOTS_HERE, COLUMNS), f32),
            jax.ShapeDtypeStruct((ROBOTS_HERE, 3, W, SPHERES), f32),
        ),
        in_specs=in_vmem(2),
        out_specs=tuple(in_vmem(2)),
        scratch_shapes=[pltpu.VMEM((LANES, LANES), f32)],
        compiler_params=pltpu.CompilerParams(vmem_limit_bytes=GRANT),
        name="finish",
    )(robot_cost, gathered)
    return robot_cost, blended.transpose(0, 1, 3, 2)


def solution(mesh):
    return jax.shard_map(
        local,
        mesh=mesh,
        in_specs=(P("robot", None, None, "seed"), P("robot", None), P("robot"), P("robot", None)),
        out_specs=(P("robot", "seed"), P("robot", None, None, None)),
        check_vma=False,
    )
```

```python
import functools
import math

import jax
import jax.numpy as jnp
from jax import lax
from jax.experimental import pallas as pl
from jax.experimental.pallas import tpu as pltpu
from jax.sharding import PartitionSpec as P

W = 32
SPHERES = 52
GROUPS = 7
FIRST_GROUPS = 4
ROBOTS_HERE = 2
ROBOT_DEVICES = 16
ROBOTS = ROBOTS_HERE * ROBOT_DEVICES
LANES = 128
COLUMNS = 256
PART = 16
ROWS = ROBOTS_HERE * GROUPS * 4
SHARED = 4 * (GROUPS - 1)
MESSAGE = ROWS - 4
Z = 8
CHUNK = 11
COUNT_LANE = 32
ROOT = math.sqrt(math.log2(math.e))
FAR = 1.0e6
STEP_ROWS = 8
ROW_IDS = ROBOTS * GROUPS
WORDS = 56
STEPS_WORD = 56
ENTRY = 64
ORDER = ROBOTS * ENTRY
CASE_STEPS = ORDER + 32
CASE_START = ORDER + 40
LATE = ORDER + 48
LATE_STEPS = 28
LATE_SLOTS = 256
TABLE_ROWS = 24
ARRIVALS = 3
EARLY_GROUPS = 3
GRANT = 16 * 1024 * 1024
MESH = pl.DeviceIdType.MESH


def iota(axis, shape=(8, LANES)):
    return lax.broadcasted_iota(jnp.int32, shape, axis)


def pair_argument(a, b):
    dx, dy, dz = a[0] - b[0], a[1] - b[1], a[2] - b[2]
    spread = a[3] + b[3]
    return (dx * dx + dy * dy + dz * dz) / (-spread * spread)


def pair_term(a, b):
    return jnp.exp2(pair_argument(a, b))


def centre_rows(ref, robot, axis, group, half):
    first = min(8 * group, SPHERES - 8)
    row = ((axis * SPHERES + first) * 2 + half) * ROBOTS_HERE + robot
    value = ref[pl.ds(row, 8, stride=2 * ROBOTS_HERE), :]
    return value if first == 8 * group else pltpu.roll(value, 4, 0)


def spread_kernel(
    counts_hbm,
    centres_hbm,
    radius_hbm,
    adjacency_hbm,
    recv_ref,
    turned_ref,
    self_ref,
    table_ref,
    counts_ref,
    centres_ref,
    radius_ref,
    adjacency_ref,
    send,
    swept,
    note_send,
    note_recv,
    note,
    load_sem,
    send_sem,
    recv_sem,
    note_send_sem,
    note_recv_sem,
):
    me = lax.axis_index("robot")
    seed = lax.axis_index("seed")
    peers = [lax.rem(me + step, ROBOT_DEVICES) for step in range(1, ROBOT_DEVICES)]

    loads = [
        pltpu.make_async_copy(counts_hbm, counts_ref, load_sem.at[0]),
        pltpu.make_async_copy(radius_hbm, radius_ref, load_sem.at[1]),
        pltpu.make_async_copy(adjacency_hbm, adjacency_ref, load_sem.at[2]),
    ]
    per_axis, early = 4 * SPHERES, 4 * 8 * EARLY_GROUPS
    for axis in range(3):
        at = pl.ds(axis * per_axis, early)
        loads.append(pltpu.make_async_copy(centres_hbm.at[at], centres_ref.at[at], load_sem.at[3 + axis]))
    for axis in range(3):
        at = pl.ds(axis * per_axis + early, per_axis - early)
        loads.append(pltpu.make_async_copy(centres_hbm.at[at], centres_ref.at[at], load_sem.at[6 + axis]))
    for load in loads:
        load.start()

    barrier = pltpu.get_barrier_semaphore()
    for peer in peers:
        pl.semaphore_signal(barrier, inc=1, device_id=(peer, seed), device_id_type=MESH)

    for load in loads[:6]:
        load.wait()

    sub, lane = iota(0), iota(1)
    part = lane // PART
    last_waypoint = lane % W == W - 1
    radius_lane = iota(1, (8, SPHERES))
    radius_sub = iota(0, (8, SPHERES))
    note_send[...] = jnp.zeros((ROBOTS_HERE, LANES), jnp.int32)
    note_send[:, 0:ROBOTS] = adjacency_ref[...]
    for robot in range(ROBOTS_HERE):
        note_send[robot : robot + 1, COUNT_LANE : COUNT_LANE + 1] = jnp.full((1, 1), counts_ref[robot], jnp.int32)
    ends = {}
    for group in range(GROUPS):
        if group == EARLY_GROUPS:
            for load in loads[6:]:
                load.wait()
        for robot in range(ROBOTS_HERE):
            count = counts_ref[robot]
            radius_row = jnp.broadcast_to(radius_ref[robot : robot + 1, :], (8, SPHERES))
            number = (me * ROBOTS_HERE + robot) * 64 + 1
            radius = jnp.sum(
                jnp.where(radius_lane == radius_sub + 8 * group, radius_row, 0.0),
                axis=1,
                keepdims=True,
            )
            sphere = sub + 8 * group
            active = sphere < count
            far = FAR * (sphere + number).astype(jnp.float32)
            for half in range(2):
                out, square = [], None
                for axis in range(3):
                    here = centre_rows(centres_ref, robot, axis, group, half)
                    ahead = jnp.where(last_waypoint, here, pltpu.roll(here, LANES - 1, 1))
                    step = ahead - here
                    square = step * step if square is None else square + step * step
                    middle = (here + ahead) * (0.5 * ROOT)
                    out.append(jnp.where(active, middle, far if axis == 0 else 0.0))
                out.append(jnp.where(active, radius + 0.5 * jnp.sqrt(square + 1e-6), 1.0))
                for quantity in range(4):
                    value = out[quantity]
                    swept[half * ROBOTS_HERE + robot, quantity, 8 * group : 8 * group + 8, :] = value
                    if group == GROUPS - 1:
                        if robot == 0:
                            ends[half, quantity] = value
                            continue
                        value = jnp.where(sub < 4, ends[half, quantity], pltpu.roll(value, 4, 0))
                    value = pltpu.roll(value, 0, 1, stride=PART, stride_axis=0)
                    for bit in (1, 2, 4):
                        value = jnp.where(part & bit != 0, pltpu.roll(value, 8 - bit, 0), value)
                    row = (robot * GROUPS + group) * 4 + quantity
                    if group == GROUPS - 1:
                        row = SHARED + quantity
                    send[pl.ds(half * 8 * ROWS + row, 8, stride=ROWS), :] = value

    pl.semaphore_wait(barrier, ROBOT_DEVICES - 1)

    def slot_of(device):
        return (device // 8) * 8 + lax.rem(8 - lax.rem(device, 8), 8)

    def sent_of(slot):
        return pl.ds(pl.multiple_of(slot * ROWS, 8), MESSAGE)

    def send_note(number):
        return pltpu.make_async_remote_copy(
            src_ref=note_send,
            dst_ref=note_recv.at[me],
            send_sem=note_send_sem.at[number],
            recv_sem=note_recv_sem.at[number],
            device_id=(lax.rem(me + 1 + number, ROBOT_DEVICES), seed),
            device_id_type=MESH,
        )

    def send_rows(number):
        peer = lax.rem(me + 1 + number, ROBOT_DEVICES)
        return pltpu.make_async_remote_copy(
            src_ref=send.at[sent_of(slot_of(peer))],
            dst_ref=recv_ref.at[sent_of(me)],
            send_sem=send_sem.at[number],
            recv_sem=recv_sem.at[number],
            device_id=(peer, seed),
            device_id_type=MESH,
        )

    def for_peers(act):
        def one(number, carry):
            act(number)
            return carry

        lax.fori_loop(0, ROBOT_DEVICES - 1, one, 0)

    for_peers(lambda number: send_note(number).start())
    for_peers(lambda number: send_rows(number).start())
    note_recv[me] = note_send[...]
    recv_ref[sent_of(me), :] = send[sent_of(slot_of(me)), :]
    first_robot = ((part[0:1, :] + (8 - lax.rem(me, 8))) & 7) < 4

    def split_shared(device):
        row = pl.multiple_of(device * ROWS, 8)
        for quantity in range(4):
            shared = recv_ref[pl.ds(row + SHARED + quantity, 1), :]
            second = shared
            if quantity == 0:
                number = (device * ROBOTS_HERE) * 64 + 61
                far = FAR * jnp.full((1, LANES), number, jnp.int32).astype(jnp.float32)
                second = jnp.where(first_robot, far + 64.0 * FAR, shared)
                recv_ref[pl.ds(row + SHARED, 1), :] = jnp.where(first_robot, shared, far)
            recv_ref[pl.ds(row + MESSAGE + quantity, 1), :] = second
    def turn_rows(device):
        row = pl.multiple_of(device * ROWS, 8)
        for n in range(ROWS):
            line = jnp.broadcast_to(recv_ref[pl.ds(row + n, 1), :], (8, LANES))
            turned_ref[row + n] = pltpu.roll(line, 0, 1, stride=PART, stride_axis=0)

    split_shared(me)
    turn_rows(me)
    for index in range(2 * ROBOTS_HERE):
        robot = index % ROBOTS_HERE
        number = (me * ROBOTS_HERE + robot) * 64 + 1
        for quantity in range(4):
            fill = jnp.full((8, LANES), float(quantity == 3))
            if quantity == 0:
                fill = FAR * (sub + 8 * GROUPS + number).astype(jnp.float32)
            swept[index, quantity, 8 * GROUPS : 8 * GROUPS + 8, :] = fill

    def self_pairs(index, carry):
        sums = [jnp.zeros((8, LANES), jnp.float32) for _ in range(4)]
        turn = 0
        for group in range(GROUPS):
            first = [swept[index, q, 8 * group : 8 * group + 8, :] for q in range(4)]
            for apart in range(2, SPHERES - 8 * group):
                start = 8 * group + apart
                second = [swept[index, q, start : start + 8, :] for q in range(4)]
                sums[turn] = sums[turn] + pair_term(first, second)
                turn = (turn + 1) % 4
        total = jnp.sum((sums[0] + sums[1]) + (sums[2] + sums[3]), axis=0, keepdims=True)
        self_ref[pl.ds(index, 1), :] = total * (1.0 / (SPHERES * SPHERES))
        return carry

    lax.fori_loop(0, 2 * ROBOTS_HERE, self_pairs, 0)

    for_peers(lambda number: send_note(number).wait_recv())
    for device in range(ROBOT_DEVICES):
        note[ROBOTS_HERE * device : ROBOTS_HERE * (device + 1), :] = note_recv[device]
    shape = (ROBOTS, LANES)
    row, column = iota(0, shape), iota(1, shape)
    row_number = row.astype(jnp.float32)
    noted = note[...].astype(jnp.float32)
    link = jnp.where((column > row) & (column < ROBOTS) & (noted != 0.0), 1.0, 0.0)
    counts = jnp.sum(jnp.where(column == COUNT_LANE, noted, 0.0), axis=1, keepdims=True)
    groups = jnp.floor((counts + 7.0) * 0.125)

    def as_row(value):
        return jnp.sum(jnp.where(row == column, value, 0.0), axis=0, keepdims=True)

    length = link * as_row(groups)
    before = (iota(0, (LANES, LANES)) < iota(1, (LANES, LANES))).astype(jnp.float32)
    start = jnp.dot(length, before, preferred_element_type=jnp.float32)
    end = start + length
    words = jnp.zeros(shape, jnp.int32)
    for byte in range(4):
        place = (column * 4 + byte).astype(jnp.float32)
        listed = jnp.full(shape, float(ROW_IDS))
        for robot in range(1, ROBOTS):
            first, past = start[:, robot : robot + 1], end[:, robot : robot + 1]
            listed = jnp.where(
                (place >= first) & (place < past), place + (float(GROUPS * robot) - first), listed
            )
        words = words | (listed.astype(jnp.int32) << (8 * byte))
    steps = jnp.floor((jnp.sum(length, axis=1, keepdims=True) + (STEP_ROWS - 1.0)) * (1.0 / STEP_ROWS))
    words = jnp.where(column == STEPS_WORD, steps.astype(jnp.int32), words)
    note[...] = jnp.where(column < ENTRY, words, 0)
    table_ref[0:16, :] = note[pl.ds(0, 16, stride=2), :] + pltpu.roll(
        note[pl.ds(1, 16, stride=2), :], ENTRY, 1
    )
    busy = jnp.where(steps > 0.0, 1.0, 0.0)
    key = groups * 32.0 + row_number
    key_row, busy_row = as_row(key), as_row(busy)
    rank = jnp.sum(jnp.where(key_row < key, busy_row, 0.0), axis=1, keepdims=True)
    lane_number = column.astype(jnp.float32)
    last = jnp.sum(
        jnp.where((rank == lane_number) & (busy > 0.0), row_number, 0.0), axis=0, keepdims=True
    )
    steps_row = as_row(steps)
    rank_row = as_row(rank)
    done_before = jnp.sum(
        jnp.where((rank_row < rank) & (busy_row > 0.0), steps_row, 0.0), axis=1, keepdims=True
    )
    all_steps = jnp.sum(steps_row, axis=1, keepdims=True)
    late_start = jnp.maximum(all_steps - float(LATE_STEPS), 0.0)
    holds = (busy > 0.0) & (done_before <= late_start) & (late_start < done_before + steps)

    def held(value):
        return jnp.sum(jnp.where(holds, value, 0.0), axis=0, keepdims=True)

    line = iota(1, (1, LANES))
    for n, value in enumerate((held(rank), held(late_start - done_before), all_steps - late_start)):
        last = jnp.where(line == LATE - ORDER + n, value, last)
    for case in range(FIRST_GROUPS, GROUPS + 1):
        of_case = jnp.sum(jnp.where(groups == float(case), steps, 0.0), axis=0, keepdims=True)
        before_case = jnp.sum(jnp.where(groups < float(case), steps, 0.0), axis=0, keepdims=True)
        earlier = jnp.sum(jnp.where(groups < float(case), busy, 0.0), axis=0, keepdims=True)
        of_case = jnp.minimum(jnp.maximum(late_start - before_case, 0.0), of_case)
        last = jnp.where(line == CASE_STEPS - ORDER + case - FIRST_GROUPS, of_case, last)
        last = jnp.where(line == CASE_START - ORDER + case - FIRST_GROUPS, earlier, last)
    table_ref[16:24, :] = jnp.broadcast_to(last, (8, LANES)).astype(jnp.int32)
    recv_ref[ROBOT_DEVICES * ROWS : ROBOT_DEVICES * ROWS + 8, :] = jnp.where(
        sub == 0, -1000.0 * FAR, jnp.where(sub == 3, 1.0, 0.0)
    )

    def arrive(index, carry):
        numbers = [ARRIVALS * index + n for n in range(ARRIVALS)]
        sources = [lax.rem(me + ROBOT_DEVICES - 1 - number, ROBOT_DEVICES) for number in numbers]
        for number in numbers:
            send_rows(number).wait_recv()
        for source in sources:
            split_shared(source)
        for source in sources:
            turn_rows(source)
        return carry

    lax.fori_loop(0, (ROBOT_DEVICES - 1) // ARRIVALS, arrive, 0)
    for_peers(lambda number: send_note(number).wait_send())
    for_peers(lambda number: send_rows(number).wait_send())


def pair_sums(rows, turned, groups, robot, ids):
    a_row = robot * (4 * GROUPS)
    sums = []
    for row_id in ids:
        b = [jnp.broadcast_to(rows[pl.ds(row_id * 4 + q, 1), :], (8, LANES)) for q in range(4)]
        terms = []
        for group in range(groups):
            a = [turned[a_row + (group * 4 + q)] for q in range(4)]
            terms.append(pair_term(a, b))
        while len(terms) > 1:
            terms = [p + q for p, q in zip(terms[0::2], terms[1::2])] + terms[len(terms) & ~1 :]
        sums.append(terms[0])
    own = sums
    while len(own) > 1:
        own = [p + q for p, q in zip(own[0::2], own[1::2])]
    return sums + own


def step_of(table, turn, step, there):
    robot = jnp.minimum(table[ORDER + turn], ROBOTS - 1)
    entry = robot * ENTRY
    nothing = jnp.int32(ROW_IDS * 0x01010101 - (1 << 32))
    words = [jnp.where(there, table[entry + 2 * step + n], nothing) for n in range(2)]
    ids = [lax.shift_right_logical(word, 8 * n) & 255 for word in words for n in range(4)]
    step = step + 1
    over = (step >= table[entry + STEPS_WORD]).astype(jnp.int32)
    return robot, ids, jnp.minimum(turn + over, ROBOTS - 1), step * (1 - over)


def cross_kernel(table, rows, turned, total):
    zero = jnp.zeros((8, LANES), jnp.float32)

    def clear(index, carry):
        for n in range(15):
            total[index * 15 + n] = zero
        return carry

    lax.fori_loop(0, (ROW_IDS + 1) // 15, clear, 0)

    def add_up(robot, ids, found):
        ids = ids + [robot * GROUPS]
        olds = [total[row_id] for row_id in ids]
        for row_id, old, new in zip(ids, olds, found):
            total[row_id] = old + new

    for groups in range(FIRST_GROUPS, GROUPS + 1):
        steps = table[CASE_STEPS + groups - FIRST_GROUPS]

        def two_steps_of(index, turn, step):
            robot, ids, turn, step = step_of(table, turn, step, 2 * index < steps)
            other, other_ids, turn, step = step_of(table, turn, step, 2 * index + 1 < steps)
            return turn, step, robot, other, *ids, *other_ids

        def two_steps(index, state, groups=groups, two_steps_of=two_steps_of):
            turn, step, robot, other, *ids = state
            ids, other_ids = ids[:STEP_ROWS], ids[STEP_ROWS:]
            found = pair_sums(rows, turned, groups, robot, ids)
            other_found = pair_sums(rows, turned, groups, other, other_ids)
            add_up(robot, ids, found)
            add_up(other, other_ids, other_found)
            return two_steps_of(index + 1, turn, step)

        start = jnp.minimum(table[CASE_START + groups - FIRST_GROUPS], ROBOTS - 1)
        lax.fori_loop(0, (steps + 1) >> 1, two_steps, two_steps_of(0, start, jnp.int32(0)))


def blend_kernel(
    table_ref,
    rows,
    turned,
    total,
    self_ref,
    centres_ref,
    robot_cost_ref,
    gathered,
    table,
    late,
    late_robot,
    sums,
    cost_ref,
    cost_recv,
    weight,
    packed,
    parts,
    table_sem,
    cost_sems,
    part_sems,
    gather_sems,
):
    me = lax.axis_index("robot")
    seed = lax.axis_index("seed")
    x, z = seed // Z, lax.rem(seed, Z)
    peers = [lax.rem(me + step, ROBOT_DEVICES) for step in range(1, ROBOT_DEVICES)]
    z_peers = [lax.rem(z + step, Z) for step in (4, 3, 5, 2, 6, 1, 7)]
    seed_peers = [lax.rem((1 - x) * Z + lax.rem(z + 4, Z), 2 * Z)] + [p for step in (3, 5, 2, 6, 1, 7, 0) for p in ([(1 - x) * Z + lax.rem(z + step, Z)])]
    seed_peers = seed_peers[:3] + [x * Z + lax.rem(z + 4, Z)] + seed_peers[3:5] + [x * Z + lax.rem(z + 3, Z), x * Z + lax.rem(z + 5, Z)] + seed_peers[5:7] + [x * Z + lax.rem(z + 2, Z), x * Z + lax.rem(z + 6, Z)] + seed_peers[7:] + [x * Z + lax.rem(z + 1, Z), x * Z + lax.rem(z + 7, Z)]

    barrier = pltpu.get_barrier_semaphore()

    def greet(number, carry):
        peer = lax.rem(me + 1 + lax.rem(number + 7, ROBOT_DEVICES - 1), ROBOT_DEVICES)
        pl.semaphore_signal(barrier, inc=1, device_id=(peer, seed), device_id_type=MESH)
        return carry

    lax.fori_loop(0, ROBOT_DEVICES - 1, greet, 0)

    def greet_seed(number, carry):
        peer = lax.rem(seed + 1 + number, 2 * Z)
        pl.semaphore_signal(barrier, inc=1, device_id=(me, peer), device_id_type=MESH)
        return carry

    lax.fori_loop(0, 2 * Z - 1, greet_seed, 0)

    load = pltpu.make_async_copy(table_ref, table, table_sem)
    load.start()
    line = iota(1, (1, LANES))
    for robot in range(ROBOTS):
        found = total[robot * GROUPS]
        for group in range(1, GROUPS):
            found = found + total[robot * GROUPS + group]
        sums[robot] = found
    for slot in range(9 * LATE_STEPS, LATE_SLOTS):
        late[slot] = jnp.zeros((8, LANES), jnp.float32)
        late_robot[slot : slot + 1, :] = jnp.zeros((1, LANES), jnp.float32)
    load.wait()
    late_count = table[LATE + 2]

    def late_steps(index, place):
        turn, step = place
        jobs = []
        for n in range(4):
            jobs.append(step_of(table, turn, step, 4 * index + n < late_count))
            turn, step = jobs[-1][2:]
        slot = 4 * (STEP_ROWS + 1) * index
        for robot, ids, _, _ in jobs:
            found = pair_sums(rows, turned, GROUPS, robot, ids)
            for value, holder in zip(found, [row_id // GROUPS for row_id in ids] + [robot]):
                late[slot] = value
                late_robot[pl.ds(slot, 1), :] = jnp.where(line == holder, 1.0, 0.0)
                slot = slot + 1
        return turn, step

    lax.fori_loop(0, LATE_STEPS // 4, late_steps, (table[LATE], table[LATE + 1]))
    late_cost = lax.dot_general(
        late_robot[...],
        jnp.sum(late[...], axis=1),
        (((0,), (0,)), ((), ())),
        precision=lax.Precision.HIGHEST,
        preferred_element_type=jnp.float32,
    )
    cost = jnp.sum(sums[...], axis=1) + late_cost[0:ROBOTS, :]
    for shift in (64, 32, 16):
        cost = cost + pltpu.roll(cost, shift, 1)
    cost = cost * (1.0 / (SPHERES * SPHERES))
    for device in range(ROBOT_DEVICES):
        cost_ref[device] = cost[ROBOTS_HERE * device : ROBOTS_HERE * (device + 1), :]

    pl.semaphore_wait(barrier, ROBOT_DEVICES - 1 + 2 * Z - 1)

    def start(src, dst, sems, number, device):
        copy = pltpu.make_async_remote_copy(
            src_ref=src,
            dst_ref=dst,
            send_sem=sems.at[0, number],
            recv_sem=sems.at[1, number],
            device_id=device,
            device_id_type=MESH,
        )
        copy.start()
        return copy

    copies = [
        start(cost_ref.at[peer], cost_recv.at[me], cost_sems, number, (peer, seed))
        for number, peer in enumerate(peers)
    ]
    cost_recv[me] = cost_ref[me]
    for copy in copies:
        copy.wait_recv()
    sent = copies

    lane = iota(1, (ROBOTS_HERE, LANES))
    part = lane // PART
    square = (LANES, LANES)
    same_seed = jnp.where(iota(0, square) // W == iota(1, square) // W, 1.0, 0.0)
    for half in range(2):
        cost = self_ref[half * ROBOTS_HERE : (half + 1) * ROBOTS_HERE, :]
        for k in range(8):
            cost = cost + jnp.where(part == k, cost_recv[half * 8 + k], 0.0)
        robot_cost_ref[:, half * LANES : (half + 1) * LANES] = cost
        cost = jnp.dot(
            cost, same_seed, precision=lax.Precision.HIGHEST, preferred_element_type=jnp.float32
        )
        weight[half] = 1.0 / (1.0 + cost)
    weights = weight[0] + weight[1]
    weights = weights + pltpu.roll(weights, 64, 1)
    weights = weights + pltpu.roll(weights, 32, 1)
    total_row = jnp.where(line < 64, weights[0:1, :], weights[1:2, :])

    quarter = iota(1) // W
    units = [[], []]
    for robot in range(ROBOTS_HERE):
        weights = [
            jnp.broadcast_to(weight[half, robot : robot + 1, :], (8, LANES)) for half in range(2)
        ]
        for axis in range(3):
            for group in range(GROUPS):
                value = (
                    centre_rows(centres_ref, robot, axis, group, 0) * weights[0]
                    + centre_rows(centres_ref, robot, axis, group, 1) * weights[1]
                )
                value = value + pltpu.roll(value, 64, 1)
                units[robot].append(value + pltpu.roll(value, 32, 1))
        units[robot].append(jnp.zeros((8, LANES), jnp.float32))
    for v in range(CHUNK):
        value = jnp.where(
            quarter < 2,
            jnp.where(quarter == 0, units[0][v], units[0][CHUNK + v]),
            jnp.where(quarter == 2, units[1][v], units[1][CHUNK + v]),
        )
        done = 0
        while done < 8:
            chunk, row = divmod(8 * v + done, CHUNK)
            length = min(8 - done, CHUNK - row)
            packed[chunk, row : row + length, :] = value[done : done + length, :]
            done += length
    for chunk in range(Z):
        packed[chunk, CHUNK : CHUNK + 1, :] = total_row

    copies = [
        start(packed.at[peer], parts.at[number], part_sems, number, (me, x * Z + peer))
        for number, peer in enumerate(z_peers)
    ]
    found = packed[z]
    for number, copy in enumerate(copies):
        copy.wait_recv()
        found = found + parts[number]
    sent = sent + copies

    gathered[seed] = found
    copies = [
        start(gathered.at[seed], gathered.at[seed], gather_sems, number, (me, peer))
        for number, peer in enumerate(seed_peers)
    ]
    for copy in copies:
        copy.wait_recv()
    sent = sent + copies

    for copy in sent:
        copy.wait_send()


def finish_kernel(cost_in, gathered, cost_out, blended, lines):
    cost_out[...] = cost_in[...]
    for chunk in range(Z):
        found = gathered[chunk] + gathered[Z + chunk]
        found = found / found[CHUNK : CHUNK + 1, :]
        lines[CHUNK * chunk : CHUNK * (chunk + 1), :] = found[0:CHUNK, :]
    turned = lines[...].T
    for robot in range(ROBOTS_HERE):
        for axis in range(3):
            for quarter in range(2):
                low = max(axis * GROUPS, quarter * CHUNK)
                high = min((axis + 1) * GROUPS, (quarter + 1) * CHUNK)
                if low < high:
                    source = (robot * 2 + quarter) * W
                    lane = 8 * (low - quarter * CHUNK)
                    first = 8 * (low - axis * GROUPS)
                    width = min(8 * (high - low), SPHERES - first)
                    blended[robot, axis, :, first : first + width] = turned[
                        source : source + W, lane : lane + width
                    ]


def in_vmem(count):
    return [pl.BlockSpec(memory_space=pltpu.VMEM)] * count


IN_SMEM = pl.BlockSpec(memory_space=pltpu.SMEM)


def local(centres, sphere_radius, counts, adjacency):
    dma = pltpu.SemaphoreType.DMA
    f32 = jnp.float32
    peers = ROBOT_DEVICES - 1
    rows = centres.transpose(1, 2, 0, 3).reshape(3 * SPHERES, ROBOTS_HERE, 2, LANES)
    rows = rows.transpose(0, 2, 1, 3).reshape(3 * SPHERES * 2 * ROBOTS_HERE, LANES)
    in_hbm = pl.BlockSpec(memory_space=pltpu.HBM)
    received, turned, self_cost, table = pl.pallas_call(
        spread_kernel,
        out_shape=(
            jax.ShapeDtypeStruct((ROBOT_DEVICES * ROWS + 8, LANES), f32),
            jax.ShapeDtypeStruct((ROBOT_DEVICES * ROWS, 8, LANES), f32),
            jax.ShapeDtypeStruct((2 * ROBOTS_HERE, LANES), f32),
            jax.ShapeDtypeStruct((TABLE_ROWS, LANES), jnp.int32),
        ),
        in_specs=[in_hbm] * 4,
        out_specs=tuple(in_vmem(4)),
        scratch_shapes=[
            pltpu.SMEM((ROBOTS_HERE,), jnp.int32),
            pltpu.VMEM(rows.shape, f32),
            pltpu.VMEM((ROBOTS_HERE, SPHERES), f32),
            pltpu.VMEM((ROBOTS_HERE, ROBOTS), jnp.int32),
            pltpu.VMEM((ROBOT_DEVICES * ROWS, LANES), f32),
            pltpu.VMEM((2 * ROBOTS_HERE, 4, 64, LANES), f32),
            pltpu.VMEM((ROBOTS_HERE, LANES), jnp.int32),
            pltpu.VMEM((ROBOT_DEVICES, ROBOTS_HERE, LANES), jnp.int32),
            pltpu.VMEM((ROBOTS, LANES), jnp.int32),
            dma((9,)),
            dma((peers,)),
            dma((peers,)),
            dma((peers,)),
            dma((peers,)),
        ],
        compiler_params=pltpu.CompilerParams(
            collective_id=0, has_side_effects=True, vmem_limit_bytes=GRANT
        ),
        name="spread",
    )(*[pltpu.with_memory_space_constraint(v, pltpu.HBM) for v in (counts, rows, sphere_radius, adjacency)])
    flat_table = table.reshape(TABLE_ROWS * LANES)
    total = pl.pallas_call(
        cross_kernel,
        out_shape=jax.ShapeDtypeStruct((ROW_IDS + 1, 8, LANES), f32),
        in_specs=[IN_SMEM] + in_vmem(2),
        out_specs=in_vmem(1)[0],
        compiler_params=pltpu.CompilerParams(vmem_limit_bytes=GRANT),
        name="cross",
    )(flat_table, received, turned)
    robot_cost, gathered = pl.pallas_call(
        blend_kernel,
        out_shape=(
            jax.ShapeDtypeStruct((ROBOTS_HERE, COLUMNS), f32),
            jax.ShapeDtypeStruct((2 * Z, CHUNK + 1, LANES), f32),
        ),
        in_specs=in_vmem(6),
        out_specs=tuple(in_vmem(2)),
        scratch_shapes=[
            pltpu.SMEM((TABLE_ROWS * LANES,), jnp.int32),
            pltpu.VMEM((LATE_SLOTS, 8, LANES), f32),
            pltpu.VMEM((LATE_SLOTS, LANES), f32),
            pltpu.VMEM((ROBOTS, 8, LANES), f32),
            pltpu.VMEM((ROBOT_DEVICES, ROBOTS_HERE, LANES), f32),
            pltpu.VMEM((ROBOT_DEVICES, ROBOTS_HERE, LANES), f32),
            pltpu.VMEM((2, ROBOTS_HERE, LANES), f32),
            pltpu.VMEM((Z, CHUNK + 1, LANES), f32),
            pltpu.VMEM((Z - 1, CHUNK + 1, LANES), f32),
            dma,
            dma((2, peers)),
            dma((2, Z - 1)),
            dma((2, 2 * Z - 1)),
        ],
        compiler_params=pltpu.CompilerParams(
            collective_id=1, has_side_effects=True, vmem_limit_bytes=GRANT
        ),
        name="blend",
    )(flat_table, received, turned, total, self_cost, rows)
    robot_cost, blended = pl.pallas_call(
        finish_kernel,
        out_shape=(
            jax.ShapeDtypeStruct((ROBOTS_HERE, COLUMNS), f32),
            jax.ShapeDtypeStruct((ROBOTS_HERE, 3, W, SPHERES), f32),
        ),
        in_specs=in_vmem(2),
        out_specs=tuple(in_vmem(2)),
        scratch_shapes=[pltpu.VMEM((LANES, LANES), f32)],
        compiler_params=pltpu.CompilerParams(vmem_limit_bytes=GRANT),
        name="finish",
    )(robot_cost, gathered)
    return robot_cost, blended.transpose(0, 1, 3, 2)


def solution(mesh):
    return jax.shard_map(
        local,
        mesh=mesh,
        in_specs=(P("robot", None, None, "seed"), P("robot", None), P("robot"), P("robot", None)),
        out_specs=(P("robot", "seed"), P("robot", None, None, None)),
        check_vma=False,
    )
```
